32 devices in a mesh: seq: 4 (over y, core), fsdp: 8 (over z, x).
Axes of the slice: x: 2, y: 2, z: 4, core: 2. Of those that a mesh axis runs over, the one named last changes fastest.
Arguments:
- tokens: bfloat16 [8, 1024, 2048], P('fsdp', 'seq'), may hold values from -6 to 6
- teacher: bfloat16 [8, 1024, 2048], P('fsdp', 'seq'), may hold values from -6 to 6
- segments: int32 [8, 1024], P('fsdp'), may hold values from 0 to 3, never falling along the last dimension, each value on 1 to 512 neighbouring positions
- valid: int32 [8, 1024], P('fsdp', 'seq'), may hold values from 0 to 1, as said below
- ln1_gain: bfloat16 [2048], P('fsdp'), may hold values from 0.099609375 to 1.8984375
- ln1_bias: bfloat16 [2048], P('fsdp'), may hold values from -1.75 to 1.75
- w_qkv: bfloat16 [2048, 6144], P('fsdp'), may hold values from -0.125 to 0.125
- b_qkv: bfloat16 [6144], P('fsdp'), may hold values from -1.75 to 1.75
- w_out: bfloat16 [2048, 2048], P('fsdp'), may hold values from -0.5 to 0.5
- ln2_gain: bfloat16 [2048], P('fsdp'), may hold values from 0.099609375 to 1.8984375
- ln2_bias: bfloat16 [2048], P('fsdp'), may hold values from -1.75 to 1.75
- w_gate_up: bfloat16 [5632, 2, 2048], P('fsdp'), may hold values from -0.125 to 0.125
- w_down: bfloat16 [5632, 2048], P('fsdp'), may hold values from -0.15625 to 0.15625
Outputs:
- layer_out: bfloat16 [8, 1024, 2048], P('fsdp', 'seq')
- loss: float32 [], replicated
- grad_tokens: bfloat16 [8, 1024, 2048], P('fsdp', 'seq')
- grad_ln1_gain: float32 [2048], P('fsdp')
- grad_ln1_bias: float32 [2048], P('fsdp')
- grad_w_qkv: float32 [2048, 6144], P('fsdp')
- grad_b_qkv: float32 [6144], P('fsdp')
- grad_w_out: float32 [2048, 2048], P('fsdp')
- grad_ln2_gain: float32 [2048], P('fsdp')
- grad_ln2_bias: float32 [2048], P('fsdp')
- grad_w_gate_up: float32 [5632, 2, 2048], P('fsdp')
- grad_w_down: float32 [5632, 2048], P('fsdp')
The draws below stay inside these ranges and needn't reach their ends.
Inputs may be any that keep to these rules, and one draw needn't show every extreme that they name: `segments`: segment numbers start at 0 in each sequence and never fall; each document has 1 to 512 tokens and one document of each sequence has exactly that many. `valid`: the first token of every sequence counts.
All inputs are finite; a program needn't handle non-finite values.
Results may differ from the reference program's by a relative error of at most 0.01.
Values may be sent and summed in bfloat16 or wider, within the bound.
No kernel may reach another device: no remote copies, remote signals or barrier semaphores. Data moves between devices by JAX's collectives and lax.ppermute only.
A program may use at most 704 MiB of HBM per device.

```python
import math
import jax
import jax.numpy as jnp
import numpy as np
from jax import lax

D = 2048
H = 32
HD = 64
FF = 5632
ROT = 16
LENGTH = 1024
SEQS = 8
TOKENS = 8192
DOCS = 4
BLOCK = 512


def draw_valid(key, part):
    places = jnp.arange(LENGTH, dtype=jnp.int32)[None, :]
    sequence_ids = jnp.arange(SEQS, dtype=jnp.int32)[:, None]
    threshold = 300 + 600 * places // LENGTH + 50 * sequence_ids // SEQS
    threshold = jnp.where(places == 0, 1000, threshold)
    rolled = jax.random.randint(key, (SEQS, LENGTH), 0, 1000, dtype=jnp.int32)
    return (rolled < threshold).astype(jnp.int32)


def level_of(key, shape, pieces, smallest, top_value):
    def one(position, shards_of):
        heights = jax.random.uniform(jax.random.fold_in(jax.random.fold_in(key, 6), position), (shards_of,), jnp.float32, smallest / len(pieces), top_value / len(pieces))
        return jnp.repeat(jnp.exp(heights), shape[position] // shards_of).reshape((-1,) + (1,) * (len(shape) - position - 1))

    factor_of = one(*pieces[0])
    for cut in pieces[1:]:
        factor_of = factor_of * one(*cut)
    return factor_of


def length_profile(count, total, limit, lean):
    loads = [(1 << 20) // math.isqrt(rank ** lean) + 1 for rank in range(2, count + 1)]
    spare, given = total - limit - (count - 1), [1] * (count - 1)
    while spare > 0:
        free = [i for i in range(count - 1) if given[i] < limit]
        mass, remaining = sum([loads[i] for i in free]), spare
        for i in free:
            extra = min(limit - given[i], max(1, remaining * loads[i] // mass), spare)
            given[i] = given[i] + extra
            spare = spare - extra
    return np.array([limit] + given)


def uneven(key, amount, total, most, slope):
    if amount == 2:
        one = jax.random.randint(key, (), max(1, total - most), min(most, total - 1) + 1)
        return jnp.stack([one, total - one])
    sizes = jnp.asarray(length_profile(amount, total, most, slope), jnp.int32)
    couples = (amount - 1) // 2
    source_of, sink = sizes[1:1 + 2 * couples:2], sizes[2:2 + 2 * couples:2]
    slack = jnp.minimum(source_of - 1, most - sink)
    passed = jax.random.randint(jax.random.fold_in(key, 1), (couples,), 0, 1 << 20) % (slack + 1)
    sizes = sizes.at[1:1 + 2 * couples:2].set(source_of - passed).at[2:2 + 2 * couples:2].set(sink + passed)
    return sizes[jax.random.permutation(jax.random.fold_in(key, 2), amount)]


def normal_values(rng, dims, scale, most, split=(), held_as=jnp.bfloat16):
    gain = level_of(rng, dims, split, -0.22, 0.18) if split else 1.0
    result = jax.random.normal(rng, dims, jnp.float32) * scale * gain
    return jnp.minimum(jnp.maximum(result, -most), most).astype(held_as)


def setup_inputs(seed: int = 0) -> dict:
    key_of = jax.random.split(jax.random.key(seed), 14)
    return {
        "tokens": normal_values(key_of[0], (SEQS, LENGTH, D), 1.0, 6.0, ((0, 8), (1, 4))),
        "teacher": normal_values(key_of[1], (SEQS, LENGTH, D), 1.0, 6.0, ((0, 8), (1, 4))),
        "segments": jax.vmap(lambda own: jnp.searchsorted(jnp.cumsum(uneven(own, DOCS, LENGTH, LENGTH // 2, 2)), jnp.arange(LENGTH), side="right"))(jax.random.split(key_of[2], SEQS)).reshape((SEQS, LENGTH)).astype(jnp.int32),
        "valid": draw_valid(jax.random.fold_in(key_of[13], 71), 0),
        "ln1_gain": jnp.clip(1.0 + 0.18 * jax.random.normal(key_of[4], (D,), jnp.float32), 0.099609375, 1.8984375).astype(jnp.bfloat16),
        "ln1_bias": normal_values(key_of[5], (D,), 0.3, 1.75, ((0, 8),)),
        "w_qkv": normal_values(key_of[6], (D, 3 * D), D ** -0.5, 0.125, ((0, 8),)),
        "b_qkv": normal_values(key_of[7], (3 * D,), 0.3, 1.75, ((0, 8),)),
        "w_out": normal_values(key_of[8], (D, D), (D // 16) ** -0.5, 0.5, ((0, 8),)),
        "ln2_gain": jnp.clip(1.0 + 0.18 * jax.random.normal(key_of[9], (D,), jnp.float32), 0.099609375, 1.8984375).astype(jnp.bfloat16),
        "ln2_bias": normal_values(key_of[10], (D,), 0.3, 1.75, ((0, 8),)),
        "w_gate_up": normal_values(key_of[11], (FF, 2, D), D ** -0.5, 0.125, ((0, 8),)),
        "w_down": normal_values(key_of[12], (FF, D), (FF // 4) ** -0.5, 0.15625, ((0, 8),)),
    }


EPSILON = 1e-05
MASKED_VALUE = -1e+30
HIGHEST = lax.Precision.HIGHEST

@jax.custom_vjp
def low(v):
    return lax.optimization_barrier(v.astype(jnp.bfloat16)).astype(jnp.float32)

@jax.custom_vjp
def low_back(v):
    return v

def low_keep(v):
    return (low(v), None)

def low_pass(kept, grad):
    return (grad,)

def back_keep(v):
    return (v, None)

def back_low(kept, grad):
    return (low(grad),)
low.defvjp(low_keep, low_pass)
low_back.defvjp(back_keep, back_low)

def layer_norm(values, gain_vec, shift_vec):
    mean_value = lax.optimization_barrier(jnp.mean(values, axis=-1, keepdims=True))
    centered = values - mean_value
    variance = lax.optimization_barrier(jnp.mean(centered * centered, axis=-1, keepdims=True))
    return centered * lax.rsqrt(variance + EPSILON) * gain_vec + shift_vec

def doc_positions(segment):
    places = jnp.arange(segment.shape[0], dtype=jnp.int32)
    change = jnp.concatenate([jnp.ones((1,), dtype=bool), segment[1:] != segment[:-1]])
    starts = lax.cummax(jnp.where(change, places, 0).astype(jnp.int32), axis=0)
    return places - starts

def rotate(values, positions, turn_sign):
    half_rot = ROT // 2
    inverse = 10000.0 ** (-(jnp.arange(half_rot, dtype=jnp.float32) * 2.0) / ROT)
    angles = positions.astype(jnp.float32)[:, None] * inverse[None, :]
    cosine = jnp.cos(angles)[:, None, :]
    sine_part = turn_sign * jnp.sin(angles)[:, None, :]
    front_half = values[..., :half_rot]
    back_half = values[..., half_rot:ROT]
    return jnp.concatenate([front_half * cosine - back_half * sine_part, back_half * cosine + front_half * sine_part, values[..., ROT:]], axis=-1)

def attend(query_rows, key_rows, value_rows, segment):
    places = jnp.arange(LENGTH, dtype=jnp.int32)

    def one_block(first_row):
        query_block = lax.dynamic_slice_in_dim(query_rows, first_row, BLOCK, 0)
        block_seg = lax.dynamic_slice_in_dim(segment, first_row, BLOCK, 0)
        block_places = first_row + jnp.arange(BLOCK, dtype=jnp.int32)
        scores = low_back(jnp.einsum('bhd,lhd->hbl', query_block, key_rows, precision=HIGHEST) * HD ** (-0.5))
        allowed = (block_seg[:, None] == segment[None, :]) & (block_places[:, None] >= places[None, :])
        scores = jnp.where(allowed[None], scores, MASKED_VALUE)
        row_max = lax.optimization_barrier(jnp.max(scores, axis=-1, keepdims=True))
        exp_scores = jnp.exp(scores - row_max)
        probs = low(exp_scores / lax.optimization_barrier(jnp.sum(exp_scores, axis=-1, keepdims=True)))
        return jnp.einsum('hbl,lhd->bhd', probs, value_rows, precision=HIGHEST)
    firsts = jnp.arange(LENGTH // BLOCK, dtype=jnp.int32) * BLOCK
    blocks = lax.map(jax.checkpoint(one_block), firsts)
    return blocks.reshape(LENGTH, H, HD)

def sequence_layer(params_in, inputs_pair):
    ln1_gain, ln1_bias, w_qkv, b_qkv, w_out, ln2_gain, ln2_bias, w_gate_up, w_down = params_in
    tokens_row, segment = inputs_pair
    normed_one = low(layer_norm(tokens_row, ln1_gain, ln1_bias))
    qkv_float = low_back(jnp.dot(normed_one, w_qkv, precision=HIGHEST) + b_qkv)
    split_rows = qkv_float.reshape(LENGTH, 3, H, HD)
    positions = doc_positions(segment)
    query_rows = low(rotate(split_rows[:, 0], positions, 1.0))
    key_rows = low(rotate(split_rows[:, 1], positions, 1.0))
    value_rows = low(split_rows[:, 2])
    heads_out = attend(query_rows, key_rows, value_rows, segment)
    heads_out = low_back(low(heads_out)).reshape(LENGTH, D)
    mixed = low_back(jnp.dot(heads_out, w_out, precision=HIGHEST))
    resid = tokens_row + mixed
    normed_two = low(layer_norm(resid, ln2_gain, ln2_bias))
    gate_up = low_back(jnp.einsum('td,ukd->tku', normed_two, w_gate_up, precision=HIGHEST))
    hidden = low(jax.nn.silu(gate_up[:, 0]) * gate_up[:, 1])
    branch = low_back(jnp.dot(hidden, w_down, precision=HIGHEST))
    return resid + branch

def reference(tokens, teacher, segments, valid, ln1_gain, ln1_bias, w_qkv, b_qkv, w_out, ln2_gain, ln2_bias, w_gate_up, w_down):
    params = (ln1_gain.astype(jnp.float32), ln1_bias.astype(jnp.float32), w_qkv.astype(jnp.float32), b_qkv.astype(jnp.float32), w_out.astype(jnp.float32), ln2_gain.astype(jnp.float32), ln2_bias.astype(jnp.float32), w_gate_up.astype(jnp.float32), w_down.astype(jnp.float32))
    tokens_float = tokens.astype(jnp.float32)
    teacher_float = teacher.astype(jnp.float32)
    counted = valid.astype(jnp.float32)

    def forward(tokens_in, params_in):

        def scan_step(carry_value, inputs_pair):
            return (carry_value, jax.checkpoint(sequence_layer)(params_in, inputs_pair))
        unused, outputs = lax.scan(scan_step, jnp.zeros((), jnp.float32), (tokens_in, segments))
        differ = outputs - teacher_float
        half_sum = 0.5 * jnp.sum(counted[:, :, None] * differ * differ)
        return (outputs, half_sum)
    (outputs, half_sum), pullback = jax.vjp(forward, tokens_float, params)
    grad_in, grad_params = pullback((jnp.zeros_like(outputs), jnp.ones((), jnp.float32)))
    count_all = jnp.sum(counted)
    factor = TOKENS / count_all
    loss = 2.0 * half_sum / (count_all * D)
    return (outputs.astype(jnp.bfloat16), loss, (factor * grad_in).astype(jnp.bfloat16), factor * grad_params[0], factor * grad_params[1], factor * grad_params[2], factor * grad_params[3], factor * grad_params[4], factor * grad_params[5], factor * grad_params[6], factor * grad_params[7], factor * grad_params[8])
```

```python
import functools

import jax
import jax.numpy as jnp
import numpy as np
from jax import lax
from jax.experimental import pallas as pl
from jax.experimental.pallas import tpu as pltpu
from jax.sharding import PartitionSpec as P

H = 32
HD = 64
ROT = 16
LANES = 128

EPSILON = 1e-05
MASKED_VALUE = -1e30

F32 = jnp.float32
BF16 = jnp.bfloat16
VMEM_LIMIT = 60 * 1024 * 1024

RING = (0, 2, 4, 6, 7, 5, 3, 1)
NEXT = [(RING[i], RING[(i + 1) % 8]) for i in range(8)]
PREV = [(RING[(i + 1) % 8], RING[i]) for i in range(8)]
ORDER = np.array([[RING[(RING.index(f) + j) % 8] for j in range(8)] for f in range(8)], np.int32)
CORE = [(s, s ^ 1) for s in range(4)]
ROW = [(s, s ^ 2) for s in range(4)]


def dot_nn(a, b):
    return lax.dot_general(a, b, (((1,), (0,)), ((), ())), preferred_element_type=F32)


def dot_nt(a, b):
    return lax.dot_general(a, b, (((1,), (1,)), ((), ())), preferred_element_type=F32)


def dot_tn(a, b):
    return lax.dot_general(a, b, (((0,), (0,)), ((), ())), preferred_element_type=F32)


def norm_parts(values):
    mean_value = jnp.mean(values, axis=-1, keepdims=True)
    centered = values - mean_value
    variance = jnp.mean(centered * centered, axis=-1, keepdims=True)
    inv_std = lax.rsqrt(variance + EPSILON)
    return (centered * inv_std, inv_std)


def norm_back(grad_out, normed, inv_std, gain_vec):
    scaled = grad_out * gain_vec
    mean_scaled = jnp.mean(scaled, axis=-1, keepdims=True)
    mean_cross = jnp.mean(scaled * normed, axis=-1, keepdims=True)
    return inv_std * (scaled - mean_scaled - normed * mean_cross)


def ring_gather(block, after=()):
    if after:
        block = lax.optimization_barrier((block,) + tuple(after))[0]
    half = block.shape[0] // 2
    blocks = [block] + [None] * 7
    ahead = behind = block
    for step in range(1, 4):
        ahead = lax.ppermute(ahead, "fsdp", NEXT)
        behind = lax.ppermute(behind, "fsdp", PREV)
        blocks[8 - step] = ahead
        blocks[step] = behind
    top = lax.ppermute(ahead[:half], "fsdp", NEXT)
    bottom = lax.ppermute(behind[half:], "fsdp", PREV)
    blocks[4] = (top, bottom)
    return blocks, (ahead, behind)


def ring_scatter(blocks):
    half = blocks[0].shape[0] // 2
    ahead = lax.ppermute(blocks[4][:half], "fsdp", NEXT)
    behind = lax.ppermute(blocks[4][half:], "fsdp", PREV)
    up, down = blocks[3].astype(F32), blocks[5].astype(F32)
    ahead = jnp.concatenate([up[:half] + ahead.astype(F32), up[half:]]).astype(BF16)
    behind = jnp.concatenate([down[:half], down[half:] + behind.astype(F32)]).astype(BF16)
    for step in (2, 1):
        ahead = lax.ppermute(ahead, "fsdp", NEXT)
        behind = lax.ppermute(behind, "fsdp", PREV)
        ahead = (blocks[step].astype(F32) + ahead.astype(F32)).astype(BF16)
        behind = (blocks[8 - step].astype(F32) + behind.astype(F32)).astype(BF16)
    ahead = lax.ppermute(ahead, "fsdp", NEXT)
    behind = lax.ppermute(behind, "fsdp", PREV)
    return blocks[0].astype(F32) + ahead.astype(F32) + behind.astype(F32)


def seq_gather(mine):
    over = lax.ppermute(mine, "seq", ROW)
    beside = lax.ppermute(mine, "seq", CORE)
    return [mine, beside, over, lax.ppermute(over, "seq", CORE)]


def seq_scatter(parts):
    corner = lax.ppermute(parts[3].astype(BF16), "seq", CORE)
    beside = lax.ppermute(parts[1].astype(BF16), "seq", CORE)
    far = (parts[2] + corner.astype(F32)).astype(BF16)
    over = lax.ppermute(far, "seq", ROW)
    return parts[0] + beside.astype(F32) + over.astype(F32)


class Fast:
    def __init__(self, s, f):
        self.s, self.f = s, f
        table = lax.dynamic_index_in_dim(jnp.asarray(ORDER), f, 0, keepdims=False)
        self.order = [table[j] for j in range(8)]
        self.slots = jnp.arange(4, dtype=jnp.int32) ^ s
        self.after = ()

    def weights(self, block):
        blocks, self.after = ring_gather(block, self.after)
        return blocks

    def weights_in_order(self, block):
        size = block.shape[0]
        blocks = self.weights(block)
        whole = jnp.zeros((8 * size, block.shape[1]), BF16)
        for j, part in enumerate(blocks):
            at = self.order[j] * size
            if j == 4:
                whole = lax.dynamic_update_slice(whole, part[0], (at, 0))
                whole = lax.dynamic_update_slice(whole, part[1], (at + size // 2, 0))
            else:
                whole = lax.dynamic_update_slice(whole, part, (at, 0))
        return whole

    def weights_as_found(self, block):
        blocks = self.weights(block)
        return jnp.concatenate(list(blocks[:4]) + list(blocks[4]) + list(blocks[5:]))

    def reduce_in_order(self, whole):
        size = whole.shape[0] // 8
        return ring_scatter(
            [lax.dynamic_slice_in_dim(whole, self.order[j] * size, size, 0) for j in range(8)]
        )

    def reduce_as_found(self, whole):
        size = whole.shape[0] // 8
        return ring_scatter([whole[j * size : (j + 1) * size] for j in range(8)])

    def pick_qkv(self, w_qkv):
        return pick_columns(w_qkv, self.s)

    def gather_out(self, w_out):
        rows = w_out.shape[0] // 4
        return self.weights_in_order(lax.dynamic_slice_in_dim(w_out, self.s * rows, rows, 0))

    def reduce_out(self, raw_out):
        return self.reduce_in_order(raw_out)

    def bias_of_heads(self, full_bias):
        split = full_bias.reshape(3, 4, 2, 4, HD)
        own = lax.dynamic_index_in_dim(split, self.s, 3, keepdims=False)
        return own.transpose(1, 0, 2, 3).reshape(1, 12 * LANES)

    def bias_of_all(self, own):
        split = own.reshape(4, 3, 2, HD).transpose(1, 0, 2, 3)
        here = (jnp.arange(4) == self.s).astype(F32)[None, None, None, :, None]
        return (split[:, :, :, None, :] * here).reshape(-1)

    def final_qkv(self, share, factor):
        return unpick_columns(seq_gather(share.astype(BF16)), self.s, factor)

    def final_rows(self, share, factor):
        return place_rows(seq_gather(share.astype(BF16)), self.s, factor)

    def final_out(self, share, factor):
        return self.final_rows(share, factor)

    def final_pairs(self, share, factor):
        return place_pairs(seq_gather(share.astype(BF16)), self.s, factor)

    def tokens(self, mine):
        return jnp.concatenate(seq_gather(mine))

    def tokens_sum(self, partial):
        rows = partial.shape[0] // 4
        return seq_scatter([partial[i * rows : (i + 1) * rows] for i in range(4)])

    def by_slot(self, values):
        split = values.reshape((4, values.shape[0] // 4) + values.shape[1:])
        return jnp.take(split, self.slots, axis=0).reshape(values.shape)

    def small_gather(self, mine):
        got = [mine] + [
            lax.ppermute(mine, "fsdp", [(i, (i + k) % 8) for i in range(8)]) for k in range(1, 8)
        ]
        return jnp.take(jnp.stack(got), (self.f - jnp.arange(8)) % 8, axis=0)

    def small_reduce(self, values):
        rolled = jnp.take(values, (self.f + jnp.arange(8)) % 8, axis=0)
        got = [rolled[0]] + [
            lax.ppermute(rolled[k], "fsdp", [(i, (i + k) % 8) for i in range(8)])
            for k in range(1, 8)
        ]
        total = jnp.sum(jnp.take(jnp.stack(got), (self.f - jnp.arange(8)) % 8, axis=0), axis=0)
        total = total + lax.ppermute(total, "seq", CORE)
        return total + lax.ppermute(total, "seq", ROW)


class General:
    def __init__(self, s, f):
        self.s, self.f = s, f
        self.members, self.shards = lax.axis_size("seq"), lax.axis_size("fsdp")
        self.slots = jnp.arange(self.members, dtype=jnp.int32)
        self.pairs = H // self.members // 2

    def weights_in_order(self, block):
        return lax.all_gather(block, "fsdp", axis=0, tiled=True)

    weights_as_found = weights_in_order

    def reduce_in_order(self, whole):
        return lax.psum_scatter(whole, "fsdp", scatter_dimension=0, tiled=True).astype(F32)

    reduce_as_found = reduce_in_order

    def pick_qkv(self, w_qkv):
        split = w_qkv.reshape(w_qkv.shape[0], 3, self.members, self.pairs, LANES)
        own = lax.dynamic_index_in_dim(split, self.s, 2, keepdims=False)
        return own.transpose(0, 2, 1, 3).reshape(w_qkv.shape[0], -1)

    def gather_out(self, w_out):
        rows = w_out.shape[0] * self.shards // self.members
        return lax.dynamic_slice_in_dim(self.weights_in_order(w_out), self.s * rows, rows, 0)

    def reduce_out(self, raw_out):
        rows = raw_out.shape[0]
        whole = jnp.zeros((rows * self.members, raw_out.shape[1]), raw_out.dtype)
        whole = lax.dynamic_update_slice(whole, raw_out, (self.s * rows, 0))
        return self.reduce_in_order(whole)

    def bias_of_heads(self, full_bias):
        split = full_bias.reshape(3, self.members, self.pairs, LANES)
        own = lax.dynamic_index_in_dim(split, self.s, 1, keepdims=False)
        return own.transpose(1, 0, 2).reshape(1, -1)

    def bias_of_all(self, own):
        split = own.reshape(self.pairs, 3, LANES).transpose(1, 0, 2)
        here = (jnp.arange(self.members) == self.s).astype(F32)[None, :, None, None]
        return (split[:, None] * here).reshape(-1)

    def gathered(self, share):
        return lax.all_gather(share.astype(BF16), "seq", axis=0, tiled=False)

    def final_qkv(self, share, factor):
        parts = self.gathered(share).reshape(self.members, -1, self.pairs, 3, LANES)
        return factor * parts.transpose(1, 3, 0, 2, 4).reshape(parts.shape[1], -1).astype(F32)

    def final_rows(self, share, factor):
        return factor * self.gathered(share).reshape(-1, share.shape[1]).astype(F32)

    def final_out(self, share, factor):
        return factor * lax.psum(share.astype(BF16), "seq").astype(F32)

    def final_pairs(self, share, factor):
        parts = self.gathered(share).reshape(self.members, 2, -1, share.shape[1])
        return factor * parts.transpose(0, 2, 1, 3).reshape(-1, 2, share.shape[1]).astype(F32)

    def tokens(self, mine):
        return lax.all_gather(mine, "seq", axis=0, tiled=True)

    def tokens_sum(self, partial):
        return lax.psum_scatter(partial.astype(BF16), "seq", scatter_dimension=0, tiled=True).astype(
            F32
        )

    def by_slot(self, values):
        return values

    def small_gather(self, mine):
        return lax.all_gather(mine, "fsdp", axis=0, tiled=False)

    def small_reduce(self, values):
        total = lax.psum(values, ("seq", "fsdp"))
        return lax.dynamic_index_in_dim(total, self.f, 0, keepdims=False)


def call(kernel, grid, in_specs, out_specs, out_shape, scratch=(), prefetch=0, cost=None):
    return pl.pallas_call(
        kernel,
        grid_spec=pltpu.PrefetchScalarGridSpec(
            num_scalar_prefetch=prefetch,
            grid=grid,
            in_specs=in_specs,
            out_specs=out_specs,
            scratch_shapes=list(scratch),
        ),
        out_shape=out_shape,
        compiler_params=pltpu.CompilerParams(vmem_limit_bytes=VMEM_LIMIT),
        cost_estimate=cost,
    )


def pick_matrix(member, rows, cols, turned):
    lane = lax.broadcasted_iota(jnp.int32, (rows, cols), 0 if turned else 1)
    place = lax.broadcasted_iota(jnp.int32, (rows, cols), 1 if turned else 0)
    source = jnp.where(lane < HD, lane, lane + (256 - HD)) + member * HD
    return jnp.where(place == source, 1.0, 0.0).astype(BF16)


def pick_kernel(s_ref, w_ref, out_ref):
    out_ref[...] = dot_nn(w_ref[...], pick_matrix(s_ref[0], 512, LANES, False)).astype(BF16)


def pick_columns(w_qkv, s):
    rows = w_qkv.shape[0]
    return call(
        pick_kernel,
        (12,),
        [pl.BlockSpec((rows, 512), lambda g, s_ref: (0, (g % 3) * 4 + g // 3))],
        pl.BlockSpec((rows, LANES), lambda g, s_ref: (0, g)),
        jax.ShapeDtypeStruct((rows, 12 * LANES), BF16),
        prefetch=1,
    )(s.reshape(1), w_qkv)


def unpick_kernel(s_ref, factor_ref, p0, p1, p2, p3, out_ref):
    total = None
    for r, part in enumerate((p0, p1, p2, p3)):
        term = dot_nn(part[...], pick_matrix(s_ref[0] ^ r, LANES, 512, True))
        total = term if total is None else total + term
    out_ref[...] = total * factor_ref[0]


def unpick_columns(parts, s, factor):
    rows = parts[0].shape[0]
    return call(
        unpick_kernel,
        (12,),
        [pl.BlockSpec(memory_space=pltpu.SMEM)]
        + [pl.BlockSpec((rows, LANES), lambda g, s_ref: (0, g))] * 4,
        pl.BlockSpec((rows, 512), lambda g, s_ref: (0, (g % 3) * 4 + g // 3)),
        jax.ShapeDtypeStruct((rows, 12 * 512), F32),
        prefetch=1,
    )(s.reshape(1), factor.reshape(1), *parts)


def place_kernel(s_ref, factor_ref, p0, p1, p2, p3, out_ref):
    r = pl.program_id(0)
    for k, part in enumerate((p0, p1, p2, p3)):

        @pl.when(r == k)
        def _(part=part):
            out_ref[...] = part[...].astype(F32) * factor_ref[0]


def place_rows(parts, s, factor):
    rows, cols = parts[0].shape
    return call(
        place_kernel,
        (4,),
        [pl.BlockSpec(memory_space=pltpu.SMEM)]
        + [pl.BlockSpec((rows, cols), lambda r, s_ref: (0, 0))] * 4,
        pl.BlockSpec((rows, cols), lambda r, s_ref: (s_ref[0] ^ r, 0)),
        jax.ShapeDtypeStruct((4 * rows, cols), F32),
        prefetch=1,
    )(s.reshape(1), factor.reshape(1), *parts)


def place_pair_kernel(s_ref, factor_ref, p0, p1, p2, p3, out_ref):
    r = pl.program_id(0)
    rows = out_ref.shape[0]
    for k, part in enumerate((p0, p1, p2, p3)):

        @pl.when(r == k)
        def _(part=part):
            out_ref[:, 0, :] = part[:rows].astype(F32) * factor_ref[0]
            out_ref[:, 1, :] = part[rows:].astype(F32) * factor_ref[0]


def place_pairs(parts, s, factor):
    rows, cols = parts[0].shape
    rows = rows // 2
    return call(
        place_pair_kernel,
        (4,),
        [pl.BlockSpec(memory_space=pltpu.SMEM)]
        + [pl.BlockSpec((2 * rows, cols), lambda r, s_ref: (0, 0))] * 4,
        pl.BlockSpec((rows, 2, cols), lambda r, s_ref: (s_ref[0] ^ r, 0, 0)),
        jax.ShapeDtypeStruct((4 * rows, 2, cols), F32),
        prefetch=1,
    )(s.reshape(1), factor.reshape(1), *parts)


def turn(values, cosine, sine_low, sine_high, sign):
    half = ROT // 2
    moved = (
        pltpu.roll(values, LANES - half, 1) * sine_low + pltpu.roll(values, half, 1) * sine_high
    )
    return values * cosine + moved if sign > 0 else values * cosine - moved


def two_heads(values):
    lane = lax.broadcasted_iota(jnp.int32, values.shape, 1)
    nothing = jnp.zeros_like(values)
    return jnp.concatenate(
        [jnp.where(lane < HD, values, nothing), jnp.where(lane < HD, nothing, values)], axis=0
    )


def one_pair(stacked):
    rows = stacked.shape[0] // 2
    lane = lax.broadcasted_iota(jnp.int32, (rows, LANES), 1)
    return jnp.where(lane < HD, stacked[:rows], stacked[rows:])


def forward_kernel(
    block, slots, slot_ref, first_ref, qkv, bias, cosine, low, high, start, turned, out
):
    scale = HD ** (-0.5)

    def rotate_block(i, unused):
        rows = pl.ds(pl.multiple_of(i * block, block), block)
        tables = (cosine[rows, :], low[rows, :], high[rows, :], 1)
        query = qkv[rows, 0:LANES] + bias[:, 0:LANES]
        key = qkv[rows, LANES : 2 * LANES] + bias[:, LANES : 2 * LANES]
        value = qkv[rows, 2 * LANES : 3 * LANES] + bias[:, 2 * LANES : 3 * LANES]
        turned[rows, 0:LANES] = turn(query, *tables).astype(BF16)
        turned[rows, LANES : 2 * LANES] = turn(key, *tables).astype(BF16)
        turned[rows, 2 * LANES : 3 * LANES] = value.astype(BF16)
        return unused

    lax.fori_loop(0, slots, rotate_block, 0)

    column = lax.broadcasted_iota(jnp.int32, (2 * block, block), 1)
    line = lax.broadcasted_iota(jnp.int32, (2 * block, block), 0) & (block - 1)

    def query_block(i, unused):
        rows = pl.ds(pl.multiple_of(slot_ref[i] * block, block), block)
        query = two_heads((turned[rows, 0:LANES].astype(F32) * scale).astype(BF16))
        first = start[rows, :]
        first = jnp.concatenate([first, first], axis=0)

        def scores(j):
            keys = pl.ds(pl.multiple_of(slot_ref[j] * block, block), block)
            result = dot_nt(query, turned[keys, LANES : 2 * LANES])
            allowed = column >= first - j * block
            return result, allowed, turned[keys, 2 * LANES : 3 * LANES]

        result, allowed, value = scores(i)
        result = jnp.where(allowed & (column <= line), result, MASKED_VALUE)
        peak = jnp.max(result, axis=1, keepdims=True)
        weight = jnp.exp(result - peak)
        total = jnp.sum(weight, axis=1, keepdims=True)
        gathered = dot_nn(weight.astype(BF16), value)

        def key_block(j, carry):
            peak, total, gathered = carry
            result, allowed, value = scores(j)
            result = jnp.where(allowed, result, MASKED_VALUE)
            higher = jnp.maximum(peak, jnp.max(result, axis=1, keepdims=True))
            shrink = jnp.exp(peak - higher)
            weight = jnp.exp(result - higher)
            total = total * shrink + jnp.sum(weight, axis=1, keepdims=True)
            gathered = gathered * shrink + dot_nn(weight.astype(BF16), value)
            return higher, total, gathered

        peak, total, gathered = lax.fori_loop(first_ref[i], i, key_block, (peak, total, gathered))
        out[rows, :] = one_pair(gathered / total).astype(BF16)
        return unused

    lax.fori_loop(0, slots, query_block, 0)


def attention_forward(qkv, bias, tables, start, slot_of, first_slot, block):
    length, width = qkv.shape
    pairs = width // (3 * LANES)
    slots = length // block
    whole = pl.BlockSpec((length, LANES), lambda p, *_: (0, 0))
    return call(
        functools.partial(forward_kernel, block, slots),
        (pairs,),
        [
            pl.BlockSpec((length, 3 * LANES), lambda p, *_: (0, p)),
            pl.BlockSpec((1, 3 * LANES), lambda p, *_: (0, p)),
            whole,
            whole,
            whole,
            pl.BlockSpec((length, 1), lambda p, *_: (0, 0)),
        ],
        [
            pl.BlockSpec((length, 3 * LANES), lambda p, *_: (0, p)),
            pl.BlockSpec((length, LANES), lambda p, *_: (0, p)),
        ],
        [
            jax.ShapeDtypeStruct((length, width), BF16),
            jax.ShapeDtypeStruct((length, width // 3), BF16),
        ],
        prefetch=2,
        cost=pl.CostEstimate(
            flops=length * length * width * 2,
            bytes_accessed=length * width * 8,
            transcendentals=length * length * width // (3 * HD),
        ),
    )(slot_of, first_slot, qkv, bias, *tables, start)


def backward_kernel(
    block,
    slots,
    slot_ref,
    first_ref,
    turned,
    out_grad,
    cosine,
    low,
    high,
    start,
    grads,
    key_sum,
    value_sum,
    weights,
    products,
):
    scale = HD ** (-0.5)
    key_sum[...] = jnp.zeros_like(key_sum)
    value_sum[...] = jnp.zeros_like(value_sum)
    column = lax.broadcasted_iota(jnp.int32, (block, 2 * block), 1) & (block - 1)
    line = lax.broadcasted_iota(jnp.int32, (block, 2 * block), 0)

    def query_block(i, unused):
        begin = pl.multiple_of(slot_ref[i] * block, block)
        rows = pl.ds(begin, block)
        query = two_heads((turned[rows, 0:LANES].astype(F32) * scale).astype(BF16))
        grad = two_heads(out_grad[rows, :])
        first = start[:, pl.ds(begin, block)]
        first = jnp.concatenate([first, first], axis=1)

        def scores(j):
            keys = pl.ds(pl.multiple_of(slot_ref[j] * block, block), block)
            result = dot_nt(turned[keys, LANES : 2 * LANES], query)
            return result, line >= first - j * block

        result, allowed = scores(i)
        result = jnp.where(allowed & (line <= column), result, MASKED_VALUE)
        weights[0] = result
        peak = jnp.max(result, axis=0, keepdims=True)

        def score_block(j, peak):
            result, allowed = scores(j)
            result = jnp.where(allowed, result, MASKED_VALUE)
            weights[i - j] = result
            return jnp.maximum(peak, jnp.max(result, axis=0, keepdims=True))

        peak = lax.fori_loop(first_ref[i], i, score_block, peak)

        def weight_block(j, carry):
            total, cross = carry
            keys = pl.ds(pl.multiple_of(slot_ref[j] * block, block), block)
            weight = jnp.exp(weights[i - j] - peak)
            product = dot_nt(turned[keys, 2 * LANES : 3 * LANES], grad)
            weights[i - j] = weight
            products[i - j] = product
            total = total + jnp.sum(weight, axis=0, keepdims=True)
            cross = cross + jnp.sum(weight * product, axis=0, keepdims=True)
            return total, cross

        zero = jnp.zeros((1, 2 * block), F32)
        total, cross = lax.fori_loop(first_ref[i], i + 1, weight_block, (zero, zero))
        share = 1.0 / total
        cross = cross * share

        def grad_block(j, query_sum):
            keys = pl.ds(pl.multiple_of(slot_ref[j] * block, block), block)
            weight = weights[i - j] * share
            score_grad = (weight * (products[i - j] - cross)).astype(BF16)
            value_sum[keys, :] += dot_nn(weight.astype(BF16), grad)
            key_sum[keys, :] += dot_nn(score_grad, query)
            return query_sum + dot_tn(score_grad, turned[keys, LANES : 2 * LANES])

        query_sum = lax.fori_loop(
            first_ref[i], i + 1, grad_block, jnp.zeros((2 * block, LANES), F32)
        )
        tables = (cosine[rows, :], low[rows, :], high[rows, :], -1)
        grads[rows, 0:LANES] = turn(one_pair(query_sum) * scale, *tables).astype(BF16)
        return unused

    lax.fori_loop(0, slots, query_block, 0)

    def finish(i, unused):
        rows = pl.ds(pl.multiple_of(i * block, block), block)
        tables = (cosine[rows, :], low[rows, :], high[rows, :], -1)
        grads[rows, LANES : 2 * LANES] = turn(key_sum[rows, :], *tables).astype(BF16)
        grads[rows, 2 * LANES : 3 * LANES] = value_sum[rows, :].astype(BF16)
        return unused

    lax.fori_loop(0, slots, finish, 0)


def attention_backward(turned, out_grad, tables, start, slot_of, first_slot, block):
    length, width = turned.shape
    pairs = width // (3 * LANES)
    slots = length // block
    whole = pl.BlockSpec((length, LANES), lambda p, *_: (0, 0))
    return call(
        functools.partial(backward_kernel, block, slots),
        (pairs,),
        [
            pl.BlockSpec((length, 3 * LANES), lambda p, *_: (0, p)),
            pl.BlockSpec((length, LANES), lambda p, *_: (0, p)),
            whole,
            whole,
            whole,
            pl.BlockSpec((1, length), lambda p, *_: (0, 0)),
        ],
        pl.BlockSpec((length, 3 * LANES), lambda p, *_: (0, p)),
        jax.ShapeDtypeStruct((length, width), BF16),
        scratch=[
            pltpu.VMEM((length, LANES), F32),
            pltpu.VMEM((length, LANES), F32),
            pltpu.VMEM((slots, block, 2 * block), F32),
            pltpu.VMEM((slots, block, 2 * block), F32),
        ],
        prefetch=2,
        cost=pl.CostEstimate(
            flops=length * length * width * 5,
            bytes_accessed=length * width * 6,
            transcendentals=length * length * width // (3 * HD),
        ),
    )(slot_of, first_slot, turned, out_grad, *tables, start)


def doc_starts(segment):
    places = jnp.arange(segment.shape[0], dtype=jnp.int32)
    change = jnp.concatenate([jnp.ones((1,), dtype=bool), segment[1:] != segment[:-1]])
    return lax.cummax(jnp.where(change, places, 0), axis=0)


def turn_tables(positions):
    half = ROT // 2
    inverse = 10000.0 ** (-(jnp.arange(half, dtype=F32) * 2.0) / ROT)
    angles = inverse[:, None] * positions.astype(F32)[None, :]
    cosine, sine = jnp.cos(angles).T, jnp.sin(angles).T
    length = positions.shape[0]
    rest = jnp.zeros((length, HD - ROT), F32)
    none = jnp.zeros_like(sine)

    def twice(*pieces):
        return jnp.concatenate(pieces * 2, axis=1)

    return (
        twice(cosine, cosine, rest + 1.0),
        twice(-sine, none, rest),
        twice(none, sine, rest),
    )


def per_device(
    tokens,
    teacher,
    segments,
    valid,
    ln1_gain,
    ln1_bias,
    w_qkv,
    b_qkv,
    w_out,
    ln2_gain,
    ln2_bias,
    w_gate_up,
    w_down,
):
    s = lax.axis_index("seq")
    f = lax.axis_index("fsdp")
    members, shards = lax.axis_size("seq"), lax.axis_size("fsdp")
    net = (Fast if (members, shards) == (4, 8) else General)(s, f)
    rows = tokens.shape[1]
    width = tokens.shape[2]
    length = segments.shape[1]
    units = w_down.shape[0] // members
    vec = ln1_gain.shape[0]
    bias_share = b_qkv.shape[0]

    mine_gate_up = lax.dynamic_slice_in_dim(w_gate_up, s * units, units, 0)
    mine_gate_up = jnp.concatenate([mine_gate_up[:, 0], mine_gate_up[:, 1]])
    mine_down = lax.dynamic_slice_in_dim(w_down, s * units, units, 0)

    small = jnp.concatenate([ln1_gain, ln1_bias, ln2_gain, ln2_bias, b_qkv])
    small = net.small_gather(small.reshape(-1, LANES).astype(F32))
    small = small.reshape(shards, 4 * vec + bias_share)
    gain_one, shift_one, gain_two, shift_two = (
        small[:, i * vec : (i + 1) * vec].reshape(width) for i in range(4)
    )
    own_bias = net.bias_of_heads(small[:, 4 * vec :].reshape(-1))

    tokens_all = net.tokens(tokens[0])
    full_qkv = net.weights_in_order(net.pick_qkv(w_qkv))
    full_out = net.gather_out(w_out)
    full_gate_up = net.weights_as_found(mine_gate_up)
    full_down = net.weights_as_found(mine_down)

    starts = doc_starts(segments[0])
    positions = jnp.arange(length, dtype=jnp.int32) - starts
    first_slot = starts.reshape(members, rows)[:, 0] // rows
    slot_start = net.by_slot(starts)
    tables = turn_tables(net.by_slot(positions))

    normed_all, unused = norm_parts(tokens_all.astype(F32))
    hidden_one = (normed_all * gain_one + shift_one).astype(BF16)
    qkv = dot_nn(hidden_one, full_qkv)
    turned, heads_out = attention_forward(
        qkv, own_bias, tables, slot_start[:, None], net.slots, first_slot, rows
    )
    tokens_in = tokens[0].astype(F32)
    resid = tokens_in + net.tokens_sum(dot_nn(heads_out, full_out))

    normed_two, inv_std_two = norm_parts(resid)
    hidden_two = net.tokens((normed_two * gain_two + shift_two).astype(BF16))
    gate_up = dot_nt(full_gate_up, hidden_two).reshape(shards, 2, units, length)
    gate, up = gate_up[:, 0], gate_up[:, 1]
    hidden = (jax.nn.silu(gate) * up).astype(BF16).reshape(shards * units, length)
    outputs = resid + net.tokens_sum(dot_tn(hidden, full_down))
    counted = valid[0].astype(F32)
    differ = outputs - teacher[0].astype(F32)
    cot = counted[:, None] * differ
    half_sum = 0.5 * jnp.sum(cot * differ)
    count_here = jnp.sum(counted)
    cot_low = net.tokens(cot.astype(BF16))

    raw_down = dot_nn(hidden, cot_low).astype(BF16)
    sum_down = net.reduce_as_found(raw_down)
    hidden_grad = dot_nt(full_down, cot_low).reshape(shards, units, length)
    sigma = jax.nn.sigmoid(gate)
    silu_grad = hidden_grad * up
    gate_grad = silu_grad * sigma + silu_grad * gate * sigma * (1.0 - sigma)
    up_grad = hidden_grad * (gate * sigma)
    grads = jnp.stack([gate_grad, up_grad], axis=1).astype(BF16).reshape(2 * shards * units, length)
    two_grad = net.tokens_sum(dot_tn(grads, full_gate_up))
    raw_gate_up = dot_nn(grads, hidden_two).astype(BF16)
    sum_gate_up = net.reduce_as_found(raw_gate_up)
    resid_grad = cot + norm_back(two_grad, normed_two, inv_std_two, gain_two)
    gain_two_grad = jnp.sum(two_grad * normed_two, axis=0)
    shift_two_grad = jnp.sum(two_grad, axis=0)
    resid_low = net.tokens(resid_grad.astype(BF16))

    out_grad = dot_nt(resid_low, full_out).astype(BF16)
    raw_out = dot_tn(heads_out, resid_low).astype(BF16)
    sum_out = net.reduce_out(raw_out)
    qkv_grad = attention_backward(
        turned, out_grad, tables, slot_start[None, :], net.slots, first_slot, rows
    )
    grad_one = net.tokens_sum(dot_nt(qkv_grad, full_qkv))
    raw_qkv = dot_tn(hidden_one, qkv_grad).astype(BF16)
    sum_qkv = net.reduce_in_order(raw_qkv)
    normed_one, inv_std_one = norm_parts(tokens_in)
    tokens_grad = resid_grad + norm_back(grad_one, normed_one, inv_std_one, gain_one)
    gain_one_grad = jnp.sum(grad_one * normed_one, axis=0)
    shift_one_grad = jnp.sum(grad_one, axis=0)

    bias_grad = net.bias_of_all(jnp.sum(qkv_grad.astype(F32), axis=0)).reshape(shards, -1)

    vectors = jnp.concatenate(
        [
            v.reshape(shards, vec)
            for v in (gain_one_grad, shift_one_grad, gain_two_grad, shift_two_grad)
        ]
        + [
            bias_grad,
            jnp.full((shards, LANES), half_sum),
            jnp.full((shards, LANES), count_here),
        ],
        axis=1,
    )
    vectors = net.small_reduce(vectors.reshape(shards, -1, LANES)).reshape(-1)
    sum_half = vectors[4 * vec + bias_share]
    sum_count = vectors[4 * vec + bias_share + LANES]
    factor = (rows * members * shards) / sum_count
    loss = 2.0 * sum_half / (sum_count * width)
    scaled = factor * vectors

    return (
        outputs.astype(BF16)[None],
        loss,
        (factor * tokens_grad).astype(BF16)[None],
        scaled[:vec],
        scaled[vec : 2 * vec],
        net.final_qkv(sum_qkv, factor),
        scaled[4 * vec : 4 * vec + bias_share],
        net.final_out(sum_out, factor),
        scaled[2 * vec : 3 * vec],
        scaled[3 * vec : 4 * vec],
        net.final_pairs(sum_gate_up, factor),
        net.final_rows(sum_down, factor),
    )


def solution(mesh):
    placed = (
        P("fsdp", "seq", None),
        P("fsdp", "seq", None),
        P("fsdp", None),
        P("fsdp", "seq"),
        P("fsdp"),
        P("fsdp"),
        P("fsdp", None),
        P("fsdp"),
        P("fsdp", None),
        P("fsdp"),
        P("fsdp"),
        P("fsdp", None, None),
        P("fsdp", None),
    )
    return jax.shard_map(
        per_device,
        mesh=mesh,
        in_specs=placed,
        out_specs=(
            P("fsdp", "seq", None),
            P(),
            P("fsdp", "seq", None),
            P("fsdp"),
            P("fsdp"),
            P("fsdp", None),
            P("fsdp"),
            P("fsdp", None),
            P("fsdp"),
            P("fsdp"),
            P("fsdp", None, None),
            P("fsdp", None),
        ),
        check_vma=False,
    )
```

```python
import functools

import jax
import jax.numpy as jnp
import numpy as np
from jax import lax
from jax.experimental import pallas as pl
from jax.experimental.pallas import tpu as pltpu
from jax.sharding import PartitionSpec as P

H = 32
HD = 64
ROT = 16
LANES = 128

EPSILON = 1e-05
MASKED_VALUE = -1e30

F32 = jnp.float32
BF16 = jnp.bfloat16
VMEM_LIMIT = 60 * 1024 * 1024

RING = (0, 2, 4, 6, 7, 5, 3, 1)
NEXT = [(RING[i], RING[(i + 1) % 8]) for i in range(8)]
PREV = [(RING[(i + 1) % 8], RING[i]) for i in range(8)]
ORDER = np.array([[RING[(RING.index(f) + j) % 8] for j in range(8)] for f in range(8)], np.int32)
PLACE = np.array([RING.index(f) for f in range(8)], np.int32)
CORE = [(s, s ^ 1) for s in range(4)]
ROW = [(s, s ^ 2) for s in range(4)]


def dot_nn(a, b):
    return lax.dot_general(a, b, (((1,), (0,)), ((), ())), preferred_element_type=F32)


def dot_nt(a, b):
    return lax.dot_general(a, b, (((1,), (1,)), ((), ())), preferred_element_type=F32)


def dot_tn(a, b):
    return lax.dot_general(a, b, (((0,), (0,)), ((), ())), preferred_element_type=F32)


def norm_parts(values):
    mean_value = jnp.mean(values, axis=-1, keepdims=True)
    centered = values - mean_value
    variance = jnp.mean(centered * centered, axis=-1, keepdims=True)
    inv_std = lax.rsqrt(variance + EPSILON)
    return (centered * inv_std, inv_std)


def norm_back(grad_out, normed, inv_std, gain_vec):
    scaled = grad_out * gain_vec
    mean_scaled = jnp.mean(scaled, axis=-1, keepdims=True)
    mean_cross = jnp.mean(scaled * normed, axis=-1, keepdims=True)
    return inv_std * (scaled - mean_scaled - normed * mean_cross)


def pin(value, *after):
    return lax.optimization_barrier((value,) + after)[0] if after else value


class RingGather:
    def __init__(self, block):
        self.ahead = self.behind = block
        self.half = block.shape[0] // 2
        self.blocks = [block] + [None] * 7
        self.done = 0

    def step(self, *after):
        self.done += 1
        ahead, behind = self.ahead, self.behind
        if after:
            ahead, behind = pin(ahead, *after), pin(behind, *after)
        if self.done == 4:
            ahead, behind = ahead[: self.half], behind[self.half :]
        ahead = lax.ppermute(ahead, "fsdp", NEXT)
        behind = lax.ppermute(behind, "fsdp", PREV)
        if self.done == 4:
            self.blocks[4] = (ahead, behind)
        else:
            self.blocks[8 - self.done], self.blocks[self.done] = ahead, behind
        self.ahead, self.behind = ahead, behind
        return ahead, behind

    def pieces(self):
        for j, block in enumerate(self.blocks):
            if j == 4:
                yield j, 0, block[0]
                yield j, self.half, block[1]
            else:
                yield j, 0, block


class RingScatter:
    def __init__(self, blocks):
        self.blocks = blocks
        self.half = blocks[0].shape[0] // 2
        self.ahead, self.behind = blocks[4][: self.half], blocks[4][self.half :]
        self.done = 0

    def step(self, *after):
        self.done += 1
        half = self.half
        ahead = lax.ppermute(pin(self.ahead, *after), "fsdp", NEXT)
        behind = lax.ppermute(pin(self.behind, *after), "fsdp", PREV)
        got = (ahead, behind)
        ahead, behind = ahead.astype(F32), behind.astype(F32)
        if self.done == 1:
            up, down = self.blocks[3].astype(F32), self.blocks[5].astype(F32)
            ahead = jnp.concatenate([up[:half] + ahead, up[half:]])
            behind = jnp.concatenate([down[:half], down[half:] + behind])
        elif self.done < 4:
            ahead = self.blocks[4 - self.done].astype(F32) + ahead
            behind = self.blocks[4 + self.done].astype(F32) + behind
        else:
            self.total = self.blocks[0].astype(F32) + ahead + behind
            return got
        self.ahead, self.behind = ahead.astype(BF16), behind.astype(BF16)
        return got


def seq_gather(mine):
    over = lax.ppermute(mine, "seq", ROW)
    beside = lax.ppermute(mine, "seq", CORE)
    return [mine, beside, over, lax.ppermute(over, "seq", CORE)]


def seq_scatter(parts):
    corner = lax.ppermute(parts[3].astype(BF16), "seq", CORE)
    beside = lax.ppermute(parts[1].astype(BF16), "seq", CORE)
    far = (parts[2] + corner.astype(F32)).astype(BF16)
    over = lax.ppermute(far, "seq", ROW)
    return parts[0] + beside.astype(F32) + over.astype(F32), far


class Fast:
    def __init__(self, s, f):
        self.s, self.f = s, f
        table = lax.dynamic_index_in_dim(jnp.asarray(ORDER), f, 0, keepdims=False)
        self.order = [table[j] for j in range(8)]
        self.slots = jnp.arange(4, dtype=jnp.int32) ^ s
        self.rings = {}

    def gather(self, **blocks):
        self.rings.update({name: RingGather(block) for name, block in blocks.items()})

    def scatter(self, **wholes):
        for name, whole in wholes.items():
            order = self.order if name in "FSO" else range(8)
            size = whole.shape[0] // 8
            self.rings[name] = RingScatter(
                [lax.dynamic_slice_in_dim(whole, order[j] * size, size, 0) for j in range(8)]
            )

    def hop(self, names, *after):
        got = ()
        for name in names:
            got += self.rings[name].step(*after)
        return got

    def whole(self, name):
        form = {"q": self.in_order, "o": self.shuffled}.get(name, self.as_found)
        return form(self.rings[name])

    def total(self, name):
        return self.rings[name].total

    def in_order(self, ring):
        size, cols = ring.blocks[0].shape
        whole = jnp.zeros((8 * size, cols), BF16)
        for j, first, part in ring.pieces():
            at = self.order[j] * size + first
            whole = lax.dynamic_update_slice(whole, part, (at, 0))
        return whole

    def shuffled(self, ring):
        size, cols = ring.blocks[0].shape
        whole = self.as_found(ring).reshape(8, size, cols)
        places = (jnp.asarray(PLACE) - jnp.asarray(PLACE)[self.f]) % 8
        return jnp.take(whole, places, axis=0).reshape(8 * size, cols)

    def as_found(self, ring):
        return jnp.concatenate([part for unused, unused, part in ring.pieces()])

    def pick_qkv(self, w_qkv):
        return pick_columns(w_qkv, self.s)

    def own_out(self, w_out):
        rows = w_out.shape[0] // 4
        return lax.dynamic_slice_in_dim(w_out, self.s * rows, rows, 0)

    def bias_of_heads(self, full_bias):
        split = full_bias.reshape(3, 4, 2, 4, HD)
        own = lax.dynamic_index_in_dim(split, self.s, 3, keepdims=False)
        return own.transpose(1, 0, 2, 3).reshape(1, 12 * LANES)

    def bias_of_all(self, own):
        split = own.reshape(4, 3, 2, HD).transpose(1, 0, 2, 3)
        here = (jnp.arange(4) == self.s).astype(F32)[None, None, None, :, None]
        return (split[:, :, :, None, :] * here).reshape(-1)

    def final_qkv(self, shares, factor):
        parts = [seq_gather(share.astype(BF16)) for share in shares]
        return unpick_columns(parts, self.s, factor)

    def final_rows(self, share, factor):
        return place_rows(seq_gather(share.astype(BF16)), self.s, factor)

    def final_out(self, share, factor):
        return self.final_rows(share, factor)

    def final_pairs(self, first, second, factor):
        parts = [seq_gather(share.astype(BF16)) for share in (first, second)]
        return place_pairs(parts[0] + parts[1], self.s, factor)

    def tokens(self, mine):
        return jnp.concatenate(seq_gather(mine))

    def tokens_sum(self, partial):
        rows = partial.shape[0] // 4
        return seq_scatter([partial[i * rows : (i + 1) * rows] for i in range(4)])

    def by_slot(self, values):
        split = values.reshape((4, values.shape[0] // 4) + values.shape[1:])
        return jnp.take(split, self.slots, axis=0).reshape(values.shape)

    def small_gather(self, mine):
        got = [mine] + [
            lax.ppermute(mine, "fsdp", [(i, i ^ k) for i in range(8)]) for k in range(1, 8)
        ]
        return jnp.take(jnp.stack(got), self.f ^ jnp.arange(8), axis=0)

    def small_reduce(self, values):
        total = jnp.take(values, self.f ^ jnp.arange(8), axis=0)
        for bit in (4, 2, 1):
            other = lax.ppermute(total[bit:], "fsdp", [(i, i ^ bit) for i in range(8)])
            total = total[:bit] + other
        return self.seq_sum(total[0])

    def seq_sum(self, total):
        total = total + lax.ppermute(total, "seq", CORE)
        return total + lax.ppermute(total, "seq", ROW)


class General:
    def __init__(self, s, f):
        self.s, self.f = s, f
        self.members, self.shards = lax.axis_size("seq"), lax.axis_size("fsdp")
        self.slots = jnp.arange(self.members, dtype=jnp.int32)
        self.pairs = H // self.members // 2
        self.wholes, self.totals = {}, {}

    def gather(self, **blocks):
        for name, block in blocks.items():
            self.wholes[name] = lax.all_gather(block, "fsdp", axis=0, tiled=True)

    def scatter(self, **wholes):
        for name, whole in wholes.items():
            if name == "O":
                rows = whole.shape[0]
                every = jnp.zeros((rows * self.members, whole.shape[1]), whole.dtype)
                whole = lax.dynamic_update_slice(every, whole, (self.s * rows, 0))
            total = lax.psum_scatter(whole, "fsdp", scatter_dimension=0, tiled=True)
            self.totals[name] = total.astype(F32)

    def hop(self, names, *after):
        return ()

    def whole(self, name):
        if name != "o":
            return self.wholes[name]
        rows = self.wholes[name].shape[0] // self.members
        return lax.dynamic_slice_in_dim(self.wholes[name], self.s * rows, rows, 0)

    def total(self, name):
        return self.totals[name]

    def pick_qkv(self, w_qkv):
        split = w_qkv.reshape(w_qkv.shape[0], 3, self.members, self.pairs, LANES)
        own = lax.dynamic_index_in_dim(split, self.s, 2, keepdims=False)
        return own.transpose(0, 2, 1, 3).reshape(w_qkv.shape[0], -1)

    def own_out(self, w_out):
        return w_out

    def bias_of_heads(self, full_bias):
        split = full_bias.reshape(3, self.members, self.pairs, LANES)
        own = lax.dynamic_index_in_dim(split, self.s, 1, keepdims=False)
        return own.transpose(1, 0, 2).reshape(1, -1)

    def bias_of_all(self, own):
        split = own.reshape(self.pairs, 3, LANES).transpose(1, 0, 2)
        here = (jnp.arange(self.members) == self.s).astype(F32)[None, :, None, None]
        return (split[:, None] * here).reshape(-1)

    def gathered(self, share):
        return lax.all_gather(share.astype(BF16), "seq", axis=0, tiled=False)

    def final_qkv(self, shares, factor):
        share = jnp.concatenate(shares, axis=1)
        parts = self.gathered(share).reshape(self.members, -1, self.pairs, 3, LANES)
        return factor * parts.transpose(1, 3, 0, 2, 4).reshape(parts.shape[1], -1).astype(F32)

    def final_rows(self, share, factor):
        return factor * self.gathered(share).reshape(-1, share.shape[1]).astype(F32)

    def final_out(self, share, factor):
        return factor * lax.psum(share.astype(BF16), "seq").astype(F32)

    def final_pairs(self, first, second, factor):
        parts = jnp.stack([first, second], axis=1)
        parts = lax.all_gather(parts.astype(BF16), "seq", axis=0, tiled=True)
        return factor * parts.astype(F32)

    def tokens(self, mine):
        return lax.all_gather(mine, "seq", axis=0, tiled=True)

    def tokens_sum(self, partial):
        total = lax.psum_scatter(partial.astype(BF16), "seq", scatter_dimension=0, tiled=True)
        return total.astype(F32), total

    def by_slot(self, values):
        return values

    def small_gather(self, mine):
        return lax.all_gather(mine, "fsdp", axis=0, tiled=False)

    def small_reduce(self, values):
        total = lax.psum(values, ("seq", "fsdp"))
        return lax.dynamic_index_in_dim(total, self.f, 0, keepdims=False)

    def seq_sum(self, total):
        return lax.psum(total, "seq")


def call(kernel, grid, in_specs, out_specs, out_shape, scratch=(), prefetch=0, cost=None):
    return pl.pallas_call(
        kernel,
        grid_spec=pltpu.PrefetchScalarGridSpec(
            num_scalar_prefetch=prefetch,
            grid=grid,
            in_specs=in_specs,
            out_specs=out_specs,
            scratch_shapes=list(scratch),
        ),
        out_shape=out_shape,
        compiler_params=pltpu.CompilerParams(vmem_limit_bytes=VMEM_LIMIT),
        cost_estimate=cost,
    )


def pick_kernel(s_ref, w_ref, out_ref):
    s = s_ref[0]
    lane = lax.broadcasted_iota(jnp.int32, (w_ref.shape[0], LANES), 1)
    odd = (s & 1) == 1
    for pair in range(4):
        for part in range(3):
            at = part * 2048 + pair * 512 + (s >> 1) * LANES
            one = w_ref[:, pl.ds(pl.multiple_of(at, LANES), LANES)].astype(F32)
            two = w_ref[:, pl.ds(pl.multiple_of(at + 256, LANES), LANES)].astype(F32)
            one = jnp.where(odd, pltpu.roll(one, HD, 1), one)
            two = jnp.where(odd, two, pltpu.roll(two, HD, 1))
            to = (pair * 3 + part) * LANES
            out_ref[:, to : to + LANES] = jnp.where(lane < HD, one, two).astype(BF16)


def pick_columns(w_qkv, s):
    rows, cols = w_qkv.shape
    step = rows // 4
    return call(
        pick_kernel,
        (4,),
        [pl.BlockSpec((step, cols), lambda g, s_ref: (g, 0))],
        pl.BlockSpec((step, 12 * LANES), lambda g, s_ref: (g, 0)),
        jax.ShapeDtypeStruct((rows, 12 * LANES), BF16),
        prefetch=1,
    )(s.reshape(1), w_qkv)


def unpick_kernel(s_ref, factor_ref, *refs):
    out_ref, ordered = refs[-2:]
    s = s_ref[0]
    factor = factor_ref[0]
    rows = out_ref.shape[0]
    lane = lax.broadcasted_iota(jnp.int32, (rows, LANES), 1)
    for half in range(2):
        for r in range(4):
            ordered[s ^ r] = refs[4 * half + r][...].astype(F32) * factor
        for pair in range(2):
            for part in range(3):
                at = slice((pair * 3 + part) * LANES, (pair * 3 + part + 1) * LANES)
                heads = [ordered[m, :, at] for m in range(4)]
                turned = [pltpu.roll(h, HD, 1) for h in heads]
                to = part * 2048 + (2 * half + pair) * 512
                for m in (0, 2):
                    low = jnp.where(lane < HD, heads[m], turned[m + 1])
                    high = jnp.where(lane < HD, turned[m], heads[m + 1])
                    out_ref[:, to + m * HD : to + m * HD + LANES] = low
                    out_ref[:, to + 256 + m * HD : to + 256 + m * HD + LANES] = high


def unpick_columns(parts, s, factor):
    rows, cols = parts[0][0].shape
    step = rows // 4
    return call(
        unpick_kernel,
        (4,),
        [pl.BlockSpec(memory_space=pltpu.SMEM)]
        + [pl.BlockSpec((step, cols), lambda g, s_ref: (g, 0))] * 8,
        pl.BlockSpec((step, 8 * cols), lambda g, s_ref: (g, 0)),
        jax.ShapeDtypeStruct((rows, 8 * cols), F32),
        scratch=[pltpu.VMEM((4, step, cols), F32)],
        prefetch=1,
    )(s.reshape(1), factor.reshape(1), *parts[0], *parts[1])


def place_kernel(s_ref, factor_ref, p0, p1, p2, p3, out_ref):
    r = pl.program_id(0)
    for k, part in enumerate((p0, p1, p2, p3)):

        @pl.when(r == k)
        def _(part=part):
            out_ref[...] = part[...].astype(F32) * factor_ref[0]


def place_rows(parts, s, factor):
    rows, cols = parts[0].shape
    return call(
        place_kernel,
        (4,),
        [pl.BlockSpec(memory_space=pltpu.SMEM)]
        + [pl.BlockSpec((rows, cols), lambda r, s_ref: (0, 0))] * 4,
        pl.BlockSpec((rows, cols), lambda r, s_ref: (s_ref[0] ^ r, 0)),
        jax.ShapeDtypeStruct((4 * rows, cols), F32),
        prefetch=1,
    )(s.reshape(1), factor.reshape(1), *parts)


def place_pair_kernel(s_ref, factor_ref, *refs):
    out_ref = refs[8]
    r = pl.program_id(0)
    for k in range(4):

        @pl.when(r == k)
        def _(k=k):
            out_ref[:, 0, :] = refs[k][...].astype(F32) * factor_ref[0]
            out_ref[:, 1, :] = refs[4 + k][...].astype(F32) * factor_ref[0]


def place_pairs(parts, s, factor):
    rows, cols = parts[0].shape
    return call(
        place_pair_kernel,
        (4,),
        [pl.BlockSpec(memory_space=pltpu.SMEM)]
        + [pl.BlockSpec((rows, cols), lambda r, s_ref: (0, 0))] * 8,
        pl.BlockSpec((rows, 2, cols), lambda r, s_ref: (s_ref[0] ^ r, 0, 0)),
        jax.ShapeDtypeStruct((4 * rows, 2, cols), F32),
        prefetch=1,
    )(s.reshape(1), factor.reshape(1), *parts)


def turn(values, cosine, sine_low, sine_high, sign):
    half = ROT // 2
    moved = (
        pltpu.roll(values, LANES - half, 1) * sine_low + pltpu.roll(values, half, 1) * sine_high
    )
    return values * cosine + moved if sign > 0 else values * cosine - moved


def two_heads(values):
    lane = lax.broadcasted_iota(jnp.int32, values.shape, 1)
    nothing = jnp.zeros_like(values)
    return jnp.concatenate(
        [jnp.where(lane < HD, values, nothing), jnp.where(lane < HD, nothing, values)], axis=0
    )


def one_pair(stacked):
    rows = stacked.shape[0] // 2
    lane = lax.broadcasted_iota(jnp.int32, (rows, LANES), 1)
    return jnp.where(lane < HD, stacked[:rows], stacked[rows:])


def forward_kernel(
    block, slots, slot_ref, first_ref, qkv, bias, cosine, low, high, start, turned, out
):
    scale = HD ** (-0.5)

    def rotate_block(i, unused):
        rows = pl.ds(pl.multiple_of(i * block, block), block)
        tables = (cosine[rows, :], low[rows, :], high[rows, :], 1)
        query = qkv[rows, 0:LANES] + bias[:, 0:LANES]
        key = qkv[rows, LANES : 2 * LANES] + bias[:, LANES : 2 * LANES]
        value = qkv[rows, 2 * LANES : 3 * LANES] + bias[:, 2 * LANES : 3 * LANES]
        turned[rows, 0:LANES] = turn(query, *tables).astype(BF16)
        turned[rows, LANES : 2 * LANES] = turn(key, *tables).astype(BF16)
        turned[rows, 2 * LANES : 3 * LANES] = value.astype(BF16)
        return unused

    lax.fori_loop(0, slots, rotate_block, 0)

    column = lax.broadcasted_iota(jnp.int32, (2 * block, block), 1)
    line = lax.broadcasted_iota(jnp.int32, (2 * block, block), 0) & (block - 1)

    def query_block(i, unused):
        rows = pl.ds(pl.multiple_of(slot_ref[i] * block, block), block)
        query = two_heads((turned[rows, 0:LANES].astype(F32) * scale).astype(BF16))
        first = start[rows, :]
        first = jnp.concatenate([first, first], axis=0)

        def scores(j):
            keys = pl.ds(pl.multiple_of(slot_ref[j] * block, block), block)
            result = dot_nt(query, turned[keys, LANES : 2 * LANES])
            allowed = column >= first - j * block
            return result, allowed, turned[keys, 2 * LANES : 3 * LANES]

        result, allowed, value = scores(i)
        result = jnp.where(allowed & (column <= line), result, MASKED_VALUE)
        peak = jnp.max(result, axis=1, keepdims=True)
        weight = jnp.exp(result - peak)
        total = jnp.sum(weight, axis=1, keepdims=True)
        gathered = dot_nn(weight.astype(BF16), value)

        def key_block(j, carry):
            peak, total, gathered = carry
            result, allowed, value = scores(j)
            result = jnp.where(allowed, result, MASKED_VALUE)
            higher = jnp.maximum(peak, jnp.max(result, axis=1, keepdims=True))
            shrink = jnp.exp(peak - higher)
            weight = jnp.exp(result - higher)
            total = total * shrink + jnp.sum(weight, axis=1, keepdims=True)
            gathered = gathered * shrink + dot_nn(weight.astype(BF16), value)
            return higher, total, gathered

        peak, total, gathered = lax.fori_loop(first_ref[i], i, key_block, (peak, total, gathered))
        out[rows, :] = one_pair(gathered / total).astype(BF16)
        return unused

    lax.fori_loop(0, slots, query_block, 0)


def attention_forward(qkv, bias, tables, start, slot_of, first_slot, *, block, skip, pairs):
    length = qkv.shape[0]
    width = pairs * 3 * LANES
    slots = length // block
    whole = pl.BlockSpec((length, LANES), lambda p, *_: (0, 0))
    return call(
        functools.partial(forward_kernel, block, slots),
        (pairs,),
        [
            pl.BlockSpec((length, 3 * LANES), lambda p, *_: (0, p + skip)),
            pl.BlockSpec((1, 3 * LANES), lambda p, *_: (0, p + skip)),
            whole,
            whole,
            whole,
            pl.BlockSpec((length, 1), lambda p, *_: (0, 0)),
        ],
        [
            pl.BlockSpec((length, 3 * LANES), lambda p, *_: (0, p)),
            pl.BlockSpec((length, LANES), lambda p, *_: (0, p)),
        ],
        [
            jax.ShapeDtypeStruct((length, width), BF16),
            jax.ShapeDtypeStruct((length, width // 3), BF16),
        ],
        prefetch=2,
        cost=pl.CostEstimate(
            flops=length * length * width * 2,
            bytes_accessed=length * width * 8,
            transcendentals=length * length * width // (3 * HD),
        ),
    )(slot_of, first_slot, qkv, bias, *tables, start)


def backward_kernel(
    block,
    slots,
    slot_ref,
    first_ref,
    turned,
    out_grad,
    cosine,
    low,
    high,
    start,
    grads,
    key_sum,
    value_sum,
    weights,
    products,
):
    scale = HD ** (-0.5)
    key_sum[...] = jnp.zeros_like(key_sum)
    value_sum[...] = jnp.zeros_like(value_sum)
    column = lax.broadcasted_iota(jnp.int32, (block, 2 * block), 1) & (block - 1)
    line = lax.broadcasted_iota(jnp.int32, (block, 2 * block), 0)

    def query_block(i, unused):
        begin = pl.multiple_of(slot_ref[i] * block, block)
        rows = pl.ds(begin, block)
        query = two_heads((turned[rows, 0:LANES].astype(F32) * scale).astype(BF16))
        grad = two_heads(out_grad[rows, :])
        first = start[:, pl.ds(begin, block)]
        first = jnp.concatenate([first, first], axis=1)

        def scores(j):
            keys = pl.ds(pl.multiple_of(slot_ref[j] * block, block), block)
            result = dot_nt(turned[keys, LANES : 2 * LANES], query)
            return result, line >= first - j * block

        result, allowed = scores(i)
        result = jnp.where(allowed & (line <= column), result, MASKED_VALUE)
        weights[0] = result
        peak = jnp.max(result, axis=0, keepdims=True)

        def score_block(j, peak):
            result, allowed = scores(j)
            result = jnp.where(allowed, result, MASKED_VALUE)
            weights[i - j] = result
            return jnp.maximum(peak, jnp.max(result, axis=0, keepdims=True))

        peak = lax.fori_loop(first_ref[i], i, score_block, peak)

        def weight_block(j, carry):
            total, cross = carry
            keys = pl.ds(pl.multiple_of(slot_ref[j] * block, block), block)
            weight = jnp.exp(weights[i - j] - peak)
            product = dot_nt(turned[keys, 2 * LANES : 3 * LANES], grad)
            weights[i - j] = weight
            products[i - j] = product
            total = total + jnp.sum(weight, axis=0, keepdims=True)
            cross = cross + jnp.sum(weight * product, axis=0, keepdims=True)
            return total, cross

        zero = jnp.zeros((1, 2 * block), F32)
        total, cross = lax.fori_loop(first_ref[i], i + 1, weight_block, (zero, zero))
        share = 1.0 / total
        cross = cross * share

        def grad_block(j, query_sum):
            keys = pl.ds(pl.multiple_of(slot_ref[j] * block, block), block)
            weight = weights[i - j] * share
            score_grad = (weight * (products[i - j] - cross)).astype(BF16)
            value_sum[keys, :] += dot_nn(weight.astype(BF16), grad)
            key_sum[keys, :] += dot_nn(score_grad, query)
            return query_sum + dot_tn(score_grad, turned[keys, LANES : 2 * LANES])

        query_sum = lax.fori_loop(
            first_ref[i], i + 1, grad_block, jnp.zeros((2 * block, LANES), F32)
        )
        tables = (cosine[rows, :], low[rows, :], high[rows, :], -1)
        grads[rows, 0:LANES] = turn(one_pair(query_sum) * scale, *tables).astype(BF16)
        return unused

    lax.fori_loop(0, slots, query_block, 0)

    def finish(i, unused):
        rows = pl.ds(pl.multiple_of(i * block, block), block)
        tables = (cosine[rows, :], low[rows, :], high[rows, :], -1)
        grads[rows, LANES : 2 * LANES] = turn(key_sum[rows, :], *tables).astype(BF16)
        grads[rows, 2 * LANES : 3 * LANES] = value_sum[rows, :].astype(BF16)
        return unused

    lax.fori_loop(0, slots, finish, 0)


def attention_backward(turned, out_grad, tables, start, slot_of, first_slot, block, skip):
    length, width = turned.shape
    pairs = width // (3 * LANES)
    slots = length // block
    whole = pl.BlockSpec((length, LANES), lambda p, *_: (0, 0))
    return call(
        functools.partial(backward_kernel, block, slots),
        (pairs,),
        [
            pl.BlockSpec((length, 3 * LANES), lambda p, *_: (0, p)),
            pl.BlockSpec((length, LANES), lambda p, *_: (0, p + skip)),
            whole,
            whole,
            whole,
            pl.BlockSpec((1, length), lambda p, *_: (0, 0)),
        ],
        pl.BlockSpec((length, 3 * LANES), lambda p, *_: (0, p)),
        jax.ShapeDtypeStruct((length, width), BF16),
        scratch=[
            pltpu.VMEM((length, LANES), F32),
            pltpu.VMEM((length, LANES), F32),
            pltpu.VMEM((slots, block, 2 * block), F32),
            pltpu.VMEM((slots, block, 2 * block), F32),
        ],
        prefetch=2,
        cost=pl.CostEstimate(
            flops=length * length * width * 5,
            bytes_accessed=length * width * 6,
            transcendentals=length * length * width // (3 * HD),
        ),
    )(slot_of, first_slot, turned, out_grad, *tables, start)


def turn_tables(positions):
    half = ROT // 2
    lane = jnp.arange(LANES, dtype=jnp.int32) % HD
    inverse = 10000.0 ** (-((lane % half).astype(F32) * 2.0) / ROT)
    angles = positions.astype(F32)[:, None] * jnp.where(lane < ROT, inverse, 0.0)[None, :]
    cosine, sine = jnp.cos(angles), jnp.sin(angles)
    lane = lane[None, :]
    return (
        cosine,
        jnp.where(lane < half, -sine, 0.0),
        jnp.where((lane >= half) & (lane < ROT), sine, 0.0),
    )


def per_device(
    tokens,
    teacher,
    segments,
    valid,
    ln1_gain,
    ln1_bias,
    w_qkv,
    b_qkv,
    w_out,
    ln2_gain,
    ln2_bias,
    w_gate_up,
    w_down,
):
    s = lax.axis_index("seq")
    f = lax.axis_index("fsdp")
    members, shards = lax.axis_size("seq"), lax.axis_size("fsdp")
    net = (Fast if (members, shards) == (4, 8) else General)(s, f)
    rows = tokens.shape[1]
    width = tokens.shape[2]
    length = segments.shape[1]
    units = w_down.shape[0] // members
    vec = ln1_gain.shape[0]
    bias_share = b_qkv.shape[0]
    pairs = H // members // 2

    tokens_all = net.tokens(tokens[0])

    mine_gate_up = lax.dynamic_slice_in_dim(w_gate_up, s * units, units, 0)
    net.gather(
        q=net.pick_qkv(w_qkv),
        o=net.own_out(w_out),
        g=mine_gate_up[:, 0],
        u=mine_gate_up[:, 1],
        d=lax.dynamic_slice_in_dim(w_down, s * units, units, 0),
    )
    done = net.hop("qo")

    segment = pin(segments, *done)[0]
    slot_segment = net.by_slot(segment)
    slot_start = jnp.sum((segment[None, :] < slot_segment[:, None]).astype(jnp.int32), axis=1)
    slot_place = net.by_slot(jnp.arange(length, dtype=jnp.int32))
    block_first = segment.reshape(members, rows)[:, 0]
    first_slot = (
        jnp.sum((segment[None, :] < block_first[:, None]).astype(jnp.int32), axis=1) // rows
    )
    tables = turn_tables(slot_place - slot_start)
    done = net.hop("qo") + tables + (slot_start, first_slot)

    counted = pin(valid, *done)[0].astype(F32)
    small = [pin(v, *done) for v in (ln1_gain, ln1_bias, ln2_gain, ln2_bias, b_qkv)]
    small = jnp.concatenate(small).astype(F32)
    small = jnp.concatenate([small, jnp.full((LANES,), jnp.sum(counted))])
    small = net.small_gather(small.reshape(-1, LANES)).reshape(shards, -1)
    gain_one, shift_one, gain_two, shift_two = (
        small[:, i * vec : (i + 1) * vec].reshape(width) for i in range(4)
    )
    own_bias = net.bias_of_heads(small[:, 4 * vec : 4 * vec + bias_share].reshape(-1))
    sum_count = net.seq_sum(jnp.sum(small[:, -LANES:], axis=0))[0]
    factor = (rows * members * shards) / sum_count
    done = net.hop("qo")

    tokens_all = pin(tokens_all, own_bias, *done)
    normed_all, unused = norm_parts(tokens_all.astype(F32))
    hidden_one = (normed_all * gain_one + shift_one).astype(BF16)
    net.hop("qo")
    done = net.hop("g", *done)
    qkv = dot_nn(hidden_one, pin(net.whole("q"), *done))
    half_pairs = pairs // 2
    forward = functools.partial(
        attention_forward,
        qkv,
        own_bias,
        tables,
        slot_start[:, None],
        net.slots,
        block=rows,
        pairs=half_pairs,
    )
    turned_one, heads_one = forward(first_slot, skip=0)
    done = net.hop("gu", *done)
    turned_two, heads_two = forward(pin(first_slot, heads_one, *done), skip=half_pairs)
    heads_out = jnp.concatenate([heads_one, heads_two], axis=1)
    tokens_in = tokens[0].astype(F32)
    done = net.hop("gu", heads_one)
    partial = dot_nn(pin(heads_out, *done), net.whole("o"))
    attended = net.tokens_sum(partial)[0]
    done = net.hop("gu", heads_two)
    resid = tokens_in + pin(attended, *done)

    normed_two, inv_std_two = norm_parts(resid)
    mine_two = (normed_two * gain_two + shift_two).astype(BF16)
    hidden_two = net.tokens(mine_two)
    done = net.hop("u", mine_two) + net.hop("d", mine_two)
    full_gate = net.whole("g")
    gate = dot_nt(full_gate, pin(hidden_two, *done))
    done = net.hop("d")
    full_up = net.whole("u")
    up = dot_nt(pin(full_up, gate, *done), hidden_two)
    hidden = (jax.nn.silu(gate) * up).astype(BF16)
    done = net.hop("d", gate)
    hidden = pin(hidden, *done)
    net.hop("d", hidden)
    full_down = net.whole("d")
    outputs = resid + net.tokens_sum(dot_tn(hidden, full_down))[0]
    differ = outputs - teacher[0].astype(F32)
    cot = counted[:, None] * differ
    half_sum = 0.5 * jnp.sum(cot * differ)
    cot_low = net.tokens(cot.astype(BF16))

    raw_down = dot_nn(hidden, cot_low).astype(BF16)
    net.scatter(D=raw_down)
    done = net.hop("D")
    hidden_grad = dot_nt(pin(full_down, raw_down), cot_low)
    sigma = jax.nn.sigmoid(gate)
    silu_grad = hidden_grad * up
    gate_grad = (silu_grad * sigma + silu_grad * gate * sigma * (1.0 - sigma)).astype(BF16)
    up_grad = (hidden_grad * (gate * sigma)).astype(BF16)

    raw_gate = dot_nn(gate_grad, pin(hidden_two, *done)).astype(BF16)
    done = net.hop("D", gate_grad)

    net.scatter(G=pin(raw_gate, *done))
    partial = dot_tn(gate_grad, pin(full_gate, raw_gate, *done)) + dot_tn(up_grad, full_up)
    done = net.hop("DG", raw_gate)

    two_grad, far = net.tokens_sum(pin(partial, *done))
    raw_up = dot_nn(up_grad, pin(hidden_two, far)).astype(BF16)
    done = net.hop("DG", partial)

    two_grad = pin(two_grad, raw_up, *done)
    resid_grad = cot + norm_back(two_grad, normed_two, inv_std_two, gain_two)
    gain_two_grad = jnp.sum(two_grad * normed_two, axis=0)
    shift_two_grad = jnp.sum(two_grad, axis=0)
    mine_low = resid_grad.astype(BF16)
    resid_low = net.tokens(mine_low)
    net.scatter(U=pin(raw_up, *done))
    done = net.hop("GU", raw_up)

    full_out, full_qkv = net.whole("o"), net.whole("q")
    out_grad = dot_nt(pin(resid_low, *done), full_out).astype(BF16)
    backward = functools.partial(
        attention_backward,
        tables=tables,
        start=slot_start[None, :],
        slot_of=net.slots,
        block=rows,
    )
    grad_first = backward(turned_one, out_grad, first_slot=first_slot, skip=0)
    raw_first = dot_tn(hidden_one, grad_first).astype(BF16)
    done = net.hop("GU", resid_low)

    net.scatter(F=pin(raw_first, *done))
    here = pin(first_slot, raw_first, *done)
    grad_second = backward(turned_two, out_grad, first_slot=here, skip=half_pairs)
    done = net.hop("UF", raw_first)

    qkv_grad = pin(jnp.concatenate([grad_first, grad_second], axis=1), *done)
    partial = dot_nt(qkv_grad, full_qkv)
    grad_one, far = net.tokens_sum(partial)
    raw_second = dot_tn(hidden_one, pin(grad_second, partial)).astype(BF16)
    raw_out = dot_tn(heads_out, pin(resid_low, raw_second)).astype(BF16)
    grad_w_down = net.final_rows(net.total("D"), factor)
    done = net.hop("UF", grad_second)

    grad_w_gate_up = net.final_pairs(net.total("G"), net.total("U"), factor)
    net.scatter(S=pin(raw_second, far, *done), O=pin(raw_out, far, *done))
    done = net.hop("FSO", raw_out)
    grad_one = pin(grad_one, raw_out, *done)
    normed_one, inv_std_one = norm_parts(tokens_in)
    tokens_grad = resid_grad + norm_back(grad_one, normed_one, inv_std_one, gain_one)
    gain_one_grad = jnp.sum(grad_one * normed_one, axis=0)
    shift_one_grad = jnp.sum(grad_one, axis=0)
    bias_grad = net.bias_of_all(jnp.sum(qkv_grad.astype(F32), axis=0)).reshape(shards, -1)
    vectors = jnp.concatenate(
        [
            v.reshape(shards, vec)
            for v in (gain_one_grad, shift_one_grad, gain_two_grad, shift_two_grad)
        ]
        + [bias_grad, jnp.full((shards, LANES), half_sum)],
        axis=1,
    ).reshape(shards, -1, LANES)
    done = net.hop("FSO")

    vectors = net.small_reduce(pin(vectors, *done)).reshape(-1)
    loss = 2.0 * vectors[4 * vec + bias_share] / (sum_count * width)
    scaled = factor * vectors
    done = net.hop("SO", scaled, grad_w_down)
    net.hop("SO", grad_w_gate_up)

    return (
        outputs.astype(BF16)[None],
        loss,
        (factor * tokens_grad).astype(BF16)[None],
        scaled[:vec],
        scaled[vec : 2 * vec],
        net.final_qkv([net.total("F"), net.total("S")], factor),
        scaled[4 * vec : 4 * vec + bias_share],
        net.final_out(net.total("O"), factor),
        scaled[2 * vec : 3 * vec],
        scaled[3 * vec : 4 * vec],
        grad_w_gate_up,
        grad_w_down,
    )


def solution(mesh):
    placed = (
        P("fsdp", "seq", None),
        P("fsdp", "seq", None),
        P("fsdp", None),
        P("fsdp", "seq"),
        P("fsdp"),
        P("fsdp"),
        P("fsdp", None),
        P("fsdp"),
        P("fsdp", None),
        P("fsdp"),
        P("fsdp"),
        P("fsdp", None, None),
        P("fsdp", None),
    )
    return jax.shard_map(
        per_device,
        mesh=mesh,
        in_specs=placed,
        out_specs=(
            P("fsdp", "seq", None),
            P(),
            P("fsdp", "seq", None),
            P("fsdp"),
            P("fsdp"),
            P("fsdp", None),
            P("fsdp"),
            P("fsdp", None),
            P("fsdp"),
            P("fsdp"),
            P("fsdp", None, None),
            P("fsdp", None),
        ),
        check_vma=False,
    )
```

```python
import functools

import jax
import jax.numpy as jnp
import numpy as np
from jax import lax
from jax.experimental import pallas as pl
from jax.experimental.pallas import tpu as pltpu
from jax.sharding import PartitionSpec as P

H = 32
HD = 64
ROT = 16
LANES = 128

EPSILON = 1e-05
MASKED_VALUE = -1e30

F32 = jnp.float32
BF16 = jnp.bfloat16
VMEM_LIMIT = 60 * 1024 * 1024

RING = (0, 2, 4, 6, 7, 5, 3, 1)
NEXT = [(RING[i], RING[(i + 1) % 8]) for i in range(8)]
PREV = [(RING[(i + 1) % 8], RING[i]) for i in range(8)]
ORDER = np.array([[RING[(RING.index(f) + j) % 8] for j in range(8)] for f in range(8)], np.int32)
PLACE = np.array([RING.index(f) for f in range(8)], np.int32)
CORE = [(s, s ^ 1) for s in range(4)]
ROW = [(s, s ^ 2) for s in range(4)]


def dot_nn(a, b):
    return lax.dot_general(a, b, (((1,), (0,)), ((), ())), preferred_element_type=F32)


def dot_nt(a, b):
    return lax.dot_general(a, b, (((1,), (1,)), ((), ())), preferred_element_type=F32)


def dot_tn(a, b):
    return lax.dot_general(a, b, (((0,), (0,)), ((), ())), preferred_element_type=F32)


def norm_parts(values):
    mean_value = jnp.mean(values, axis=-1, keepdims=True)
    centered = values - mean_value
    variance = jnp.mean(centered * centered, axis=-1, keepdims=True)
    inv_std = lax.rsqrt(variance + EPSILON)
    return (centered * inv_std, inv_std)


def norm_back(grad_out, normed, inv_std, gain_vec):
    scaled = grad_out * gain_vec
    mean_scaled = jnp.mean(scaled, axis=-1, keepdims=True)
    mean_cross = jnp.mean(scaled * normed, axis=-1, keepdims=True)
    return inv_std * (scaled - mean_scaled - normed * mean_cross)


def pin(value, *after):
    return lax.optimization_barrier((value,) + after)[0] if after else value


class RingGather:
    def __init__(self, block):
        self.ahead = self.behind = block
        self.half = block.shape[0] // 2
        self.blocks = [block] + [None] * 7
        self.done = 0

    def step(self, *after):
        self.done += 1
        ahead, behind = self.ahead, self.behind
        if after:
            ahead, behind = pin(ahead, *after), pin(behind, *after)
        if self.done == 4:
            ahead, behind = ahead[: self.half], behind[self.half :]
        ahead = lax.ppermute(ahead, "fsdp", NEXT)
        behind = lax.ppermute(behind, "fsdp", PREV)
        if self.done == 4:
            self.blocks[4] = (ahead, behind)
        else:
            self.blocks[8 - self.done], self.blocks[self.done] = ahead, behind
        self.ahead, self.behind = ahead, behind
        return ahead, behind

    def pieces(self):
        for j, block in enumerate(self.blocks):
            if j == 4:
                yield j, 0, block[0]
                yield j, self.half, block[1]
            else:
                yield j, 0, block


class RingScatter:
    def __init__(self, blocks):
        self.blocks = blocks
        self.half = blocks[0].shape[0] // 2
        self.ahead, self.behind = blocks[4][: self.half], blocks[4][self.half :]
        self.done = 0

    def step(self, *after):
        self.done += 1
        half = self.half
        ahead = lax.ppermute(pin(self.ahead, *after), "fsdp", NEXT)
        behind = lax.ppermute(pin(self.behind, *after), "fsdp", PREV)
        got = (ahead, behind)
        ahead, behind = ahead.astype(F32), behind.astype(F32)
        if self.done == 1:
            up, down = self.blocks[3].astype(F32), self.blocks[5].astype(F32)
            ahead = jnp.concatenate([up[:half] + ahead, up[half:]])
            behind = jnp.concatenate([down[:half], down[half:] + behind])
        elif self.done < 4:
            ahead = self.blocks[4 - self.done].astype(F32) + ahead
            behind = self.blocks[4 + self.done].astype(F32) + behind
        else:
            self.total = self.blocks[0].astype(F32) + ahead + behind
            return got
        self.ahead, self.behind = ahead.astype(BF16), behind.astype(BF16)
        return got


def seq_gather(mine):
    over = lax.ppermute(mine, "seq", ROW)
    beside = lax.ppermute(mine, "seq", CORE)
    return [mine, beside, over, lax.ppermute(over, "seq", CORE)]


def seq_scatter(parts):
    corner = lax.ppermute(parts[3].astype(BF16), "seq", CORE)
    beside = lax.ppermute(parts[1].astype(BF16), "seq", CORE)
    far = (parts[2] + corner.astype(F32)).astype(BF16)
    over = lax.ppermute(far, "seq", ROW)
    return parts[0] + beside.astype(F32) + over.astype(F32), far


class Fast:
    def __init__(self, s, f):
        self.s, self.f = s, f
        table = lax.dynamic_index_in_dim(jnp.asarray(ORDER), f, 0, keepdims=False)
        self.order = [table[j] for j in range(8)]
        self.slots = jnp.arange(4, dtype=jnp.int32) ^ s
        self.rings = {}

    def gather(self, **blocks):
        self.rings.update({name: RingGather(block) for name, block in blocks.items()})

    def scatter(self, **wholes):
        for name, whole in wholes.items():
            order = self.order if name in "FS" else range(8)
            size = whole.shape[0] // 8
            self.rings[name] = RingScatter(
                [lax.dynamic_slice_in_dim(whole, order[j] * size, size, 0) for j in range(8)]
            )

    def hop(self, names, *after):
        got = ()
        for name in names:
            got += self.rings[name].step(*after)
        return got

    def gather_out(self, w_out, small, count):
        size = w_out.shape[0] // 4
        self.out_rows = size
        own = lax.dynamic_slice_in_dim(w_out, self.s * size, size, 0)
        pad = jnp.full((w_out.shape[1] - small.shape[0],), count.astype(BF16))
        line = jnp.broadcast_to(jnp.concatenate([small, pad])[None], (16, w_out.shape[1]))
        self.gather(o=jnp.concatenate([own, line]))

    def close_out(self):
        whole = self.as_found(self.rings["o"])
        whole = whole.reshape(8, -1, whole.shape[1])
        places = (jnp.asarray(PLACE) - jnp.asarray(PLACE)[self.f]) % 8
        rows = jnp.take(whole[:, : self.out_rows], places, axis=0)
        small = jnp.take(whole[:, self.out_rows], places, axis=0)
        return rows.reshape(-1, whole.shape[2]), small.astype(F32)

    def whole(self, name):
        return self.in_order(self.rings[name]) if name == "q" else self.as_found(self.rings[name])

    def scatter_first(self, raw_first, raw_out, *after):
        rows, cols = raw_out.shape
        split = raw_out.reshape(8, rows // 8, 4, cols // 4).transpose(0, 2, 1, 3)
        both = jnp.concatenate([raw_first, split.reshape(-1, cols // 4)], axis=1)
        self.first_cols = raw_first.shape[1]
        self.scatter(F=pin(both, *after))

    def total(self, name):
        if name not in "FO":
            return self.rings[name].total
        total = self.rings["F"].total
        if name == "F":
            return total[:, : self.first_cols]
        split = total[:, self.first_cols :].reshape(4, self.out_rows, -1)
        return split.transpose(1, 0, 2).reshape(self.out_rows, -1)

    def in_order(self, ring):
        size, cols = ring.blocks[0].shape
        whole = jnp.zeros((8 * size, cols), BF16)
        for j, first, part in ring.pieces():
            at = self.order[j] * size + first
            whole = lax.dynamic_update_slice(whole, part, (at, 0))
        return whole

    def as_found(self, ring):
        return jnp.concatenate([part for unused, unused, part in ring.pieces()])

    def pick_qkv(self, w_qkv):
        return pick_columns(w_qkv, self.s)

    def bias_of_heads(self, full_bias):
        split = full_bias.reshape(3, 4, 2, 4, HD)
        own = lax.dynamic_index_in_dim(split, self.s, 3, keepdims=False)
        return own.transpose(1, 0, 2, 3).reshape(1, 12 * LANES)

    def bias_of_all(self, own):
        split = own.reshape(4, 3, 2, HD).transpose(1, 0, 2, 3)
        here = (jnp.arange(4) == self.s).astype(F32)[None, None, None, :, None]
        return (split[:, :, :, None, :] * here).reshape(-1)

    def spread(self, name):
        return seq_gather(self.total(name).astype(BF16))

    def final_qkv(self, first, second, factor):
        return unpick_columns([first, second], self.s, factor)

    def final_rows(self, parts, factor):
        return place_rows(parts, self.s, factor)

    final_out = final_rows

    def final_pairs(self, first, second, factor):
        return place_pairs(first + second, self.s, factor)

    def tokens(self, mine):
        return jnp.concatenate(seq_gather(mine))

    def tokens_sum(self, partial):
        rows = partial.shape[0] // 4
        return seq_scatter([partial[i * rows : (i + 1) * rows] for i in range(4)])

    def by_slot(self, values):
        split = values.reshape((4, values.shape[0] // 4) + values.shape[1:])
        return jnp.take(split, self.slots, axis=0).reshape(values.shape)

    def small_reduce(self, values):
        total = jnp.take(values, self.f ^ jnp.arange(8), axis=0)
        for bit in (4, 2, 1):
            other = lax.ppermute(total[bit:], "fsdp", [(i, i ^ bit) for i in range(8)])
            total = total[:bit] + other
        return self.seq_sum(total[0])

    def seq_sum(self, total):
        total = total + lax.ppermute(total, "seq", CORE)
        return total + lax.ppermute(total, "seq", ROW)


class General:
    def __init__(self, s, f):
        self.s, self.f = s, f
        self.members, self.shards = lax.axis_size("seq"), lax.axis_size("fsdp")
        self.slots = jnp.arange(self.members, dtype=jnp.int32)
        self.pairs = H // self.members // 2
        self.wholes, self.totals = {}, {}

    def gather(self, **blocks):
        for name, block in blocks.items():
            self.wholes[name] = lax.all_gather(block, "fsdp", axis=0, tiled=True)

    def scatter(self, **wholes):
        for name, whole in wholes.items():
            if name == "O":
                rows = whole.shape[0]
                every = jnp.zeros((rows * self.members, whole.shape[1]), whole.dtype)
                whole = lax.dynamic_update_slice(every, whole, (self.s * rows, 0))
            total = lax.psum_scatter(whole, "fsdp", scatter_dimension=0, tiled=True)
            self.totals[name] = total.astype(F32)

    def hop(self, names, *after):
        return ()

    def gather_out(self, w_out, small, count):
        self.gather(o=w_out)
        small = jnp.concatenate([small.astype(F32), jnp.full((LANES,), count)])
        self.small = lax.all_gather(small, "fsdp", axis=0, tiled=False)

    def close_out(self):
        rows = self.wholes["o"].shape[0] // self.members
        own = lax.dynamic_slice_in_dim(self.wholes["o"], self.s * rows, rows, 0)
        return own, self.small

    def whole(self, name):
        return self.wholes[name]

    def scatter_first(self, raw_first, raw_out, *after):
        self.scatter(F=raw_first, O=raw_out)

    def total(self, name):
        return self.totals[name]

    def pick_qkv(self, w_qkv):
        split = w_qkv.reshape(w_qkv.shape[0], 3, self.members, self.pairs, LANES)
        own = lax.dynamic_index_in_dim(split, self.s, 2, keepdims=False)
        return own.transpose(0, 2, 1, 3).reshape(w_qkv.shape[0], -1)

    def bias_of_heads(self, full_bias):
        split = full_bias.reshape(3, self.members, self.pairs, LANES)
        own = lax.dynamic_index_in_dim(split, self.s, 1, keepdims=False)
        return own.transpose(1, 0, 2).reshape(1, -1)

    def bias_of_all(self, own):
        split = own.reshape(self.pairs, 3, LANES).transpose(1, 0, 2)
        here = (jnp.arange(self.members) == self.s).astype(F32)[None, :, None, None]
        return (split[:, None] * here).reshape(-1)

    def gathered(self, share):
        return lax.all_gather(share.astype(BF16), "seq", axis=0, tiled=False)

    def spread(self, name):
        return [self.total(name)]

    def final_qkv(self, first, second, factor):
        share = jnp.concatenate(first + second, axis=1)
        parts = self.gathered(share).reshape(self.members, -1, self.pairs, 3, LANES)
        return factor * parts.transpose(1, 3, 0, 2, 4).reshape(parts.shape[1], -1).astype(F32)

    def final_rows(self, parts, factor):
        share = parts[0]
        return factor * self.gathered(share).reshape(-1, share.shape[1]).astype(F32)

    def final_out(self, parts, factor):
        return factor * lax.psum(parts[0].astype(BF16), "seq").astype(F32)

    def final_pairs(self, first, second, factor):
        parts = jnp.stack(first + second, axis=1)
        parts = lax.all_gather(parts.astype(BF16), "seq", axis=0, tiled=True)
        return factor * parts.astype(F32)

    def tokens(self, mine):
        return lax.all_gather(mine, "seq", axis=0, tiled=True)

    def tokens_sum(self, partial):
        total = lax.psum_scatter(partial.astype(BF16), "seq", scatter_dimension=0, tiled=True)
        return total.astype(F32), total

    def by_slot(self, values):
        return values

    def small_reduce(self, values):
        total = lax.psum(values, ("seq", "fsdp"))
        return lax.dynamic_index_in_dim(total, self.f, 0, keepdims=False)

    def seq_sum(self, total):
        return lax.psum(total, "seq")


def call(kernel, grid, in_specs, out_specs, out_shape, scratch=(), prefetch=0, cost=None):
    return pl.pallas_call(
        kernel,
        grid_spec=pltpu.PrefetchScalarGridSpec(
            num_scalar_prefetch=prefetch,
            grid=grid,
            in_specs=in_specs,
            out_specs=out_specs,
            scratch_shapes=list(scratch),
        ),
        out_shape=out_shape,
        compiler_params=pltpu.CompilerParams(vmem_limit_bytes=VMEM_LIMIT),
        cost_estimate=cost,
    )


def pick_kernel(s_ref, w_ref, out_ref):
    s = s_ref[0]
    lane = lax.broadcasted_iota(jnp.int32, (w_ref.shape[0], LANES), 1)
    odd = (s & 1) == 1
    for pair in range(4):
        for part in range(3):
            at = part * 2048 + pair * 512 + (s >> 1) * LANES
            one = w_ref[:, pl.ds(pl.multiple_of(at, LANES), LANES)].astype(F32)
            two = w_ref[:, pl.ds(pl.multiple_of(at + 256, LANES), LANES)].astype(F32)
            one = jnp.where(odd, pltpu.roll(one, HD, 1), one)
            two = jnp.where(odd, two, pltpu.roll(two, HD, 1))
            to = (pair * 3 + part) * LANES
            out_ref[:, to : to + LANES] = jnp.where(lane < HD, one, two).astype(BF16)


def pick_columns(w_qkv, s):
    rows, cols = w_qkv.shape
    step = rows // 4
    return call(
        pick_kernel,
        (4,),
        [pl.BlockSpec((step, cols), lambda g, s_ref: (g, 0))],
        pl.BlockSpec((step, 12 * LANES), lambda g, s_ref: (g, 0)),
        jax.ShapeDtypeStruct((rows, 12 * LANES), BF16),
        prefetch=1,
    )(s.reshape(1), w_qkv)


def unpick_kernel(s_ref, factor_ref, *refs):
    out_ref, ordered = refs[-2:]
    s = s_ref[0]
    factor = factor_ref[0]
    rows = out_ref.shape[0]
    lane = lax.broadcasted_iota(jnp.int32, (rows, LANES), 1)
    for half in range(2):
        for r in range(4):
            ordered[s ^ r] = refs[4 * half + r][...].astype(F32) * factor
        for pair in range(2):
            for part in range(3):
                at = slice((pair * 3 + part) * LANES, (pair * 3 + part + 1) * LANES)
                heads = [ordered[m, :, at] for m in range(4)]
                turned = [pltpu.roll(h, HD, 1) for h in heads]
                to = part * 2048 + (2 * half + pair) * 512
                for m in (0, 2):
                    low = jnp.where(lane < HD, heads[m], turned[m + 1])
                    high = jnp.where(lane < HD, turned[m], heads[m + 1])
                    out_ref[:, to + m * HD : to + m * HD + LANES] = low
                    out_ref[:, to + 256 + m * HD : to + 256 + m * HD + LANES] = high


def unpick_columns(parts, s, factor):
    rows, cols = parts[0][0].shape
    step = rows // 4
    return call(
        unpick_kernel,
        (4,),
        [pl.BlockSpec(memory_space=pltpu.SMEM)]
        + [pl.BlockSpec((step, cols), lambda g, s_ref: (g, 0))] * 8,
        pl.BlockSpec((step, 8 * cols), lambda g, s_ref: (g, 0)),
        jax.ShapeDtypeStruct((rows, 8 * cols), F32),
        scratch=[pltpu.VMEM((4, step, cols), F32)],
        prefetch=1,
    )(s.reshape(1), factor.reshape(1), *parts[0], *parts[1])


def place_kernel(s_ref, factor_ref, p0, p1, p2, p3, out_ref):
    r = pl.program_id(0)
    for k, part in enumerate((p0, p1, p2, p3)):

        @pl.when(r == k)
        def _(part=part):
            out_ref[...] = part[...].astype(F32) * factor_ref[0]


def place_rows(parts, s, factor):
    rows, cols = parts[0].shape
    return call(
        place_kernel,
        (4,),
        [pl.BlockSpec(memory_space=pltpu.SMEM)]
        + [pl.BlockSpec((rows, cols), lambda r, s_ref: (0, 0))] * 4,
        pl.BlockSpec((rows, cols), lambda r, s_ref: (s_ref[0] ^ r, 0)),
        jax.ShapeDtypeStruct((4 * rows, cols), F32),
        prefetch=1,
    )(s.reshape(1), factor.reshape(1), *parts)


def place_pair_kernel(s_ref, factor_ref, *refs):
    out_ref = refs[8]
    r = pl.program_id(0)
    for k in range(4):

        @pl.when(r == k)
        def _(k=k):
            out_ref[:, 0, :] = refs[k][...].astype(F32) * factor_ref[0]
            out_ref[:, 1, :] = refs[4 + k][...].astype(F32) * factor_ref[0]


def place_pairs(parts, s, factor):
    rows, cols = parts[0].shape
    return call(
        place_pair_kernel,
        (4,),
        [pl.BlockSpec(memory_space=pltpu.SMEM)]
        + [pl.BlockSpec((rows, cols), lambda r, s_ref: (0, 0))] * 8,
        pl.BlockSpec((rows, 2, cols), lambda r, s_ref: (s_ref[0] ^ r, 0, 0)),
        jax.ShapeDtypeStruct((4 * rows, 2, cols), F32),
        prefetch=1,
    )(s.reshape(1), factor.reshape(1), *parts)


def turn(values, cosine, sine_low, sine_high, sign):
    half = ROT // 2
    moved = (
        pltpu.roll(values, LANES - half, 1) * sine_low + pltpu.roll(values, half, 1) * sine_high
    )
    return values * cosine + moved if sign > 0 else values * cosine - moved


def two_heads(values):
    lane = lax.broadcasted_iota(jnp.int32, values.shape, 1)
    nothing = jnp.zeros_like(values)
    return jnp.concatenate(
        [jnp.where(lane < HD, values, nothing), jnp.where(lane < HD, nothing, values)], axis=0
    )


def one_pair(stacked):
    rows = stacked.shape[0] // 2
    lane = lax.broadcasted_iota(jnp.int32, (rows, LANES), 1)
    return jnp.where(lane < HD, stacked[:rows], stacked[rows:])


def forward_kernel(
    block, slots, slot_ref, first_ref, qkv, bias, cosine, low, high, start, turned, out
):
    scale = HD ** (-0.5)

    def rotate_block(i, unused):
        rows = pl.ds(pl.multiple_of(i * block, block), block)
        tables = (cosine[rows, :], low[rows, :], high[rows, :], 1)
        query = qkv[rows, 0:LANES] + bias[:, 0:LANES]
        key = qkv[rows, LANES : 2 * LANES] + bias[:, LANES : 2 * LANES]
        value = qkv[rows, 2 * LANES : 3 * LANES] + bias[:, 2 * LANES : 3 * LANES]
        turned[rows, 0:LANES] = turn(query, *tables).astype(BF16)
        turned[rows, LANES : 2 * LANES] = turn(key, *tables).astype(BF16)
        turned[rows, 2 * LANES : 3 * LANES] = value.astype(BF16)
        return unused

    lax.fori_loop(0, slots, rotate_block, 0)

    column = lax.broadcasted_iota(jnp.int32, (2 * block, block), 1)
    line = lax.broadcasted_iota(jnp.int32, (2 * block, block), 0) & (block - 1)

    def query_block(i, unused):
        rows = pl.ds(pl.multiple_of(slot_ref[i] * block, block), block)
        query = two_heads((turned[rows, 0:LANES].astype(F32) * scale).astype(BF16))
        first = start[rows, :]
        first = jnp.concatenate([first, first], axis=0)

        def scores(j):
            keys = pl.ds(pl.multiple_of(slot_ref[j] * block, block), block)
            result = dot_nt(query, turned[keys, LANES : 2 * LANES])
            allowed = column >= first - j * block
            return result, allowed, turned[keys, 2 * LANES : 3 * LANES]

        result, allowed, value = scores(i)
        result = jnp.where(allowed & (column <= line), result, MASKED_VALUE)
        peak = jnp.max(result, axis=1, keepdims=True)
        weight = jnp.exp(result - peak)
        total = jnp.sum(weight, axis=1, keepdims=True)
        gathered = dot_nn(weight.astype(BF16), value)

        def key_block(j, carry):
            peak, total, gathered = carry
            result, allowed, value = scores(j)
            result = jnp.where(allowed, result, MASKED_VALUE)
            higher = jnp.maximum(peak, jnp.max(result, axis=1, keepdims=True))
            shrink = jnp.exp(peak - higher)
            weight = jnp.exp(result - higher)
            total = total * shrink + jnp.sum(weight, axis=1, keepdims=True)
            gathered = gathered * shrink + dot_nn(weight.astype(BF16), value)
            return higher, total, gathered

        peak, total, gathered = lax.fori_loop(first_ref[i], i, key_block, (peak, total, gathered))
        out[rows, :] = one_pair(gathered / total).astype(BF16)
        return unused

    lax.fori_loop(0, slots, query_block, 0)


def attention_forward(qkv, bias, tables, start, slot_of, first_slot, *, block, skip, pairs):
    length = qkv.shape[0]
    width = pairs * 3 * LANES
    slots = length // block
    whole = pl.BlockSpec((length, LANES), lambda p, *_: (0, 0))
    return call(
        functools.partial(forward_kernel, block, slots),
        (pairs,),
        [
            pl.BlockSpec((length, 3 * LANES), lambda p, *_: (0, p + skip)),
            pl.BlockSpec((1, 3 * LANES), lambda p, *_: (0, p + skip)),
            whole,
            whole,
            whole,
            pl.BlockSpec((length, 1), lambda p, *_: (0, 0)),
        ],
        [
            pl.BlockSpec((length, 3 * LANES), lambda p, *_: (0, p)),
            pl.BlockSpec((length, LANES), lambda p, *_: (0, p)),
        ],
        [
            jax.ShapeDtypeStruct((length, width), BF16),
            jax.ShapeDtypeStruct((length, width // 3), BF16),
        ],
        prefetch=2,
        cost=pl.CostEstimate(
            flops=length * length * width * 2,
            bytes_accessed=length * width * 8,
            transcendentals=length * length * width // (3 * HD),
        ),
    )(slot_of, first_slot, qkv, bias, *tables, start)


def backward_kernel(
    block,
    slots,
    slot_ref,
    first_ref,
    turned,
    out_grad,
    cosine,
    low,
    high,
    start,
    grads,
    key_sum,
    value_sum,
    weights,
    products,
):
    scale = HD ** (-0.5)
    key_sum[...] = jnp.zeros_like(key_sum)
    value_sum[...] = jnp.zeros_like(value_sum)
    column = lax.broadcasted_iota(jnp.int32, (block, 2 * block), 1) & (block - 1)
    line = lax.broadcasted_iota(jnp.int32, (block, 2 * block), 0)

    def query_block(i, unused):
        begin = pl.multiple_of(slot_ref[i] * block, block)
        rows = pl.ds(begin, block)
        query = two_heads((turned[rows, 0:LANES].astype(F32) * scale).astype(BF16))
        grad = two_heads(out_grad[rows, :])
        first = start[:, pl.ds(begin, block)]
        first = jnp.concatenate([first, first], axis=1)

        def scores(j):
            keys = pl.ds(pl.multiple_of(slot_ref[j] * block, block), block)
            result = dot_nt(turned[keys, LANES : 2 * LANES], query)
            return result, line >= first - j * block

        result, allowed = scores(i)
        result = jnp.where(allowed & (line <= column), result, MASKED_VALUE)
        weights[0] = result
        peak = jnp.max(result, axis=0, keepdims=True)

        def score_block(j, peak):
            result, allowed = scores(j)
            result = jnp.where(allowed, result, MASKED_VALUE)
            weights[i - j] = result
            return jnp.maximum(peak, jnp.max(result, axis=0, keepdims=True))

        peak = lax.fori_loop(first_ref[i], i, score_block, peak)

        def weight_block(j, carry):
            total, cross = carry
            keys = pl.ds(pl.multiple_of(slot_ref[j] * block, block), block)
            weight = jnp.exp(weights[i - j] - peak)
            product = dot_nt(turned[keys, 2 * LANES : 3 * LANES], grad)
            weights[i - j] = weight
            products[i - j] = product
            total = total + jnp.sum(weight, axis=0, keepdims=True)
            cross = cross + jnp.sum(weight * product, axis=0, keepdims=True)
            return total, cross

        zero = jnp.zeros((1, 2 * block), F32)
        total, cross = lax.fori_loop(first_ref[i], i + 1, weight_block, (zero, zero))
        share = 1.0 / total
        cross = cross * share

        def grad_block(j, query_sum):
            keys = pl.ds(pl.multiple_of(slot_ref[j] * block, block), block)
            weight = weights[i - j] * share
            score_grad = (weight * (products[i - j] - cross)).astype(BF16)
            value_sum[keys, :] += dot_nn(weight.astype(BF16), grad)
            key_sum[keys, :] += dot_nn(score_grad, query)
            return query_sum + dot_tn(score_grad, turned[keys, LANES : 2 * LANES])

        query_sum = lax.fori_loop(
            first_ref[i], i + 1, grad_block, jnp.zeros((2 * block, LANES), F32)
        )
        tables = (cosine[rows, :], low[rows, :], high[rows, :], -1)
        grads[rows, 0:LANES] = turn(one_pair(query_sum) * scale, *tables).astype(BF16)
        return unused

    lax.fori_loop(0, slots, query_block, 0)

    def finish(i, unused):
        rows = pl.ds(pl.multiple_of(i * block, block), block)
        tables = (cosine[rows, :], low[rows, :], high[rows, :], -1)
        grads[rows, LANES : 2 * LANES] = turn(key_sum[rows, :], *tables).astype(BF16)
        grads[rows, 2 * LANES : 3 * LANES] = value_sum[rows, :].astype(BF16)
        return unused

    lax.fori_loop(0, slots, finish, 0)


def attention_backward(turned, out_grad, tables, start, slot_of, first_slot, block, skip):
    length, width = turned.shape
    pairs = width // (3 * LANES)
    slots = length // block
    whole = pl.BlockSpec((length, LANES), lambda p, *_: (0, 0))
    return call(
        functools.partial(backward_kernel, block, slots),
        (pairs,),
        [
            pl.BlockSpec((length, 3 * LANES), lambda p, *_: (0, p)),
            pl.BlockSpec((length, LANES), lambda p, *_: (0, p + skip)),
            whole,
            whole,
            whole,
            pl.BlockSpec((1, length), lambda p, *_: (0, 0)),
        ],
        pl.BlockSpec((length, 3 * LANES), lambda p, *_: (0, p)),
        jax.ShapeDtypeStruct((length, width), BF16),
        scratch=[
            pltpu.VMEM((length, LANES), F32),
            pltpu.VMEM((length, LANES), F32),
            pltpu.VMEM((slots, block, 2 * block), F32),
            pltpu.VMEM((slots, block, 2 * block), F32),
        ],
        prefetch=2,
        cost=pl.CostEstimate(
            flops=length * length * width * 5,
            bytes_accessed=length * width * 6,
            transcendentals=length * length * width // (3 * HD),
        ),
    )(slot_of, first_slot, turned, out_grad, *tables, start)


def turn_tables(positions):
    half = ROT // 2
    lane = jnp.arange(LANES, dtype=jnp.int32) % HD
    inverse = 10000.0 ** (-((lane % half).astype(F32) * 2.0) / ROT)
    angles = positions.astype(F32)[:, None] * jnp.where(lane < ROT, inverse, 0.0)[None, :]
    cosine, sine = jnp.cos(angles), jnp.sin(angles)
    lane = lane[None, :]
    return (
        cosine,
        jnp.where(lane < half, -sine, 0.0),
        jnp.where((lane >= half) & (lane < ROT), sine, 0.0),
    )


def per_device(
    tokens,
    teacher,
    segments,
    valid,
    ln1_gain,
    ln1_bias,
    w_qkv,
    b_qkv,
    w_out,
    ln2_gain,
    ln2_bias,
    w_gate_up,
    w_down,
):
    s = lax.axis_index("seq")
    f = lax.axis_index("fsdp")
    members, shards = lax.axis_size("seq"), lax.axis_size("fsdp")
    net = (Fast if (members, shards) == (4, 8) else General)(s, f)
    rows = tokens.shape[1]
    width = tokens.shape[2]
    length = segments.shape[1]
    units = w_down.shape[0] // members
    vec = ln1_gain.shape[0]
    bias_share = b_qkv.shape[0]
    pairs = H // members // 2

    tokens_all = net.tokens(tokens[0])

    mine_gate_up = lax.dynamic_slice_in_dim(w_gate_up, s * units, units, 0)
    counted = valid[0].astype(F32)
    small = jnp.concatenate([ln1_gain, ln1_bias, ln2_gain, ln2_bias, b_qkv])
    net.gather_out(w_out, small, jnp.sum(counted))
    net.gather(
        q=net.pick_qkv(w_qkv),
        g=mine_gate_up[:, 0],
        u=mine_gate_up[:, 1],
        d=lax.dynamic_slice_in_dim(w_down, s * units, units, 0),
    )
    done = net.hop("qo")

    normed_all, unused = norm_parts(pin(tokens_all, *done).astype(F32))
    done = net.hop("q")

    segment = pin(segments, *done)[0]
    slot_segment = net.by_slot(segment)
    slot_start = jnp.sum((segment[None, :] < slot_segment[:, None]).astype(jnp.int32), axis=1)
    slot_place = net.by_slot(jnp.arange(length, dtype=jnp.int32))
    block_first = segment.reshape(members, rows)[:, 0]
    first_slot = (
        jnp.sum((segment[None, :] < block_first[:, None]).astype(jnp.int32), axis=1) // rows
    )
    done = net.hop("q") + net.hop("o", *done)
    tables = turn_tables(slot_place - pin(slot_start, *done))
    net.hop("qo", *done)
    net.hop("o")
    full_out, small = net.close_out()
    gain_one, shift_one, gain_two, shift_two = (
        small[:, i * vec : (i + 1) * vec].reshape(width) for i in range(4)
    )
    own_bias = net.bias_of_heads(small[:, 4 * vec : 4 * vec + bias_share].reshape(-1))
    sum_count = net.seq_sum(jnp.sum(small[:, -LANES:], axis=0))[0]
    factor = (rows * members * shards) / sum_count
    hidden_one = (normed_all * gain_one + shift_one).astype(BF16)
    done = net.hop("g", *done)
    qkv = dot_nn(hidden_one, pin(net.whole("q"), *done, *tables))
    half_pairs = pairs // 2
    forward = functools.partial(
        attention_forward,
        qkv,
        own_bias,
        tables,
        slot_start[:, None],
        net.slots,
        block=rows,
        pairs=half_pairs,
    )
    turned_one, heads_one = forward(pin(first_slot, factor), skip=0)
    done = net.hop("gu", *done)
    turned_two, heads_two = forward(pin(first_slot, heads_one, *done), skip=half_pairs)
    heads_out = jnp.concatenate([heads_one, heads_two], axis=1)
    tokens_in = tokens[0].astype(F32)
    done = net.hop("gu", heads_one)
    partial = dot_nn(pin(heads_out, *done), full_out)
    attended = net.tokens_sum(partial)[0]
    done = net.hop("gu", heads_two)
    resid = tokens_in + pin(attended, *done)

    normed_two, inv_std_two = norm_parts(resid)
    mine_two = (normed_two * gain_two + shift_two).astype(BF16)
    hidden_two = net.tokens(mine_two)
    done = net.hop("u", mine_two) + net.hop("d", mine_two)
    full_gate = net.whole("g")
    gate = dot_nt(full_gate, pin(hidden_two, *done))
    done = net.hop("d")
    full_up = net.whole("u")
    up = dot_nt(pin(full_up, gate, *done), hidden_two)
    hidden = (jax.nn.silu(gate) * up).astype(BF16)
    done = net.hop("d", gate)
    hidden = pin(hidden, *done)
    net.hop("d", hidden)
    full_down = net.whole("d")
    outputs = resid + net.tokens_sum(dot_tn(hidden, full_down))[0]
    differ = outputs - teacher[0].astype(F32)
    cot = counted[:, None] * differ
    half_sum = 0.5 * jnp.sum(cot * differ)
    cot_low = net.tokens(cot.astype(BF16))

    raw_down = dot_nn(hidden, cot_low).astype(BF16)
    net.scatter(D=raw_down)
    done = net.hop("D")
    hidden_grad = dot_nt(pin(full_down, raw_down), cot_low)
    sigma = jax.nn.sigmoid(gate)
    silu_grad = hidden_grad * up
    gate_grad = (silu_grad * sigma + silu_grad * gate * sigma * (1.0 - sigma)).astype(BF16)
    up_grad = (hidden_grad * (gate * sigma)).astype(BF16)

    raw_gate = dot_nn(gate_grad, pin(hidden_two, *done)).astype(BF16)
    done = net.hop("D", gate_grad)
    partial = dot_tn(gate_grad, pin(full_gate, raw_gate, *done))

    net.scatter(G=pin(raw_gate, *done))
    done = net.hop("G")
    partial = partial + dot_tn(up_grad, pin(full_up, partial, *done))
    two_grad, far = net.tokens_sum(partial)
    done = net.hop("DG", *done)

    raw_up = dot_nn(up_grad, pin(hidden_two, far, *done)).astype(BF16)
    net.scatter(U=raw_up)
    done = net.hop("D", *done)

    two_grad = pin(two_grad, *done)
    resid_grad = cot + norm_back(two_grad, normed_two, inv_std_two, gain_two)
    gain_two_grad = jnp.sum(two_grad * normed_two, axis=0)
    shift_two_grad = jnp.sum(two_grad, axis=0)
    mine_low = resid_grad.astype(BF16)
    resid_low = net.tokens(mine_low)
    done = net.hop("UG", *done)

    full_qkv = net.whole("q")
    out_grad = dot_nt(pin(resid_low, *done), full_out).astype(BF16)
    backward = functools.partial(
        attention_backward,
        tables=tables,
        start=slot_start[None, :],
        slot_of=net.slots,
        block=rows,
    )
    raw_out = dot_tn(heads_out, pin(resid_low, out_grad)).astype(BF16)
    grad_first = backward(turned_one, pin(out_grad, raw_out), first_slot=first_slot, skip=0)
    raw_first = dot_tn(hidden_one, grad_first).astype(BF16)
    done = net.hop("UG", resid_low)

    net.scatter_first(raw_first, raw_out, *done)
    parts_down = net.spread("D")
    here = pin(first_slot, raw_first, *done, *parts_down)
    grad_second = backward(turned_two, out_grad, first_slot=here, skip=half_pairs)
    done = net.hop("FU", raw_first)

    parts_gate = net.spread("G")
    qkv_grad = pin(jnp.concatenate([grad_first, grad_second], axis=1), *done, *parts_gate)
    partial = dot_nt(qkv_grad, full_qkv)
    grad_one, far = net.tokens_sum(partial)
    raw_second = dot_tn(hidden_one, pin(grad_second, partial)).astype(BF16)
    done = net.hop("FU", grad_second)

    net.scatter(S=pin(raw_second, far, *done))
    done = net.hop("SF", raw_second)

    grad_one = pin(grad_one, raw_second, *done)
    normed_one, inv_std_one = norm_parts(tokens_in)
    tokens_grad = resid_grad + norm_back(grad_one, normed_one, inv_std_one, gain_one)
    gain_one_grad = jnp.sum(grad_one * normed_one, axis=0)
    shift_one_grad = jnp.sum(grad_one, axis=0)
    bias_grad = net.bias_of_all(jnp.sum(qkv_grad.astype(F32), axis=0)).reshape(shards, -1)
    vectors = jnp.concatenate(
        [
            v.reshape(shards, vec)
            for v in (gain_one_grad, shift_one_grad, gain_two_grad, shift_two_grad)
        ]
        + [bias_grad, jnp.full((shards, LANES), half_sum)],
        axis=1,
    ).reshape(shards, -1, LANES)
    grad_w_down = net.final_rows(parts_down, factor)
    parts_up = net.spread("U")
    done = net.hop("SF", *done)

    vectors = net.small_reduce(pin(vectors, *done)).reshape(-1)
    loss = 2.0 * vectors[4 * vec + bias_share] / (sum_count * width)
    scaled = factor * vectors
    parts_first, parts_out = net.spread("F"), net.spread("O")
    done = net.hop("S", grad_w_down, *done)
    grad_w_gate_up = net.final_pairs(parts_gate, parts_up, factor)
    grad_w_out = net.final_out(parts_out, factor)
    net.hop("S", scaled, grad_w_gate_up, grad_w_out)

    return (
        outputs.astype(BF16)[None],
        loss,
        (factor * tokens_grad).astype(BF16)[None],
        scaled[:vec],
        scaled[vec : 2 * vec],
        net.final_qkv(parts_first, net.spread("S"), factor),
        scaled[4 * vec : 4 * vec + bias_share],
        grad_w_out,
        scaled[2 * vec : 3 * vec],
        scaled[3 * vec : 4 * vec],
        grad_w_gate_up,
        grad_w_down,
    )


def solution(mesh):
    placed = (
        P("fsdp", "seq", None),
        P("fsdp", "seq", None),
        P("fsdp", None),
        P("fsdp", "seq"),
        P("fsdp"),
        P("fsdp"),
        P("fsdp", None),
        P("fsdp"),
        P("fsdp", None),
        P("fsdp"),
        P("fsdp"),
        P("fsdp", None, None),
        P("fsdp", None),
    )
    return jax.shard_map(
        per_device,
        mesh=mesh,
        in_specs=placed,
        out_specs=(
            P("fsdp", "seq", None),
            P(),
            P("fsdp", "seq", None),
            P("fsdp"),
            P("fsdp"),
            P("fsdp", None),
            P("fsdp"),
            P("fsdp", None),
            P("fsdp"),
            P("fsdp"),
            P("fsdp", None, None),
            P("fsdp", None),
        ),
        check_vma=False,
    )
```

```python
import functools

import jax
import jax.numpy as jnp
import numpy as np
from jax import lax
from jax.experimental import pallas as pl
from jax.experimental.pallas import tpu as pltpu
from jax.sharding import PartitionSpec as P

H = 32
HD = 64
ROT = 16
LANES = 128

EPSILON = 1e-05
MASKED_VALUE = -1e30

F32 = jnp.float32
BF16 = jnp.bfloat16
VMEM_LIMIT = 60 * 1024 * 1024

RING = (0, 2, 4, 6, 7, 5, 3, 1)
NEXT = [(RING[i], RING[(i + 1) % 8]) for i in range(8)]
PREV = [(RING[(i + 1) % 8], RING[i]) for i in range(8)]
ORDER = np.array([[RING[(RING.index(f) + j) % 8] for j in range(8)] for f in range(8)], np.int32)
PLACE = np.array([RING.index(f) for f in range(8)], np.int32)
CORE = [(s, s ^ 1) for s in range(4)]
ROW = [(s, s ^ 2) for s in range(4)]


def dot_nn(a, b):
    return lax.dot_general(a, b, (((1,), (0,)), ((), ())), preferred_element_type=F32)


def dot_nt(a, b):
    return lax.dot_general(a, b, (((1,), (1,)), ((), ())), preferred_element_type=F32)


def dot_tn(a, b):
    return lax.dot_general(a, b, (((0,), (0,)), ((), ())), preferred_element_type=F32)


def norm_parts(values):
    mean_value = jnp.mean(values, axis=-1, keepdims=True)
    centered = values - mean_value
    variance = jnp.mean(centered * centered, axis=-1, keepdims=True)
    inv_std = lax.rsqrt(variance + EPSILON)
    return (centered * inv_std, inv_std)


def norm_back(grad_out, normed, inv_std, gain_vec):
    scaled = grad_out * gain_vec
    mean_scaled = jnp.mean(scaled, axis=-1, keepdims=True)
    mean_cross = jnp.mean(scaled * normed, axis=-1, keepdims=True)
    return inv_std * (scaled - mean_scaled - normed * mean_cross)


def pin(value, *after):
    return lax.optimization_barrier((value,) + after)[0] if after else value


class RingGather:
    def __init__(self, block):
        self.ahead = self.behind = block
        self.half = block.shape[0] // 2
        self.blocks = [block] + [None] * 7
        self.done = 0

    def step(self, *after):
        self.done += 1
        ahead, behind = self.ahead, self.behind
        if after:
            ahead, behind = pin(ahead, *after), pin(behind, *after)
        if self.done == 4:
            ahead, behind = ahead[: self.half], behind[self.half :]
        ahead = lax.ppermute(ahead, "fsdp", NEXT)
        behind = lax.ppermute(behind, "fsdp", PREV)
        if self.done == 4:
            self.blocks[4] = (ahead, behind)
        else:
            self.blocks[8 - self.done], self.blocks[self.done] = ahead, behind
        self.ahead, self.behind = ahead, behind
        return ahead, behind

    def pieces(self):
        for j, block in enumerate(self.blocks):
            if j == 4:
                yield j, 0, block[0]
                yield j, self.half, block[1]
            else:
                yield j, 0, block


class RingScatter:
    def __init__(self, blocks):
        self.blocks = blocks
        self.half = blocks[0].shape[0] // 2
        self.ahead, self.behind = blocks[4][: self.half], blocks[4][self.half :]
        self.done = 0

    def step(self, *after):
        self.done += 1
        half = self.half
        ahead = lax.ppermute(pin(self.ahead, *after), "fsdp", NEXT)
        behind = lax.ppermute(pin(self.behind, *after), "fsdp", PREV)
        got = (ahead, behind)
        ahead, behind = ahead.astype(F32), behind.astype(F32)
        if self.done == 1:
            up, down = self.blocks[3].astype(F32), self.blocks[5].astype(F32)
            ahead = jnp.concatenate([up[:half] + ahead, up[half:]])
            behind = jnp.concatenate([down[:half], down[half:] + behind])
        elif self.done < 4:
            ahead = self.blocks[4 - self.done].astype(F32) + ahead
            behind = self.blocks[4 + self.done].astype(F32) + behind
        else:
            self.total = self.blocks[0].astype(F32) + ahead + behind
            return got
        self.ahead, self.behind = ahead.astype(BF16), behind.astype(BF16)
        return got


def seq_gather(mine, hold=()):
    over = lax.ppermute(mine, "seq", ROW)
    beside = lax.ppermute(mine, "seq", CORE)
    return [mine, beside, over, lax.ppermute(pin(over, *hold), "seq", CORE)]


def seq_scatter(parts):
    corner = lax.ppermute(parts[3].astype(BF16), "seq", CORE)
    beside = lax.ppermute(parts[1].astype(BF16), "seq", CORE)
    far = (parts[2] + corner.astype(F32)).astype(BF16)
    over = lax.ppermute(far, "seq", ROW)
    return parts[0] + beside.astype(F32) + over.astype(F32), far


class Fast:
    def __init__(self, s, f):
        self.s, self.f = s, f
        table = lax.dynamic_index_in_dim(jnp.asarray(ORDER), f, 0, keepdims=False)
        self.order = [table[j] for j in range(8)]
        self.slots = jnp.arange(4, dtype=jnp.int32) ^ s
        self.rings = {}

    def gather(self, **blocks):
        self.rings.update({name: RingGather(block) for name, block in blocks.items()})

    def scatter(self, **wholes):
        for name, whole in wholes.items():
            order = self.order if name in "FS" else range(8)
            size = whole.shape[0] // 8
            self.rings[name] = RingScatter(
                [lax.dynamic_slice_in_dim(whole, order[j] * size, size, 0) for j in range(8)]
            )

    def hop(self, names, *after):
        got = ()
        for name in names:
            got += self.rings[name].step(*after)
        return got

    def gather_out(self, w_out, small, count):
        size = w_out.shape[0] // 4
        self.out_rows = size
        own = lax.dynamic_slice_in_dim(w_out, self.s * size, size, 0)
        pad = jnp.full((w_out.shape[1] - small.shape[0],), count.astype(BF16))
        line = jnp.broadcast_to(jnp.concatenate([small, pad])[None], (16, w_out.shape[1]))
        self.gather(o=jnp.concatenate([own, line]))

    def close_out(self):
        whole = self.as_found(self.rings["o"])
        whole = whole.reshape(8, -1, whole.shape[1])
        places = (jnp.asarray(PLACE) - jnp.asarray(PLACE)[self.f]) % 8
        rows = jnp.take(whole[:, : self.out_rows], places, axis=0)
        small = jnp.take(whole[:, self.out_rows], places, axis=0)
        return rows.reshape(-1, whole.shape[2]), small.astype(F32)

    def whole(self, name):
        return self.in_order(self.rings[name]) if name == "q" else self.as_found(self.rings[name])

    def scatter_pair(self, gate, up):
        gates, ups = (v.reshape(8, -1, v.shape[1]) for v in (gate, up))
        self.rings["W"] = RingScatter([jnp.concatenate([gates[j], ups[j]]) for j in range(8)])

    def scatter_first(self, raw_first, raw_out, *after):
        rows, cols = raw_out.shape
        split = raw_out.reshape(8, rows // 8, 4, cols // 4).transpose(0, 2, 1, 3)
        both = jnp.concatenate([raw_first, split.reshape(-1, cols // 4)], axis=1)
        self.first_cols = raw_first.shape[1]
        self.scatter(F=pin(both, *after))

    def total(self, name):
        if name not in "FO":
            return self.rings[name].total
        total = self.rings["F"].total
        if name == "F":
            return total[:, : self.first_cols]
        split = total[:, self.first_cols :].reshape(4, self.out_rows, -1)
        return split.transpose(1, 0, 2).reshape(self.out_rows, -1)

    def in_order(self, ring):
        size, cols = ring.blocks[0].shape
        whole = jnp.zeros((8 * size, cols), BF16)
        for j, first, part in ring.pieces():
            at = self.order[j] * size + first
            whole = lax.dynamic_update_slice(whole, part, (at, 0))
        return whole

    def as_found(self, ring):
        return jnp.concatenate([part for unused, unused, part in ring.pieces()])

    def pick_qkv(self, w_qkv):
        return pick_columns(w_qkv, self.s)

    def bias_of_heads(self, full_bias):
        split = full_bias.reshape(3, 4, 2, 4, HD)
        own = lax.dynamic_index_in_dim(split, self.s, 3, keepdims=False)
        return own.transpose(1, 0, 2, 3).reshape(1, 12 * LANES)

    def bias_of_all(self, own):
        split = own.reshape(4, 3, 2, HD).transpose(1, 0, 2, 3)
        here = (jnp.arange(4) == self.s).astype(F32)[None, None, None, :, None]
        return (split[:, :, :, None, :] * here).reshape(-1)

    def spread(self, name, *after, hold=()):
        return seq_gather(pin(self.total(name).astype(BF16), *after), hold)

    def final_qkv(self, first, second, factor):
        return unpick_columns([first, second], self.s, factor)

    def final_rows(self, parts, factor):
        return place_rows(parts, self.s, factor)

    final_out = final_rows

    def final_pairs(self, parts, factor):
        return place_pairs(parts, self.s, factor)

    def tokens(self, mine):
        return jnp.concatenate(seq_gather(mine))

    def tokens_sum(self, partial):
        rows = partial.shape[0] // 4
        return seq_scatter([partial[i * rows : (i + 1) * rows] for i in range(4)])

    def by_slot(self, values):
        split = values.reshape((4, values.shape[0] // 4) + values.shape[1:])
        return jnp.take(split, self.slots, axis=0).reshape(values.shape)

    def small_reduce(self, values, *after):
        total = jnp.take(values, self.f ^ jnp.arange(8), axis=0)
        for bit in (4, 2, 1):
            other = lax.ppermute(total[bit:], "fsdp", [(i, i ^ bit) for i in range(8)])
            total = total[:bit] + other
        return self.seq_sum(pin(total[0], *after))

    def seq_sum(self, total):
        total = total + lax.ppermute(total, "seq", CORE)
        return total + lax.ppermute(total, "seq", ROW)


class General:
    def __init__(self, s, f):
        self.s, self.f = s, f
        self.members, self.shards = lax.axis_size("seq"), lax.axis_size("fsdp")
        self.slots = jnp.arange(self.members, dtype=jnp.int32)
        self.pairs = H // self.members // 2
        self.wholes, self.totals = {}, {}

    def gather(self, **blocks):
        for name, block in blocks.items():
            self.wholes[name] = lax.all_gather(block, "fsdp", axis=0, tiled=True)

    def scatter(self, **wholes):
        for name, whole in wholes.items():
            if name == "O":
                rows = whole.shape[0]
                every = jnp.zeros((rows * self.members, whole.shape[1]), whole.dtype)
                whole = lax.dynamic_update_slice(every, whole, (self.s * rows, 0))
            total = lax.psum_scatter(whole, "fsdp", scatter_dimension=0, tiled=True)
            self.totals[name] = total.astype(F32)

    def hop(self, names, *after):
        return ()

    def gather_out(self, w_out, small, count):
        self.gather(o=w_out)
        small = jnp.concatenate([small.astype(F32), jnp.full((LANES,), count)])
        self.small = lax.all_gather(small, "fsdp", axis=0, tiled=False)

    def close_out(self):
        rows = self.wholes["o"].shape[0] // self.members
        own = lax.dynamic_slice_in_dim(self.wholes["o"], self.s * rows, rows, 0)
        return own, self.small

    def whole(self, name):
        return self.wholes[name]

    def scatter_pair(self, gate, up):
        both = [v.reshape(self.shards, -1, v.shape[1]) for v in (gate, up)]
        self.scatter(W=jnp.concatenate(both, axis=1).reshape(-1, gate.shape[1]))

    def scatter_first(self, raw_first, raw_out, *after):
        self.scatter(F=raw_first, O=raw_out)

    def total(self, name):
        return self.totals[name]

    def pick_qkv(self, w_qkv):
        split = w_qkv.reshape(w_qkv.shape[0], 3, self.members, self.pairs, LANES)
        own = lax.dynamic_index_in_dim(split, self.s, 2, keepdims=False)
        return own.transpose(0, 2, 1, 3).reshape(w_qkv.shape[0], -1)

    def bias_of_heads(self, full_bias):
        split = full_bias.reshape(3, self.members, self.pairs, LANES)
        own = lax.dynamic_index_in_dim(split, self.s, 1, keepdims=False)
        return own.transpose(1, 0, 2).reshape(1, -1)

    def bias_of_all(self, own):
        split = own.reshape(self.pairs, 3, LANES).transpose(1, 0, 2)
        here = (jnp.arange(self.members) == self.s).astype(F32)[None, :, None, None]
        return (split[:, None] * here).reshape(-1)

    def gathered(self, share):
        return lax.all_gather(share.astype(BF16), "seq", axis=0, tiled=False)

    def spread(self, name, *after, hold=()):
        return [self.total(name)]

    def final_qkv(self, first, second, factor):
        share = jnp.concatenate(first + second, axis=1)
        parts = self.gathered(share).reshape(self.members, -1, self.pairs, 3, LANES)
        return factor * parts.transpose(1, 3, 0, 2, 4).reshape(parts.shape[1], -1).astype(F32)

    def final_rows(self, parts, factor):
        share = parts[0]
        return factor * self.gathered(share).reshape(-1, share.shape[1]).astype(F32)

    def final_out(self, parts, factor):
        return factor * lax.psum(parts[0].astype(BF16), "seq").astype(F32)

    def final_pairs(self, parts, factor):
        rows = parts[0].shape[0] // 2
        parts = jnp.stack([parts[0][:rows], parts[0][rows:]], axis=1)
        parts = lax.all_gather(parts.astype(BF16), "seq", axis=0, tiled=True)
        return factor * parts.astype(F32)

    def tokens(self, mine):
        return lax.all_gather(mine, "seq", axis=0, tiled=True)

    def tokens_sum(self, partial):
        total = lax.psum_scatter(partial.astype(BF16), "seq", scatter_dimension=0, tiled=True)
        return total.astype(F32), total

    def by_slot(self, values):
        return values

    def small_reduce(self, values, *after):
        total = lax.psum(values, ("seq", "fsdp"))
        return lax.dynamic_index_in_dim(total, self.f, 0, keepdims=False)

    def seq_sum(self, total):
        return lax.psum(total, "seq")


def call(kernel, grid, in_specs, out_specs, out_shape, scratch=(), prefetch=0, cost=None):
    return pl.pallas_call(
        kernel,
        grid_spec=pltpu.PrefetchScalarGridSpec(
            num_scalar_prefetch=prefetch,
            grid=grid,
            in_specs=in_specs,
            out_specs=out_specs,
            scratch_shapes=list(scratch),
        ),
        out_shape=out_shape,
        compiler_params=pltpu.CompilerParams(vmem_limit_bytes=VMEM_LIMIT),
        cost_estimate=cost,
    )


def pick_kernel(s_ref, w_ref, out_ref):
    s = s_ref[0]
    lane = lax.broadcasted_iota(jnp.int32, (w_ref.shape[0], LANES), 1)
    odd = (s & 1) == 1
    for pair in range(4):
        for part in range(3):
            at = part * 2048 + pair * 512 + (s >> 1) * LANES
            one = w_ref[:, pl.ds(pl.multiple_of(at, LANES), LANES)].astype(F32)
            two = w_ref[:, pl.ds(pl.multiple_of(at + 256, LANES), LANES)].astype(F32)
            one = jnp.where(odd, pltpu.roll(one, HD, 1), one)
            two = jnp.where(odd, two, pltpu.roll(two, HD, 1))
            to = (pair * 3 + part) * LANES
            out_ref[:, to : to + LANES] = jnp.where(lane < HD, one, two).astype(BF16)


def pick_columns(w_qkv, s):
    rows, cols = w_qkv.shape
    step = rows // 4
    return call(
        pick_kernel,
        (4,),
        [pl.BlockSpec((step, cols), lambda g, s_ref: (g, 0))],
        pl.BlockSpec((step, 12 * LANES), lambda g, s_ref: (g, 0)),
        jax.ShapeDtypeStruct((rows, 12 * LANES), BF16),
        prefetch=1,
    )(s.reshape(1), w_qkv)


def unpick_kernel(s_ref, factor_ref, *refs):
    out_ref, ordered = refs[-2:]
    s = s_ref[0]
    factor = factor_ref[0]
    rows = out_ref.shape[0]
    lane = lax.broadcasted_iota(jnp.int32, (rows, LANES), 1)
    for half in range(2):
        for r in range(4):
            ordered[s ^ r] = refs[4 * half + r][...].astype(F32) * factor
        for pair in range(2):
            for part in range(3):
                at = slice((pair * 3 + part) * LANES, (pair * 3 + part + 1) * LANES)
                heads = [ordered[m, :, at] for m in range(4)]
                turned = [pltpu.roll(h, HD, 1) for h in heads]
                to = part * 2048 + (2 * half + pair) * 512
                for m in (0, 2):
                    low = jnp.where(lane < HD, heads[m], turned[m + 1])
                    high = jnp.where(lane < HD, turned[m], heads[m + 1])
                    out_ref[:, to + m * HD : to + m * HD + LANES] = low
                    out_ref[:, to + 256 + m * HD : to + 256 + m * HD + LANES] = high


def unpick_columns(parts, s, factor):
    rows, cols = parts[0][0].shape
    step = rows // 4
    return call(
        unpick_kernel,
        (4,),
        [pl.BlockSpec(memory_space=pltpu.SMEM)]
        + [pl.BlockSpec((step, cols), lambda g, s_ref: (g, 0))] * 8,
        pl.BlockSpec((step, 8 * cols), lambda g, s_ref: (g, 0)),
        jax.ShapeDtypeStruct((rows, 8 * cols), F32),
        scratch=[pltpu.VMEM((4, step, cols), F32)],
        prefetch=1,
    )(s.reshape(1), factor.reshape(1), *parts[0], *parts[1])


def place_kernel(s_ref, factor_ref, p0, p1, p2, p3, out_ref):
    r = pl.program_id(0)
    for k, part in enumerate((p0, p1, p2, p3)):

        @pl.when(r == k)
        def _(part=part):
            out_ref[...] = part[...].astype(F32) * factor_ref[0]


def place_rows(parts, s, factor):
    rows, cols = parts[0].shape
    return call(
        place_kernel,
        (4,),
        [pl.BlockSpec(memory_space=pltpu.SMEM)]
        + [pl.BlockSpec((rows, cols), lambda r, s_ref: (0, 0))] * 4,
        pl.BlockSpec((rows, cols), lambda r, s_ref: (s_ref[0] ^ r, 0)),
        jax.ShapeDtypeStruct((4 * rows, cols), F32),
        prefetch=1,
    )(s.reshape(1), factor.reshape(1), *parts)


def place_pair_kernel(s_ref, factor_ref, p0, p1, p2, p3, out_ref):
    r = pl.program_id(0)
    rows = out_ref.shape[0]
    for k, part in enumerate((p0, p1, p2, p3)):

        @pl.when(r == k)
        def _(part=part):
            out_ref[:, 0, :] = part[:rows, :].astype(F32) * factor_ref[0]
            out_ref[:, 1, :] = part[rows:, :].astype(F32) * factor_ref[0]


def place_pairs(parts, s, factor):
    rows, cols = parts[0].shape
    half = rows // 2
    return call(
        place_pair_kernel,
        (4,),
        [pl.BlockSpec(memory_space=pltpu.SMEM)]
        + [pl.BlockSpec((rows, cols), lambda r, s_ref: (0, 0))] * 4,
        pl.BlockSpec((half, 2, cols), lambda r, s_ref: (s_ref[0] ^ r, 0, 0)),
        jax.ShapeDtypeStruct((4 * half, 2, cols), F32),
        prefetch=1,
    )(s.reshape(1), factor.reshape(1), *parts)


def turn(values, cosine, sine_low, sine_high, sign):
    half = ROT // 2
    moved = (
        pltpu.roll(values, LANES - half, 1) * sine_low + pltpu.roll(values, half, 1) * sine_high
    )
    return values * cosine + moved if sign > 0 else values * cosine - moved


def two_heads(values):
    lane = lax.broadcasted_iota(jnp.int32, values.shape, 1)
    nothing = jnp.zeros_like(values)
    return jnp.concatenate(
        [jnp.where(lane < HD, values, nothing), jnp.where(lane < HD, nothing, values)], axis=0
    )


def one_pair(stacked):
    rows = stacked.shape[0] // 2
    lane = lax.broadcasted_iota(jnp.int32, (rows, LANES), 1)
    return jnp.where(lane < HD, stacked[:rows], stacked[rows:])


def forward_kernel(
    block, slots, slot_ref, first_ref, qkv, bias, cosine, low, high, start, turned, out
):
    scale = HD ** (-0.5)

    def rotate_block(i, unused):
        rows = pl.ds(pl.multiple_of(i * block, block), block)
        tables = (cosine[rows, :], low[rows, :], high[rows, :], 1)
        query = qkv[rows, 0:LANES] + bias[:, 0:LANES]
        key = qkv[rows, LANES : 2 * LANES] + bias[:, LANES : 2 * LANES]
        value = qkv[rows, 2 * LANES : 3 * LANES] + bias[:, 2 * LANES : 3 * LANES]
        turned[rows, 0:LANES] = turn(query, *tables).astype(BF16)
        turned[rows, LANES : 2 * LANES] = turn(key, *tables).astype(BF16)
        turned[rows, 2 * LANES : 3 * LANES] = value.astype(BF16)
        return unused

    lax.fori_loop(0, slots, rotate_block, 0)

    column = lax.broadcasted_iota(jnp.int32, (2 * block, block), 1)
    line = lax.broadcasted_iota(jnp.int32, (2 * block, block), 0) & (block - 1)

    def query_block(i, unused):
        rows = pl.ds(pl.multiple_of(slot_ref[i] * block, block), block)
        query = two_heads((turned[rows, 0:LANES].astype(F32) * scale).astype(BF16))
        first = start[rows, :]
        first = jnp.concatenate([first, first], axis=0)

        def scores(j):
            keys = pl.ds(pl.multiple_of(slot_ref[j] * block, block), block)
            result = dot_nt(query, turned[keys, LANES : 2 * LANES])
            allowed = column >= first - j * block
            return result, allowed, turned[keys, 2 * LANES : 3 * LANES]

        result, allowed, value = scores(i)
        result = jnp.where(allowed & (column <= line), result, MASKED_VALUE)
        peak = jnp.max(result, axis=1, keepdims=True)
        weight = jnp.exp(result - peak)
        total = jnp.sum(weight, axis=1, keepdims=True)
        gathered = dot_nn(weight.astype(BF16), value)

        def key_block(j, carry):
            peak, total, gathered = carry
            result, allowed, value = scores(j)
            result = jnp.where(allowed, result, MASKED_VALUE)
            higher = jnp.maximum(peak, jnp.max(result, axis=1, keepdims=True))
            shrink = jnp.exp(peak - higher)
            weight = jnp.exp(result - higher)
            total = total * shrink + jnp.sum(weight, axis=1, keepdims=True)
            gathered = gathered * shrink + dot_nn(weight.astype(BF16), value)
            return higher, total, gathered

        peak, total, gathered = lax.fori_loop(first_ref[i], i, key_block, (peak, total, gathered))
        out[rows, :] = one_pair(gathered / total).astype(BF16)
        return unused

    lax.fori_loop(0, slots, query_block, 0)


def attention_forward(qkv, bias, tables, start, slot_of, first_slot, *, block, skip, pairs):
    length = qkv.shape[0]
    width = pairs * 3 * LANES
    slots = length // block
    whole = pl.BlockSpec((length, LANES), lambda p, *_: (0, 0))
    return call(
        functools.partial(forward_kernel, block, slots),
        (pairs,),
        [
            pl.BlockSpec((length, 3 * LANES), lambda p, *_: (0, p + skip)),
            pl.BlockSpec((1, 3 * LANES), lambda p, *_: (0, p + skip)),
            whole,
            whole,
            whole,
            pl.BlockSpec((length, 1), lambda p, *_: (0, 0)),
        ],
        [
            pl.BlockSpec((length, 3 * LANES), lambda p, *_: (0, p)),
            pl.BlockSpec((length, LANES), lambda p, *_: (0, p)),
        ],
        [
            jax.ShapeDtypeStruct((length, width), BF16),
            jax.ShapeDtypeStruct((length, width // 3), BF16),
        ],
        prefetch=2,
        cost=pl.CostEstimate(
            flops=length * length * width * 2,
            bytes_accessed=length * width * 8,
            transcendentals=length * length * width // (3 * HD),
        ),
    )(slot_of, first_slot, qkv, bias, *tables, start)


def backward_kernel(
    block,
    slots,
    slot_ref,
    first_ref,
    turned,
    out_grad,
    cosine,
    low,
    high,
    start,
    grads,
    key_sum,
    value_sum,
    weights,
    products,
):
    scale = HD ** (-0.5)
    key_sum[...] = jnp.zeros_like(key_sum)
    value_sum[...] = jnp.zeros_like(value_sum)
    column = lax.broadcasted_iota(jnp.int32, (block, 2 * block), 1) & (block - 1)
    line = lax.broadcasted_iota(jnp.int32, (block, 2 * block), 0)

    def query_block(i, unused):
        begin = pl.multiple_of(slot_ref[i] * block, block)
        rows = pl.ds(begin, block)
        query = two_heads((turned[rows, 0:LANES].astype(F32) * scale).astype(BF16))
        grad = two_heads(out_grad[rows, :])
        first = start[:, pl.ds(begin, block)]
        first = jnp.concatenate([first, first], axis=1)

        def scores(j):
            keys = pl.ds(pl.multiple_of(slot_ref[j] * block, block), block)
            result = dot_nt(turned[keys, LANES : 2 * LANES], query)
            return result, line >= first - j * block

        result, allowed = scores(i)
        result = jnp.where(allowed & (line <= column), result, MASKED_VALUE)
        weights[0] = result
        peak = jnp.max(result, axis=0, keepdims=True)

        def score_block(j, peak):
            result, allowed = scores(j)
            result = jnp.where(allowed, result, MASKED_VALUE)
            weights[i - j] = result
            return jnp.maximum(peak, jnp.max(result, axis=0, keepdims=True))

        peak = lax.fori_loop(first_ref[i], i, score_block, peak)

        def weight_block(j, carry):
            total, cross = carry
            keys = pl.ds(pl.multiple_of(slot_ref[j] * block, block), block)
            weight = jnp.exp(weights[i - j] - peak)
            product = dot_nt(turned[keys, 2 * LANES : 3 * LANES], grad)
            weights[i - j] = weight
            products[i - j] = product
            total = total + jnp.sum(weight, axis=0, keepdims=True)
            cross = cross + jnp.sum(weight * product, axis=0, keepdims=True)
            return total, cross

        zero = jnp.zeros((1, 2 * block), F32)
        total, cross = lax.fori_loop(first_ref[i], i + 1, weight_block, (zero, zero))
        share = 1.0 / total
        cross = cross * share

        def grad_block(j, query_sum):
            keys = pl.ds(pl.multiple_of(slot_ref[j] * block, block), block)
            weight = weights[i - j] * share
            score_grad = (weight * (products[i - j] - cross)).astype(BF16)
            value_sum[keys, :] += dot_nn(weight.astype(BF16), grad)
            key_sum[keys, :] += dot_nn(score_grad, query)
            return query_sum + dot_tn(score_grad, turned[keys, LANES : 2 * LANES])

        query_sum = lax.fori_loop(
            first_ref[i], i + 1, grad_block, jnp.zeros((2 * block, LANES), F32)
        )
        tables = (cosine[rows, :], low[rows, :], high[rows, :], -1)
        grads[rows, 0:LANES] = turn(one_pair(query_sum) * scale, *tables).astype(BF16)
        return unused

    lax.fori_loop(0, slots, query_block, 0)

    def finish(i, unused):
        rows = pl.ds(pl.multiple_of(i * block, block), block)
        tables = (cosine[rows, :], low[rows, :], high[rows, :], -1)
        grads[rows, LANES : 2 * LANES] = turn(key_sum[rows, :], *tables).astype(BF16)
        grads[rows, 2 * LANES : 3 * LANES] = value_sum[rows, :].astype(BF16)
        return unused

    lax.fori_loop(0, slots, finish, 0)


def attention_backward(turned, out_grad, tables, start, slot_of, first_slot, block, skip):
    length, width = turned.shape
    pairs = width // (3 * LANES)
    slots = length // block
    whole = pl.BlockSpec((length, LANES), lambda p, *_: (0, 0))
    return call(
        functools.partial(backward_kernel, block, slots),
        (pairs,),
        [
            pl.BlockSpec((length, 3 * LANES), lambda p, *_: (0, p)),
            pl.BlockSpec((length, LANES), lambda p, *_: (0, p + skip)),
            whole,
            whole,
            whole,
            pl.BlockSpec((1, length), lambda p, *_: (0, 0)),
        ],
        pl.BlockSpec((length, 3 * LANES), lambda p, *_: (0, p)),
        jax.ShapeDtypeStruct((length, width), BF16),
        scratch=[
            pltpu.VMEM((length, LANES), F32),
            pltpu.VMEM((length, LANES), F32),
            pltpu.VMEM((slots, block, 2 * block), F32),
            pltpu.VMEM((slots, block, 2 * block), F32),
        ],
        prefetch=2,
        cost=pl.CostEstimate(
            flops=length * length * width * 5,
            bytes_accessed=length * width * 6,
            transcendentals=length * length * width // (3 * HD),
        ),
    )(slot_of, first_slot, turned, out_grad, *tables, start)


def turn_tables(positions):
    half = ROT // 2
    lane = jnp.arange(LANES, dtype=jnp.int32) % HD
    inverse = 10000.0 ** (-((lane % half).astype(F32) * 2.0) / ROT)
    angles = positions.astype(F32)[:, None] * jnp.where(lane < ROT, inverse, 0.0)[None, :]
    cosine, sine = jnp.cos(angles), jnp.sin(angles)
    lane = lane[None, :]
    return (
        cosine,
        jnp.where(lane < half, -sine, 0.0),
        jnp.where((lane >= half) & (lane < ROT), sine, 0.0),
    )


def per_device(
    tokens,
    teacher,
    segments,
    valid,
    ln1_gain,
    ln1_bias,
    w_qkv,
    b_qkv,
    w_out,
    ln2_gain,
    ln2_bias,
    w_gate_up,
    w_down,
):
    s = lax.axis_index("seq")
    f = lax.axis_index("fsdp")
    members, shards = lax.axis_size("seq"), lax.axis_size("fsdp")
    net = (Fast if (members, shards) == (4, 8) else General)(s, f)
    rows = tokens.shape[1]
    width = tokens.shape[2]
    length = segments.shape[1]
    units = w_down.shape[0] // members
    vec = ln1_gain.shape[0]
    bias_share = b_qkv.shape[0]
    pairs = H // members // 2

    tokens_all = net.tokens(tokens[0])

    mine_gate_up = lax.dynamic_slice_in_dim(w_gate_up, s * units, units, 0)
    counted = valid[0].astype(F32)
    small = jnp.concatenate([ln1_gain, ln1_bias, ln2_gain, ln2_bias, b_qkv])
    net.gather_out(w_out, small, jnp.sum(counted))
    net.gather(
        q=net.pick_qkv(w_qkv),
        g=mine_gate_up[:, 0],
        u=mine_gate_up[:, 1],
        d=lax.dynamic_slice_in_dim(w_down, s * units, units, 0),
    )
    done = net.hop("qo")

    normed_all, unused = norm_parts(pin(tokens_all, *done).astype(F32))
    done = net.hop("q")

    segment = pin(segments, *done)[0]
    slot_segment = net.by_slot(segment)
    slot_start = jnp.sum((segment[None, :] < slot_segment[:, None]).astype(jnp.int32), axis=1)
    slot_place = net.by_slot(jnp.arange(length, dtype=jnp.int32))
    block_first = segment.reshape(members, rows)[:, 0]
    first_slot = (
        jnp.sum((segment[None, :] < block_first[:, None]).astype(jnp.int32), axis=1) // rows
    )
    done = net.hop("q") + net.hop("o", *done)
    tables = turn_tables(slot_place - pin(slot_start, *done))
    net.hop("qo", *done)
    net.hop("o")
    full_out, small = net.close_out()
    gain_one, shift_one, gain_two, shift_two = (
        small[:, i * vec : (i + 1) * vec].reshape(width) for i in range(4)
    )
    own_bias = net.bias_of_heads(small[:, 4 * vec : 4 * vec + bias_share].reshape(-1))
    sum_count = net.seq_sum(jnp.sum(small[:, -LANES:], axis=0))[0]
    factor = (rows * members * shards) / sum_count
    hidden_one = (normed_all * gain_one + shift_one).astype(BF16)
    done = net.hop("g", *done)
    qkv = dot_nn(hidden_one, pin(net.whole("q"), *done, *tables))
    half_pairs = pairs // 2
    forward = functools.partial(
        attention_forward,
        qkv,
        own_bias,
        tables,
        slot_start[:, None],
        net.slots,
        block=rows,
        pairs=half_pairs,
    )
    turned_one, heads_one = forward(pin(first_slot, factor), skip=0)
    done = net.hop("gu", *done)
    turned_two, heads_two = forward(pin(first_slot, heads_one, *done), skip=half_pairs)
    heads_out = jnp.concatenate([heads_one, heads_two], axis=1)
    tokens_in = tokens[0].astype(F32)
    done = net.hop("gu", heads_one)
    partial = dot_nn(pin(heads_out, *done), full_out)
    attended = net.tokens_sum(partial)[0]
    done = net.hop("gu", heads_two)
    resid = tokens_in + pin(attended, *done)

    normed_two, inv_std_two = norm_parts(resid)
    mine_two = (normed_two * gain_two + shift_two).astype(BF16)
    hidden_two = net.tokens(mine_two)
    done = net.hop("u", mine_two) + net.hop("d", mine_two)
    full_gate = net.whole("g")
    gate = dot_nt(full_gate, pin(hidden_two, *done))
    done = net.hop("d")
    full_up = net.whole("u")
    up = dot_nt(pin(full_up, gate, *done), hidden_two)
    hidden = (jax.nn.silu(gate) * up).astype(BF16)
    done = net.hop("d", gate)
    hidden = pin(hidden, *done)
    net.hop("d", hidden)
    full_down = net.whole("d")
    outputs = resid + net.tokens_sum(dot_tn(hidden, full_down))[0]
    differ = outputs - teacher[0].astype(F32)
    cot = counted[:, None] * differ
    half_sum = 0.5 * jnp.sum(cot * differ)
    cot_low = net.tokens(cot.astype(BF16))

    raw_down = dot_nn(hidden, cot_low).astype(BF16)
    net.scatter(D=raw_down)
    done = net.hop("D")
    hidden_grad = dot_nt(pin(full_down, raw_down), cot_low)
    sigma = jax.nn.sigmoid(gate)
    silu_grad = hidden_grad * up
    gate_grad = (silu_grad * sigma + silu_grad * gate * sigma * (1.0 - sigma)).astype(BF16)
    up_grad = (hidden_grad * (gate * sigma)).astype(BF16)

    raw_gate = dot_nn(gate_grad, pin(hidden_two, *done)).astype(BF16)
    raw_up = dot_nn(up_grad, pin(hidden_two, raw_gate)).astype(BF16)
    done = net.hop("D", gate_grad)
    partial = dot_tn(gate_grad, pin(full_gate, raw_up, *done))
    done = net.hop("D")
    partial = partial + dot_tn(up_grad, pin(full_up, partial))
    two_grad, far = net.tokens_sum(pin(partial, *done))
    net.scatter_pair(pin(raw_gate, *done), pin(raw_up, *done))
    done = net.hop("DW", far)

    two_grad = pin(two_grad, *done)
    resid_grad = cot + norm_back(two_grad, normed_two, inv_std_two, gain_two)
    gain_two_grad = jnp.sum(two_grad * normed_two, axis=0)
    shift_two_grad = jnp.sum(two_grad, axis=0)
    mine_low = resid_grad.astype(BF16)
    resid_low = net.tokens(mine_low)
    done = net.hop("W", mine_low)

    full_qkv = net.whole("q")
    out_grad = dot_nt(pin(resid_low, *done), full_out).astype(BF16)
    backward = functools.partial(
        attention_backward,
        tables=tables,
        start=slot_start[None, :],
        slot_of=net.slots,
        block=rows,
    )
    grad_first = backward(turned_one, out_grad, first_slot=first_slot, skip=0)
    raw_out = dot_tn(heads_out, pin(resid_low, grad_first)).astype(BF16)
    raw_first = dot_tn(hidden_one, grad_first).astype(BF16)
    done = net.hop("W", out_grad)

    net.scatter_first(raw_first, raw_out, *done)
    parts_down = net.spread("D", out_grad)
    here = pin(first_slot, raw_first, *done, *parts_down)
    grad_second = backward(turned_two, out_grad, first_slot=here, skip=half_pairs)
    done = net.hop("F", raw_first) + net.hop("W")

    raw_second = dot_tn(hidden_one, pin(grad_second, *done)).astype(BF16)
    done = net.hop("F", grad_second)
    qkv_grad = pin(jnp.concatenate([grad_first, grad_second], axis=1), raw_second, *done)
    net.scatter(S=pin(raw_second, *done))
    partial = dot_nt(qkv_grad, full_qkv)
    done = net.hop("FS")

    grad_one, far = net.tokens_sum(pin(partial, *done))
    done = net.hop("FS", far)

    third = net.hop("S", *done)
    normed_one, inv_std_one = norm_parts(tokens_in)
    tokens_grad = resid_grad + norm_back(grad_one, normed_one, inv_std_one, gain_one)
    gain_one_grad = jnp.sum(grad_one * normed_one, axis=0)
    shift_one_grad = jnp.sum(grad_one, axis=0)
    bias_grad = net.bias_of_all(jnp.sum(qkv_grad.astype(F32), axis=0)).reshape(shards, -1)
    vectors = jnp.concatenate(
        [
            v.reshape(shards, vec)
            for v in (gain_one_grad, shift_one_grad, gain_two_grad, shift_two_grad)
        ]
        + [bias_grad, jnp.full((shards, LANES), half_sum)],
        axis=1,
    ).reshape(shards, -1, LANES)
    grad_w_down = net.final_rows(parts_down, pin(factor, raw_second))
    parts_first, parts_out = net.spread("F"), net.spread("O")
    last = net.hop("S", *third)
    parts_pair = net.spread("W", grad_one, hold=last)
    vectors = net.small_reduce(pin(vectors, *third), *last).reshape(-1)
    loss = 2.0 * vectors[4 * vec + bias_share] / (sum_count * width)
    scaled = factor * vectors
    grad_w_gate_up = net.final_pairs(parts_pair, factor)
    grad_w_out = net.final_out(parts_out, factor)
    parts_second = net.spread("S", grad_w_down, grad_w_gate_up)

    return (
        outputs.astype(BF16)[None],
        loss,
        (factor * tokens_grad).astype(BF16)[None],
        scaled[:vec],
        scaled[vec : 2 * vec],
        net.final_qkv(parts_first, parts_second, factor),
        scaled[4 * vec : 4 * vec + bias_share],
        grad_w_out,
        scaled[2 * vec : 3 * vec],
        scaled[3 * vec : 4 * vec],
        grad_w_gate_up,
        grad_w_down,
    )


def solution(mesh):
    placed = (
        P("fsdp", "seq", None),
        P("fsdp", "seq", None),
        P("fsdp", None),
        P("fsdp", "seq"),
        P("fsdp"),
        P("fsdp"),
        P("fsdp", None),
        P("fsdp"),
        P("fsdp", None),
        P("fsdp"),
        P("fsdp"),
        P("fsdp", None, None),
        P("fsdp", None),
    )
    return jax.shard_map(
        per_device,
        mesh=mesh,
        in_specs=placed,
        out_specs=(
            P("fsdp", "seq", None),
            P(),
            P("fsdp", "seq", None),
            P("fsdp"),
            P("fsdp"),
            P("fsdp", None),
            P("fsdp"),
            P("fsdp", None),
            P("fsdp"),
            P("fsdp"),
            P("fsdp", None, None),
            P("fsdp", None),
        ),
        check_vma=False,
    )
```

```python
import functools

import jax
import jax.numpy as jnp
import numpy as np
from jax import lax
from jax.experimental import pallas as pl
from jax.experimental.pallas import tpu as pltpu
from jax.sharding import PartitionSpec as P

H = 32
HD = 64
ROT = 16
LANES = 128

EPSILON = 1e-05
MASKED_VALUE = -1e30

F32 = jnp.float32
BF16 = jnp.bfloat16
VMEM_LIMIT = 60 * 1024 * 1024

RING = (0, 2, 4, 6, 7, 5, 3, 1)
NEXT = [(RING[i], RING[(i + 1) % 8]) for i in range(8)]
PREV = [(RING[(i + 1) % 8], RING[i]) for i in range(8)]
ORDER = np.array([[RING[(RING.index(f) + j) % 8] for j in range(8)] for f in range(8)], np.int32)
PLACE = np.array([RING.index(f) for f in range(8)], np.int32)
CORE = [(s, s ^ 1) for s in range(4)]
ROW = [(s, s ^ 2) for s in range(4)]


def dot_nn(a, b):
    return lax.dot_general(a, b, (((1,), (0,)), ((), ())), preferred_element_type=F32)


def dot_nt(a, b):
    return lax.dot_general(a, b, (((1,), (1,)), ((), ())), preferred_element_type=F32)


def dot_tn(a, b):
    return lax.dot_general(a, b, (((0,), (0,)), ((), ())), preferred_element_type=F32)


def norm_parts(values):
    mean_value = jnp.mean(values, axis=-1, keepdims=True)
    centered = values - mean_value
    variance = jnp.mean(centered * centered, axis=-1, keepdims=True)
    inv_std = lax.rsqrt(variance + EPSILON)
    return (centered * inv_std, inv_std)


def norm_back(grad_out, normed, inv_std, gain_vec):
    scaled = grad_out * gain_vec
    mean_scaled = jnp.mean(scaled, axis=-1, keepdims=True)
    mean_cross = jnp.mean(scaled * normed, axis=-1, keepdims=True)
    return inv_std * (scaled - mean_scaled - normed * mean_cross)


def pin(value, *after):
    return lax.optimization_barrier((value,) + after)[0] if after else value


class RingGather:
    def __init__(self, block):
        self.ahead = self.behind = block
        self.half = block.shape[0] // 2
        self.blocks = [block] + [None] * 7
        self.done = 0

    def step(self, *after):
        self.done += 1
        ahead, behind = self.ahead, self.behind
        if after:
            ahead, behind = pin(ahead, *after), pin(behind, *after)
        if self.done == 4:
            ahead, behind = ahead[: self.half], behind[self.half :]
        ahead = lax.ppermute(ahead, "fsdp", NEXT)
        behind = lax.ppermute(behind, "fsdp", PREV)
        if self.done == 4:
            self.blocks[4] = (ahead, behind)
        else:
            self.blocks[8 - self.done], self.blocks[self.done] = ahead, behind
        self.ahead, self.behind = ahead, behind
        return ahead, behind

    def pieces(self):
        for j, block in enumerate(self.blocks):
            if j == 4:
                yield j, 0, block[0]
                yield j, self.half, block[1]
            else:
                yield j, 0, block


class RingScatter:
    def __init__(self, blocks):
        self.blocks = blocks
        self.half = blocks[0].shape[0] // 2
        self.ahead, self.behind = blocks[4][: self.half], blocks[4][self.half :]
        self.done = 0

    def step(self, *after):
        self.done += 1
        half = self.half
        ahead = lax.ppermute(pin(self.ahead, *after), "fsdp", NEXT)
        behind = lax.ppermute(pin(self.behind, *after), "fsdp", PREV)
        got = (ahead, behind)
        ahead, behind = ahead.astype(F32), behind.astype(F32)
        if self.done == 1:
            up, down = self.blocks[3].astype(F32), self.blocks[5].astype(F32)
            ahead = jnp.concatenate([up[:half] + ahead, up[half:]])
            behind = jnp.concatenate([down[:half], down[half:] + behind])
        elif self.done < 4:
            ahead = self.blocks[4 - self.done].astype(F32) + ahead
            behind = self.blocks[4 + self.done].astype(F32) + behind
        else:
            self.total = self.blocks[0].astype(F32) + ahead + behind
            return got
        self.ahead, self.behind = ahead.astype(BF16), behind.astype(BF16)
        return got


def seq_gather(mine, hold=()):
    over = lax.ppermute(mine, "seq", ROW)
    beside = lax.ppermute(mine, "seq", CORE)
    return [mine, beside, over, lax.ppermute(pin(over, *hold), "seq", CORE)]


def seq_scatter(parts):
    corner = lax.ppermute(parts[3].astype(BF16), "seq", CORE)
    beside = lax.ppermute(parts[1].astype(BF16), "seq", CORE)
    far = (parts[2] + corner.astype(F32)).astype(BF16)
    over = lax.ppermute(far, "seq", ROW)
    return parts[0] + beside.astype(F32) + over.astype(F32), far


class Fast:
    def __init__(self, s, f):
        self.s, self.f = s, f
        table = lax.dynamic_index_in_dim(jnp.asarray(ORDER), f, 0, keepdims=False)
        self.order = [table[j] for j in range(8)]
        self.slots = jnp.arange(4, dtype=jnp.int32) ^ s
        self.rings = {}

    def gather(self, **blocks):
        self.rings.update({name: RingGather(block) for name, block in blocks.items()})

    def scatter(self, **wholes):
        for name, whole in wholes.items():
            order = self.order if name in "FS" else range(8)
            size = whole.shape[0] // 8
            self.rings[name] = RingScatter(
                [lax.dynamic_slice_in_dim(whole, order[j] * size, size, 0) for j in range(8)]
            )

    def hop(self, names, *after):
        got = ()
        for name in names:
            got += self.rings[name].step(*after)
        return got

    def gather_out(self, w_out, small, count):
        size = w_out.shape[0] // 4
        self.out_rows = size
        own = lax.dynamic_slice_in_dim(w_out, self.s * size, size, 0)
        pad = jnp.full((w_out.shape[1] - small.shape[0],), count.astype(BF16))
        line = jnp.broadcast_to(jnp.concatenate([small, pad])[None], (16, w_out.shape[1]))
        self.gather(o=jnp.concatenate([own, line]))

    def close_out(self):
        whole = self.as_found(self.rings["o"])
        whole = whole.reshape(8, -1, whole.shape[1])
        places = (jnp.asarray(PLACE) - jnp.asarray(PLACE)[self.f]) % 8
        rows = jnp.take(whole[:, : self.out_rows], places, axis=0)
        small = jnp.take(whole[:, self.out_rows], places, axis=0)
        return rows.reshape(-1, whole.shape[2]), small.astype(F32)

    def whole(self, name):
        return self.in_order(self.rings[name]) if name == "q" else self.as_found(self.rings[name])

    def scatter_pair(self, gate, up):
        gates, ups = (v.reshape(8, -1, v.shape[1]) for v in (gate, up))
        self.rings["W"] = RingScatter([jnp.concatenate([gates[j], ups[j]]) for j in range(8)])

    def scatter_first(self, raw_first, raw_out, *after):
        rows, cols = raw_out.shape
        split = raw_out.reshape(8, rows // 8, 4, cols // 4).transpose(0, 2, 1, 3)
        both = jnp.concatenate([raw_first, split.reshape(-1, cols // 4)], axis=1)
        self.first_cols = raw_first.shape[1]
        self.scatter(F=pin(both, *after))

    def total(self, name):
        if name not in "FO":
            return self.rings[name].total
        total = self.rings["F"].total
        if name == "F":
            return total[:, : self.first_cols]
        split = total[:, self.first_cols :].reshape(4, self.out_rows, -1)
        return split.transpose(1, 0, 2).reshape(self.out_rows, -1)

    def in_order(self, ring):
        size, cols = ring.blocks[0].shape
        whole = jnp.zeros((8 * size, cols), BF16)
        for j, first, part in ring.pieces():
            at = self.order[j] * size + first
            whole = lax.dynamic_update_slice(whole, part, (at, 0))
        return whole

    def as_found(self, ring):
        return jnp.concatenate([part for unused, unused, part in ring.pieces()])

    def pick_qkv(self, w_qkv):
        return pick_columns(w_qkv, self.s)

    def bias_of_heads(self, full_bias):
        split = full_bias.reshape(3, 4, 2, 4, HD)
        own = lax.dynamic_index_in_dim(split, self.s, 3, keepdims=False)
        return own.transpose(1, 0, 2, 3).reshape(1, 12 * LANES)

    def bias_of_all(self, own):
        split = own.reshape(4, 3, 2, HD).transpose(1, 0, 2, 3)
        here = (jnp.arange(4) == self.s).astype(F32)[None, None, None, :, None]
        return (split[:, :, :, None, :] * here).reshape(-1)

    def spread(self, name, *after, hold=()):
        return seq_gather(pin(self.total(name).astype(BF16), *after), hold)

    def final_qkv(self, first, second, factor):
        return unpick_columns([first, second], self.s, factor)

    def final_rows(self, parts, factor):
        return place_rows(parts, self.s, factor)

    final_out = final_rows

    def final_pairs(self, parts, factor):
        return place_pairs(parts, self.s, factor)

    def tokens(self, mine):
        return jnp.concatenate(seq_gather(mine))

    def tokens_sum(self, partial):
        rows = partial.shape[0] // 4
        return seq_scatter([partial[i * rows : (i + 1) * rows] for i in range(4)])

    def by_slot(self, values):
        split = values.reshape((4, values.shape[0] // 4) + values.shape[1:])
        return jnp.take(split, self.slots, axis=0).reshape(values.shape)

    def small_reduce(self, values, *after):
        total = jnp.take(values, self.f ^ jnp.arange(8), axis=0)
        for bit in (4, 2, 1):
            other = lax.ppermute(total[bit:], "fsdp", [(i, i ^ bit) for i in range(8)])
            total = total[:bit] + other
        return self.seq_sum(pin(total[0], *after))

    def seq_sum(self, total):
        total = total + lax.ppermute(total, "seq", CORE)
        return total + lax.ppermute(total, "seq", ROW)


class General:
    def __init__(self, s, f):
        self.s, self.f = s, f
        self.members, self.shards = lax.axis_size("seq"), lax.axis_size("fsdp")
        self.slots = jnp.arange(self.members, dtype=jnp.int32)
        self.pairs = H // self.members // 2
        self.wholes, self.totals = {}, {}

    def gather(self, **blocks):
        for name, block in blocks.items():
            self.wholes[name] = lax.all_gather(block, "fsdp", axis=0, tiled=True)

    def scatter(self, **wholes):
        for name, whole in wholes.items():
            if name == "O":
                rows = whole.shape[0]
                every = jnp.zeros((rows * self.members, whole.shape[1]), whole.dtype)
                whole = lax.dynamic_update_slice(every, whole, (self.s * rows, 0))
            total = lax.psum_scatter(whole, "fsdp", scatter_dimension=0, tiled=True)
            self.totals[name] = total.astype(F32)

    def hop(self, names, *after):
        return ()

    def gather_out(self, w_out, small, count):
        self.gather(o=w_out)
        small = jnp.concatenate([small.astype(F32), jnp.full((LANES,), count)])
        self.small = lax.all_gather(small, "fsdp", axis=0, tiled=False)

    def close_out(self):
        rows = self.wholes["o"].shape[0] // self.members
        own = lax.dynamic_slice_in_dim(self.wholes["o"], self.s * rows, rows, 0)
        return own, self.small

    def whole(self, name):
        return self.wholes[name]

    def scatter_pair(self, gate, up):
        both = [v.reshape(self.shards, -1, v.shape[1]) for v in (gate, up)]
        self.scatter(W=jnp.concatenate(both, axis=1).reshape(-1, gate.shape[1]))

    def scatter_first(self, raw_first, raw_out, *after):
        self.scatter(F=raw_first, O=raw_out)

    def total(self, name):
        return self.totals[name]

    def pick_qkv(self, w_qkv):
        split = w_qkv.reshape(w_qkv.shape[0], 3, self.members, self.pairs, LANES)
        own = lax.dynamic_index_in_dim(split, self.s, 2, keepdims=False)
        return own.transpose(0, 2, 1, 3).reshape(w_qkv.shape[0], -1)

    def bias_of_heads(self, full_bias):
        split = full_bias.reshape(3, self.members, self.pairs, LANES)
        own = lax.dynamic_index_in_dim(split, self.s, 1, keepdims=False)
        return own.transpose(1, 0, 2).reshape(1, -1)

    def bias_of_all(self, own):
        split = own.reshape(self.pairs, 3, LANES).transpose(1, 0, 2)
        here = (jnp.arange(self.members) == self.s).astype(F32)[None, :, None, None]
        return (split[:, None] * here).reshape(-1)

    def gathered(self, share):
        return lax.all_gather(share.astype(BF16), "seq", axis=0, tiled=False)

    def spread(self, name, *after, hold=()):
        return [self.total(name)]

    def final_qkv(self, first, second, factor):
        share = jnp.concatenate(first + second, axis=1)
        parts = self.gathered(share).reshape(self.members, -1, self.pairs, 3, LANES)
        return factor * parts.transpose(1, 3, 0, 2, 4).reshape(parts.shape[1], -1).astype(F32)

    def final_rows(self, parts, factor):
        share = parts[0]
        return factor * self.gathered(share).reshape(-1, share.shape[1]).astype(F32)

    def final_out(self, parts, factor):
        return factor * lax.psum(parts[0].astype(BF16), "seq").astype(F32)

    def final_pairs(self, parts, factor):
        rows = parts[0].shape[0] // 2
        parts = jnp.stack([parts[0][:rows], parts[0][rows:]], axis=1)
        parts = lax.all_gather(parts.astype(BF16), "seq", axis=0, tiled=True)
        return factor * parts.astype(F32)

    def tokens(self, mine):
        return lax.all_gather(mine, "seq", axis=0, tiled=True)

    def tokens_sum(self, partial):
        total = lax.psum_scatter(partial.astype(BF16), "seq", scatter_dimension=0, tiled=True)
        return total.astype(F32), total

    def by_slot(self, values):
        return values

    def small_reduce(self, values, *after):
        total = lax.psum(values, ("seq", "fsdp"))
        return lax.dynamic_index_in_dim(total, self.f, 0, keepdims=False)

    def seq_sum(self, total):
        return lax.psum(total, "seq")


def call(kernel, grid, in_specs, out_specs, out_shape, scratch=(), prefetch=0, cost=None):
    return pl.pallas_call(
        kernel,
        grid_spec=pltpu.PrefetchScalarGridSpec(
            num_scalar_prefetch=prefetch,
            grid=grid,
            in_specs=in_specs,
            out_specs=out_specs,
            scratch_shapes=list(scratch),
        ),
        out_shape=out_shape,
        compiler_params=pltpu.CompilerParams(vmem_limit_bytes=VMEM_LIMIT),
        cost_estimate=cost,
    )


def pick_kernel(s_ref, w_ref, out_ref):
    s = s_ref[0]
    lane = lax.broadcasted_iota(jnp.int32, (w_ref.shape[0], LANES), 1)
    odd = (s & 1) == 1
    for pair in range(4):
        for part in range(3):
            at = part * 2048 + pair * 512 + (s >> 1) * LANES
            one = w_ref[:, pl.ds(pl.multiple_of(at, LANES), LANES)].astype(F32)
            two = w_ref[:, pl.ds(pl.multiple_of(at + 256, LANES), LANES)].astype(F32)
            one = jnp.where(odd, pltpu.roll(one, HD, 1), one)
            two = jnp.where(odd, two, pltpu.roll(two, HD, 1))
            to = (pair * 3 + part) * LANES
            out_ref[:, to : to + LANES] = jnp.where(lane < HD, one, two).astype(BF16)


def pick_columns(w_qkv, s):
    rows, cols = w_qkv.shape
    step = rows // 4
    return call(
        pick_kernel,
        (4,),
        [pl.BlockSpec((step, cols), lambda g, s_ref: (g, 0))],
        pl.BlockSpec((step, 12 * LANES), lambda g, s_ref: (g, 0)),
        jax.ShapeDtypeStruct((rows, 12 * LANES), BF16),
        prefetch=1,
    )(s.reshape(1), w_qkv)


def unpick_kernel(s_ref, factor_ref, *refs):
    out_ref, ordered = refs[-2:]
    s = s_ref[0]
    factor = factor_ref[0]
    rows = out_ref.shape[0]
    lane = lax.broadcasted_iota(jnp.int32, (rows, LANES), 1)
    for half in range(2):
        for r in range(4):
            ordered[s ^ r] = refs[4 * half + r][...].astype(F32) * factor
        for pair in range(2):
            for part in range(3):
                at = slice((pair * 3 + part) * LANES, (pair * 3 + part + 1) * LANES)
                heads = [ordered[m, :, at] for m in range(4)]
                turned = [pltpu.roll(h, HD, 1) for h in heads]
                to = part * 2048 + (2 * half + pair) * 512
                for m in (0, 2):
                    low = jnp.where(lane < HD, heads[m], turned[m + 1])
                    high = jnp.where(lane < HD, turned[m], heads[m + 1])
                    out_ref[:, to + m * HD : to + m * HD + LANES] = low
                    out_ref[:, to + 256 + m * HD : to + 256 + m * HD + LANES] = high


def unpick_columns(parts, s, factor):
    rows, cols = parts[0][0].shape
    step = rows // 4
    return call(
        unpick_kernel,
        (4,),
        [pl.BlockSpec(memory_space=pltpu.SMEM)]
        + [pl.BlockSpec((step, cols), lambda g, s_ref: (g, 0))] * 8,
        pl.BlockSpec((step, 8 * cols), lambda g, s_ref: (g, 0)),
        jax.ShapeDtypeStruct((rows, 8 * cols), F32),
        scratch=[pltpu.VMEM((4, step, cols), F32)],
        prefetch=1,
    )(s.reshape(1), factor.reshape(1), *parts[0], *parts[1])


def place_kernel(s_ref, factor_ref, p0, p1, p2, p3, out_ref):
    r = pl.program_id(0)
    for k, part in enumerate((p0, p1, p2, p3)):

        @pl.when(r == k)
        def _(part=part):
            out_ref[...] = part[...].astype(F32) * factor_ref[0]


def place_rows(parts, s, factor):
    rows, cols = parts[0].shape
    return call(
        place_kernel,
        (4,),
        [pl.BlockSpec(memory_space=pltpu.SMEM)]
        + [pl.BlockSpec((rows, cols), lambda r, s_ref: (0, 0))] * 4,
        pl.BlockSpec((rows, cols), lambda r, s_ref: (s_ref[0] ^ r, 0)),
        jax.ShapeDtypeStruct((4 * rows, cols), F32),
        prefetch=1,
    )(s.reshape(1), factor.reshape(1), *parts)


def place_pair_kernel(s_ref, factor_ref, p0, p1, p2, p3, out_ref):
    r = pl.program_id(0)
    rows = out_ref.shape[0]
    for k, part in enumerate((p0, p1, p2, p3)):

        @pl.when(r == k)
        def _(part=part):
            out_ref[:, 0, :] = part[:rows, :].astype(F32) * factor_ref[0]
            out_ref[:, 1, :] = part[rows:, :].astype(F32) * factor_ref[0]


def place_pairs(parts, s, factor):
    rows, cols = parts[0].shape
    half = rows // 2
    return call(
        place_pair_kernel,
        (4,),
        [pl.BlockSpec(memory_space=pltpu.SMEM)]
        + [pl.BlockSpec((rows, cols), lambda r, s_ref: (0, 0))] * 4,
        pl.BlockSpec((half, 2, cols), lambda r, s_ref: (s_ref[0] ^ r, 0, 0)),
        jax.ShapeDtypeStruct((4 * half, 2, cols), F32),
        prefetch=1,
    )(s.reshape(1), factor.reshape(1), *parts)


def turn(values, cosine, sine_low, sine_high, sign):
    half = ROT // 2
    moved = (
        pltpu.roll(values, LANES - half, 1) * sine_low + pltpu.roll(values, half, 1) * sine_high
    )
    return values * cosine + moved if sign > 0 else values * cosine - moved


def two_heads(values):
    lane = lax.broadcasted_iota(jnp.int32, values.shape, 1)
    nothing = jnp.zeros_like(values)
    return jnp.concatenate(
        [jnp.where(lane < HD, values, nothing), jnp.where(lane < HD, nothing, values)], axis=0
    )


def one_pair(stacked):
    rows = stacked.shape[0] // 2
    lane = lax.broadcasted_iota(jnp.int32, (rows, LANES), 1)
    return jnp.where(lane < HD, stacked[:rows], stacked[rows:])


def forward_kernel(
    block, slots, slot_ref, first_ref, qkv, bias, cosine, low, high, start, turned, out
):
    scale = HD ** (-0.5)

    def rotate_block(i, unused):
        rows = pl.ds(pl.multiple_of(i * block, block), block)
        tables = (cosine[rows, :], low[rows, :], high[rows, :], 1)
        query = qkv[rows, 0:LANES] + bias[:, 0:LANES]
        key = qkv[rows, LANES : 2 * LANES] + bias[:, LANES : 2 * LANES]
        value = qkv[rows, 2 * LANES : 3 * LANES] + bias[:, 2 * LANES : 3 * LANES]
        turned[rows, 0:LANES] = turn(query, *tables).astype(BF16)
        turned[rows, LANES : 2 * LANES] = turn(key, *tables).astype(BF16)
        turned[rows, 2 * LANES : 3 * LANES] = value.astype(BF16)
        return unused

    lax.fori_loop(0, slots, rotate_block, 0)

    column = lax.broadcasted_iota(jnp.int32, (2 * block, block), 1)
    line = lax.broadcasted_iota(jnp.int32, (2 * block, block), 0) & (block - 1)

    def query_block(i, unused):
        rows = pl.ds(pl.multiple_of(slot_ref[i] * block, block), block)
        query = two_heads((turned[rows, 0:LANES].astype(F32) * scale).astype(BF16))
        first = start[rows, :]
        first = jnp.concatenate([first, first], axis=0)

        def scores(j):
            keys = pl.ds(pl.multiple_of(slot_ref[j] * block, block), block)
            result = dot_nt(query, turned[keys, LANES : 2 * LANES])
            allowed = column >= first - j * block
            return result, allowed, turned[keys, 2 * LANES : 3 * LANES]

        result, allowed, value = scores(i)
        result = jnp.where(allowed & (column <= line), result, MASKED_VALUE)
        peak = jnp.max(result, axis=1, keepdims=True)
        weight = jnp.exp(result - peak)
        total = jnp.sum(weight, axis=1, keepdims=True)
        gathered = dot_nn(weight.astype(BF16), value)

        def key_block(j, carry):
            peak, total, gathered = carry
            result, allowed, value = scores(j)
            result = jnp.where(allowed, result, MASKED_VALUE)
            higher = jnp.maximum(peak, jnp.max(result, axis=1, keepdims=True))
            shrink = jnp.exp(peak - higher)
            weight = jnp.exp(result - higher)
            total = total * shrink + jnp.sum(weight, axis=1, keepdims=True)
            gathered = gathered * shrink + dot_nn(weight.astype(BF16), value)
            return higher, total, gathered

        peak, total, gathered = lax.fori_loop(first_ref[i], i, key_block, (peak, total, gathered))
        out[rows, :] = one_pair(gathered / total).astype(BF16)
        return unused

    lax.fori_loop(0, slots, query_block, 0)


def attention_forward(qkv, bias, tables, start, slot_of, first_slot, *, block, skip, pairs):
    length = qkv.shape[0]
    width = pairs * 3 * LANES
    slots = length // block
    whole = pl.BlockSpec((length, LANES), lambda p, *_: (0, 0))
    return call(
        functools.partial(forward_kernel, block, slots),
        (pairs,),
        [
            pl.BlockSpec((length, 3 * LANES), lambda p, *_: (0, p + skip)),
            pl.BlockSpec((1, 3 * LANES), lambda p, *_: (0, p + skip)),
            whole,
            whole,
            whole,
            pl.BlockSpec((length, 1), lambda p, *_: (0, 0)),
        ],
        [
            pl.BlockSpec((length, 3 * LANES), lambda p, *_: (0, p)),
            pl.BlockSpec((length, LANES), lambda p, *_: (0, p)),
        ],
        [
            jax.ShapeDtypeStruct((length, width), BF16),
            jax.ShapeDtypeStruct((length, width // 3), BF16),
        ],
        prefetch=2,
        cost=pl.CostEstimate(
            flops=length * length * width * 2,
            bytes_accessed=length * width * 8,
            transcendentals=length * length * width // (3 * HD),
        ),
    )(slot_of, first_slot, qkv, bias, *tables, start)


def backward_kernel(
    block,
    slots,
    slot_ref,
    first_ref,
    turned,
    out_grad,
    cosine,
    low,
    high,
    start,
    grads,
    key_sum,
    value_sum,
    weights,
    products,
):
    scale = HD ** (-0.5)
    key_sum[...] = jnp.zeros_like(key_sum)
    value_sum[...] = jnp.zeros_like(value_sum)
    column = lax.broadcasted_iota(jnp.int32, (block, 2 * block), 1) & (block - 1)
    line = lax.broadcasted_iota(jnp.int32, (block, 2 * block), 0)

    def query_block(i, unused):
        begin = pl.multiple_of(slot_ref[i] * block, block)
        rows = pl.ds(begin, block)
        query = two_heads((turned[rows, 0:LANES].astype(F32) * scale).astype(BF16))
        grad = two_heads(out_grad[rows, :])
        first = start[:, pl.ds(begin, block)]
        first = jnp.concatenate([first, first], axis=1)

        def scores(j):
            keys = pl.ds(pl.multiple_of(slot_ref[j] * block, block), block)
            result = dot_nt(turned[keys, LANES : 2 * LANES], query)
            return result, line >= first - j * block

        result, allowed = scores(i)
        result = jnp.where(allowed & (line <= column), result, MASKED_VALUE)
        weights[0] = result
        peak = jnp.max(result, axis=0, keepdims=True)

        def score_block(j, peak):
            result, allowed = scores(j)
            result = jnp.where(allowed, result, MASKED_VALUE)
            weights[i - j] = result
            return jnp.maximum(peak, jnp.max(result, axis=0, keepdims=True))

        peak = lax.fori_loop(first_ref[i], i, score_block, peak)

        def weight_block(j, carry):
            total, cross = carry
            keys = pl.ds(pl.multiple_of(slot_ref[j] * block, block), block)
            weight = jnp.exp(weights[i - j] - peak)
            product = dot_nt(turned[keys, 2 * LANES : 3 * LANES], grad)
            weights[i - j] = weight
            products[i - j] = product
            total = total + jnp.sum(weight, axis=0, keepdims=True)
            cross = cross + jnp.sum(weight * product, axis=0, keepdims=True)
            return total, cross

        zero = jnp.zeros((1, 2 * block), F32)
        total, cross = lax.fori_loop(first_ref[i], i + 1, weight_block, (zero, zero))
        share = 1.0 / total
        cross = cross * share

        def grad_block(j, query_sum):
            keys = pl.ds(pl.multiple_of(slot_ref[j] * block, block), block)
            weight = weights[i - j] * share
            score_grad = (weight * (products[i - j] - cross)).astype(BF16)
            value_sum[keys, :] += dot_nn(weight.astype(BF16), grad)
            key_sum[keys, :] += dot_nn(score_grad, query)
            return query_sum + dot_tn(score_grad, turned[keys, LANES : 2 * LANES])

        query_sum = lax.fori_loop(
            first_ref[i], i + 1, grad_block, jnp.zeros((2 * block, LANES), F32)
        )
        tables = (cosine[rows, :], low[rows, :], high[rows, :], -1)
        grads[rows, 0:LANES] = turn(one_pair(query_sum) * scale, *tables).astype(BF16)
        return unused

    lax.fori_loop(0, slots, query_block, 0)

    def finish(i, unused):
        rows = pl.ds(pl.multiple_of(i * block, block), block)
        tables = (cosine[rows, :], low[rows, :], high[rows, :], -1)
        grads[rows, LANES : 2 * LANES] = turn(key_sum[rows, :], *tables).astype(BF16)
        grads[rows, 2 * LANES : 3 * LANES] = value_sum[rows, :].astype(BF16)
        return unused

    lax.fori_loop(0, slots, finish, 0)


def attention_backward(turned, out_grad, tables, start, slot_of, first_slot, block, skip):
    length, width = turned.shape
    pairs = width // (3 * LANES)
    slots = length // block
    whole = pl.BlockSpec((length, LANES), lambda p, *_: (0, 0))
    return call(
        functools.partial(backward_kernel, block, slots),
        (pairs,),
        [
            pl.BlockSpec((length, 3 * LANES), lambda p, *_: (0, p)),
            pl.BlockSpec((length, LANES), lambda p, *_: (0, p + skip)),
            whole,
            whole,
            whole,
            pl.BlockSpec((1, length), lambda p, *_: (0, 0)),
        ],
        pl.BlockSpec((length, 3 * LANES), lambda p, *_: (0, p)),
        jax.ShapeDtypeStruct((length, width), BF16),
        scratch=[
            pltpu.VMEM((length, LANES), F32),
            pltpu.VMEM((length, LANES), F32),
            pltpu.VMEM((slots, block, 2 * block), F32),
            pltpu.VMEM((slots, block, 2 * block), F32),
        ],
        prefetch=2,
        cost=pl.CostEstimate(
            flops=length * length * width * 5,
            bytes_accessed=length * width * 6,
            transcendentals=length * length * width // (3 * HD),
        ),
    )(slot_of, first_slot, turned, out_grad, *tables, start)


def turn_tables(positions):
    half = ROT // 2
    lane = jnp.arange(LANES, dtype=jnp.int32) % HD
    inverse = 10000.0 ** (-((lane % half).astype(F32) * 2.0) / ROT)
    angles = positions.astype(F32)[:, None] * jnp.where(lane < ROT, inverse, 0.0)[None, :]
    cosine, sine = jnp.cos(angles), jnp.sin(angles)
    lane = lane[None, :]
    return (
        cosine,
        jnp.where(lane < half, -sine, 0.0),
        jnp.where((lane >= half) & (lane < ROT), sine, 0.0),
    )


def per_device(
    tokens,
    teacher,
    segments,
    valid,
    ln1_gain,
    ln1_bias,
    w_qkv,
    b_qkv,
    w_out,
    ln2_gain,
    ln2_bias,
    w_gate_up,
    w_down,
):
    s = lax.axis_index("seq")
    f = lax.axis_index("fsdp")
    members, shards = lax.axis_size("seq"), lax.axis_size("fsdp")
    net = (Fast if (members, shards) == (4, 8) else General)(s, f)
    rows = tokens.shape[1]
    width = tokens.shape[2]
    length = segments.shape[1]
    units = w_down.shape[0] // members
    vec = ln1_gain.shape[0]
    bias_share = b_qkv.shape[0]
    pairs = H // members // 2

    tokens_all = net.tokens(tokens[0])

    mine_gate_up = lax.dynamic_slice_in_dim(w_gate_up, s * units, units, 0)
    counted = valid[0].astype(F32)
    small = jnp.concatenate([ln1_gain, ln1_bias, ln2_gain, ln2_bias, b_qkv])
    net.gather_out(w_out, small, jnp.sum(counted))
    net.gather(
        q=net.pick_qkv(w_qkv),
        g=mine_gate_up[:, 0],
        u=mine_gate_up[:, 1],
        d=lax.dynamic_slice_in_dim(w_down, s * units, units, 0),
    )
    done = net.hop("qo")

    normed_all, unused = norm_parts(pin(tokens_all, *done).astype(F32))
    done = net.hop("q")

    segment = pin(segments, *done)[0]
    slot_segment = net.by_slot(segment)
    slot_start = jnp.sum((segment[None, :] < slot_segment[:, None]).astype(jnp.int32), axis=1)
    slot_place = net.by_slot(jnp.arange(length, dtype=jnp.int32))
    block_first = segment.reshape(members, rows)[:, 0]
    first_slot = (
        jnp.sum((segment[None, :] < block_first[:, None]).astype(jnp.int32), axis=1) // rows
    )
    done = net.hop("q") + net.hop("o", *done)
    tables = turn_tables(slot_place - pin(slot_start, *done))
    net.hop("qo", *done)
    net.hop("o")
    full_out, small = net.close_out()
    gain_one, shift_one, gain_two, shift_two = (
        small[:, i * vec : (i + 1) * vec].reshape(width) for i in range(4)
    )
    own_bias = net.bias_of_heads(small[:, 4 * vec : 4 * vec + bias_share].reshape(-1))
    sum_count = net.seq_sum(jnp.sum(small[:, -LANES:], axis=0))[0]
    factor = (rows * members * shards) / sum_count
    hidden_one = (normed_all * gain_one + shift_one).astype(BF16)
    done = net.hop("g", *done)
    qkv = dot_nn(hidden_one, pin(net.whole("q"), *done, *tables))
    half_pairs = pairs // 2
    forward = functools.partial(
        attention_forward,
        qkv,
        own_bias,
        tables,
        slot_start[:, None],
        net.slots,
        block=rows,
        pairs=half_pairs,
    )
    turned_one, heads_one = forward(pin(first_slot, factor), skip=0)
    done = net.hop("gu", *done)
    turned_two, heads_two = forward(pin(first_slot, heads_one, *done), skip=half_pairs)
    heads_out = jnp.concatenate([heads_one, heads_two], axis=1)
    tokens_in = tokens[0].astype(F32)
    done = net.hop("gu", heads_one)
    partial = dot_nn(pin(heads_out, *done), full_out)
    attended = net.tokens_sum(partial)[0]
    done = net.hop("gu", heads_two)
    resid = tokens_in + pin(attended, *done)

    normed_two, inv_std_two = norm_parts(resid)
    mine_two = (normed_two * gain_two + shift_two).astype(BF16)
    hidden_two = net.tokens(mine_two)
    done = net.hop("u", mine_two) + net.hop("d", mine_two)
    full_gate = net.whole("g")
    gate = dot_nt(full_gate, pin(hidden_two, *done))
    done = net.hop("d")
    full_up = net.whole("u")
    up = dot_nt(pin(full_up, gate, *done), hidden_two)
    hidden = (jax.nn.silu(gate) * up).astype(BF16)
    done = net.hop("d", gate)
    hidden = pin(hidden, *done)
    net.hop("d", hidden)
    full_down = net.whole("d")
    outputs = resid + net.tokens_sum(dot_tn(hidden, full_down))[0]
    differ = outputs - teacher[0].astype(F32)
    cot = counted[:, None] * differ
    half_sum = 0.5 * jnp.sum(cot * differ)
    cot_low = net.tokens(cot.astype(BF16))

    raw_down = dot_nn(hidden, cot_low).astype(BF16)
    net.scatter(D=raw_down)
    done = net.hop("D")
    hidden_grad = dot_nt(pin(full_down, raw_down), cot_low)
    sigma = jax.nn.sigmoid(gate)
    silu_grad = hidden_grad * up
    gate_grad = (silu_grad * sigma + silu_grad * gate * sigma * (1.0 - sigma)).astype(BF16)
    up_grad = (hidden_grad * (gate * sigma)).astype(BF16)

    raw_gate = dot_nn(gate_grad, pin(hidden_two, *done)).astype(BF16)
    raw_up = dot_nn(up_grad, pin(hidden_two, raw_gate)).astype(BF16)
    done = net.hop("D", gate_grad)
    partial = dot_tn(gate_grad, pin(full_gate, raw_up, *done))
    done = net.hop("D")
    partial = partial + dot_tn(up_grad, pin(full_up, partial))
    two_grad, far = net.tokens_sum(pin(partial, *done))
    net.scatter_pair(pin(raw_gate, *done), pin(raw_up, *done))
    done = net.hop("DW", far)

    two_grad = pin(two_grad, *done)
    resid_grad = cot + norm_back(two_grad, normed_two, inv_std_two, gain_two)
    gain_two_grad = jnp.sum(two_grad * normed_two, axis=0)
    shift_two_grad = jnp.sum(two_grad, axis=0)
    mine_low = resid_grad.astype(BF16)
    resid_low = net.tokens(mine_low)
    done = net.hop("W", mine_low)

    full_qkv = net.whole("q")
    out_grad = dot_nt(pin(resid_low, *done), full_out).astype(BF16)
    backward = functools.partial(
        attention_backward,
        tables=tables,
        start=slot_start[None, :],
        slot_of=net.slots,
        block=rows,
    )
    grad_first = backward(turned_one, out_grad, first_slot=first_slot, skip=0)
    raw_out = dot_tn(heads_out, pin(resid_low, grad_first)).astype(BF16)
    raw_first = dot_tn(hidden_one, grad_first).astype(BF16)
    done = net.hop("W", out_grad)

    net.scatter_first(raw_first, raw_out, *done)
    parts_down = net.spread("D", out_grad)
    here = pin(first_slot, raw_first, *done, *parts_down)
    grad_second = backward(turned_two, out_grad, first_slot=here, skip=half_pairs)
    done = net.hop("F", raw_first) + net.hop("W")

    raw_second = dot_tn(hidden_one, pin(grad_second, *done)).astype(BF16)
    done = net.hop("F", grad_second)
    qkv_grad = pin(jnp.concatenate([grad_first, grad_second], axis=1), raw_second, *done)
    net.scatter(S=pin(raw_second, *done))
    partial = dot_nt(qkv_grad, full_qkv)
    done = net.hop("FS")

    grad_one, far = net.tokens_sum(pin(partial, *done))
    done = net.hop("FS", far)

    third = net.hop("S", *done)
    normed_one, inv_std_one = norm_parts(tokens_in)
    tokens_grad = resid_grad + norm_back(grad_one, normed_one, inv_std_one, gain_one)
    gain_one_grad = jnp.sum(grad_one * normed_one, axis=0)
    shift_one_grad = jnp.sum(grad_one, axis=0)
    bias_grad = net.bias_of_all(jnp.sum(qkv_grad.astype(F32), axis=0)).reshape(shards, -1)
    vectors = jnp.concatenate(
        [
            v.reshape(shards, vec)
            for v in (gain_one_grad, shift_one_grad, gain_two_grad, shift_two_grad)
        ]
        + [bias_grad, jnp.full((shards, LANES), half_sum)],
        axis=1,
    ).reshape(shards, -1, LANES)
    grad_w_down = net.final_rows(parts_down, pin(factor, raw_second))
    parts_first, parts_out = net.spread("F"), net.spread("O", *third)
    last = net.hop("S", *third)
    parts_pair = net.spread("W", grad_one, hold=last)
    vectors = net.small_reduce(vectors, *last).reshape(-1)
    loss = 2.0 * vectors[4 * vec + bias_share] / (sum_count * width)
    scaled = factor * vectors
    grad_w_gate_up = net.final_pairs(parts_pair, factor)
    grad_w_out = net.final_out(parts_out, factor)
    parts_second = net.spread("S", grad_w_down, grad_w_gate_up)

    return (
        outputs.astype(BF16)[None],
        loss,
        (factor * tokens_grad).astype(BF16)[None],
        scaled[:vec],
        scaled[vec : 2 * vec],
        net.final_qkv(parts_first, parts_second, factor),
        scaled[4 * vec : 4 * vec + bias_share],
        grad_w_out,
        scaled[2 * vec : 3 * vec],
        scaled[3 * vec : 4 * vec],
        grad_w_gate_up,
        grad_w_down,
    )


def solution(mesh):
    placed = (
        P("fsdp", "seq", None),
        P("fsdp", "seq", None),
        P("fsdp", None),
        P("fsdp", "seq"),
        P("fsdp"),
        P("fsdp"),
        P("fsdp", None),
        P("fsdp"),
        P("fsdp", None),
        P("fsdp"),
        P("fsdp"),
        P("fsdp", None, None),
        P("fsdp", None),
    )
    return jax.shard_map(
        per_device,
        mesh=mesh,
        in_specs=placed,
        out_specs=(
            P("fsdp", "seq", None),
            P(),
            P("fsdp", "seq", None),
            P("fsdp"),
            P("fsdp"),
            P("fsdp", None),
            P("fsdp"),
            P("fsdp", None),
            P("fsdp"),
            P("fsdp"),
            P("fsdp", None, None),
            P("fsdp", None),
        ),
        check_vma=False,
    )
```
